32 devices in a mesh: fsdp: 4 (over y, x), dp: 8 (over z, core).
Axes of the slice: x: 2, y: 2, z: 4, core: 2. Of those that a mesh axis runs over, the one named last changes fastest.
Arguments:
- hidden_in: bfloat16 [8192, 1536], P(('fsdp', 'dp')), may hold values from -6 to 6
- lengths: int32 [32, 4], P(('fsdp', 'dp')), may hold values from 0 to 256, as said below
- norm_gain: bfloat16 [1536], P(('fsdp', 'dp')), may hold values from 0.5 to 1.5
- in_proj: bfloat16 [1536, 6448], P(('fsdp', 'dp')), may hold values from -0.15625 to 0.15625
- conv_weight: bfloat16 [3328, 4], P(('fsdp', 'dp')), may hold values from -3 to 3
- conv_bias: bfloat16 [3328], P(('fsdp', 'dp')), may hold values from -3 to 3
- gate_gain: bfloat16 [3072], P(('fsdp', 'dp')), may hold values from 0.5 to 1.5
- out_proj: bfloat16 [3072, 1536], P(('fsdp', 'dp')), may hold values from -0.109375 to 0.109375
- decay_log: float32 [48], replicated, may hold values from -3 to 1.5
- step_bias: float32 [48], replicated, may hold values from -5 to -2
- skip_gain: float32 [48], replicated, may hold values from 0.5 to 1.5
- grad_out: bfloat16 [8192, 1536], P(('fsdp', 'dp')), may hold values from -6 to 6
Outputs:
- hidden_out: bfloat16 [8192, 1536], P(('fsdp', 'dp'))
- grad_in: float32 [8192, 1536], P(('fsdp', 'dp'))
- grad_norm_gain: float32 [1536], P(('fsdp', 'dp'))
- grad_in_proj: float32 [1536, 6448], P(('fsdp', 'dp'))
- grad_conv_weight: float32 [3328, 4], P(('fsdp', 'dp'))
- grad_conv_bias: float32 [3328], P(('fsdp', 'dp'))
- grad_gate_gain: float32 [3072], P(('fsdp', 'dp'))
- grad_out_proj: float32 [3072, 1536], P(('fsdp', 'dp'))
- grad_decay_log: float32 [48], replicated
- grad_step_bias: float32 [48], replicated
- grad_skip_gain: float32 [48], replicated
The draws below stay inside these ranges and needn't reach their ends.
Inputs may be any that keep to these rules, and one draw needn't show every extreme that they name: lengths[b] lists the sequences packed from the first row of block b on, in order; a length may be 0 (an empty slot); each block's lengths sum to at most 256 and the rows after that sum are padding; in every draw one block holds a single sequence of exactly 256 rows.
All inputs are finite; a program needn't handle non-finite values.
Results may differ from the reference program's by a relative error of at most 0.0063.
Values may be sent and summed in bfloat16 or wider, within the bound.
A program may use at most 192 MiB of HBM per device.

```python
import jax
import jax.numpy as jnp
from jax import lax

D = 1536
H = 48
K = 4
SPAN = 256
SEQS_DEV = 4
TOK_DEV = 256
DI = 3072
CONV = 3328
E = 6448
SHARDS = 32
TOKENS = 8192


def draw_lengths(key, part):
    first_key, second_key, third_key = jax.random.split(key, 3)
    totals = jax.random.randint(first_key, (SHARDS,), TOK_DEV // 16, TOK_DEV + 1).astype(jnp.int32)
    raw_cuts = jax.random.randint(second_key, (SHARDS, SEQS_DEV - 1), 0, 1048576).astype(jnp.int32)
    cuts = jnp.sort(raw_cuts % (totals[:, None] + 1), axis=1)
    bounds = jnp.concatenate([jnp.zeros((SHARDS, 1), jnp.int32), cuts, totals[:, None]], axis=1)
    pieces = bounds[:, 1:] - bounds[:, :-1]
    chosen = jax.random.randint(third_key, (), 0, SHARDS)
    full_row = (jnp.arange(SHARDS) == chosen)[:, None]
    first_col = (jnp.arange(SEQS_DEV) == 0)[None, :]
    filled = jnp.where(first_col, TOK_DEV, 0)
    return jnp.where(full_row, filled, pieces).astype(jnp.int32)


def block_levels(own_key, shape, cuts, smallest, largest):
    factor_of = 1.0
    for position, blocks in cuts:
        draws = jax.random.uniform(jax.random.fold_in(jax.random.fold_in(own_key, 6), position), (blocks,), jnp.float32, smallest / len(cuts), largest / len(cuts))
        factor_of = factor_of * jnp.repeat(jnp.exp(draws), shape[position] // blocks).reshape((-1,) + (1,) * (len(shape) - 1 - position))
    return factor_of


def centred(key, extent, scale, reach, cuts=(), kind=jnp.bfloat16):
    drawn = jax.random.normal(key, extent, jnp.float32) * scale
    if len(cuts) > 0:
        drawn = block_levels(key, extent, cuts, -0.22, 0.18) * drawn
    return jnp.clip(drawn, min=-reach, max=reach).astype(kind)


def setup_inputs(seed: int = 0) -> dict:
    key_of = jax.random.split(jax.random.key(seed), 13)
    return {
        "hidden_in": centred(key_of[0], (TOKENS, D), 1.0, 6.0, ((0, 32),)),
        "lengths": draw_lengths(jax.random.fold_in(key_of[12], 71), 0),
        "norm_gain": jnp.clip(1.0 + 0.1 * jax.random.normal(key_of[2], (D,), jnp.float32), 0.5, 1.5).astype(jnp.bfloat16),
        "in_proj": centred(key_of[3], (D, E), D ** -0.5, 0.15625, ((0, 32),)),
        "conv_weight": centred(key_of[4], (CONV, K), K ** -0.5, 3.0, ((0, 32),)),
        "conv_bias": centred(key_of[5], (CONV,), 0.5, 3.0, ((0, 32),)),
        "gate_gain": jnp.clip(1.0 + 0.1 * jax.random.normal(key_of[6], (DI,), jnp.float32), 0.5, 1.5).astype(jnp.bfloat16),
        "out_proj": centred(key_of[7], (DI, D), DI ** -0.5, 0.109375, ((0, 32),)),
        "decay_log": jnp.clip(jax.random.uniform(key_of[8], (H,), jnp.float32, -3.0, 1.5), -3.0, 1.5),
        "step_bias": jnp.clip(jax.random.uniform(key_of[9], (H,), jnp.float32, -5.0, -2.0), -5.0, -2.0),
        "skip_gain": jnp.clip(jax.random.uniform(key_of[10], (H,), jnp.float32, 0.5, 1.5), 0.5, 1.5),
        "grad_out": centred(key_of[11], (TOKENS, D), 1.0, 6.0, ((0, 32),)),
    }


EPS = 1e-05
full_precision = lax.Precision.HIGHEST

def segment_ids(lens_row, row_count):
    ends = jnp.cumsum(lens_row).astype(jnp.int32)
    places = jnp.arange(row_count, dtype=jnp.int32)
    seg_ids = lax.optimization_barrier(jnp.sum((places[:, None] >= ends[None, :]).astype(jnp.int32), axis=1)).astype(jnp.int32)
    valid = (seg_ids < lens_row.shape[0]).astype(jnp.float32)
    return (seg_ids, valid)

def pre_norm(values, weight):
    return values * lax.rsqrt(lax.optimization_barrier(jnp.mean(values * values, axis=1, keepdims=True)) + EPS) * weight[None, :]

def convolve(inputs, weight, bias_row, seg_ids):
    kernel_len = weight.shape[1]
    summed = bias_row[None, :] + inputs * weight[:, kernel_len - 1][None, :]
    for offset in range(1, kernel_len):
        shifted = jnp.pad(inputs, ((offset, 0), (0, 0)))[:-offset]
        earlier = jnp.pad(seg_ids, (offset, 0), constant_values=-1)[:-offset]
        keep_mask = (earlier == seg_ids).astype(jnp.float32)
        summed = summed + shifted * keep_mask[:, None] * weight[:, kernel_len - 1 - offset][None, :]
    return summed

def state_scan(x_act, steps_dt, decay_rate, b_mat, c_mat, skips, seg_ids):
    row_count = x_act.shape[0]
    head_count = steps_dt.shape[1]
    head_dim = x_act.shape[1] // head_count
    state_dim = b_mat.shape[1]
    blocks = row_count // SPAN
    x_blocks = x_act.reshape(blocks, SPAN, head_count, head_dim)
    dt_blocks = steps_dt.reshape(blocks, SPAN, head_count)
    b_blocks = b_mat.reshape(blocks, SPAN, state_dim)
    c_blocks = c_mat.reshape(blocks, SPAN, state_dim)
    seg_blocks = seg_ids.reshape(blocks, SPAN)
    lower_tri = jnp.arange(SPAN)[:, None] >= jnp.arange(SPAN)[None, :]

    def block_step(scan_carry, block_in):
        old_state, prev_seg = scan_carry
        x_blk, dt_blk, b_blk, c_blk, seg_blk = block_in
        log_decay = jnp.cumsum(dt_blk * decay_rate[None, :], axis=0)
        same_seq = (seg_blk[:, None] == seg_blk[None, :]) & lower_tri
        spread = log_decay.T[:, :, None] - log_decay.T[:, None, :]
        decays = jnp.exp(jnp.where(same_seq[None], spread, -jnp.inf))
        inner_cb = jnp.dot(c_blk, b_blk.T, precision=full_precision)
        mixing = decays * inner_cb[None] * dt_blk.T[:, None, :]
        result = jnp.einsum('hts,shp->thp', mixing, x_blk, precision=full_precision)
        enters = (seg_blk == prev_seg).astype(jnp.float32)
        carried = jnp.einsum('tn,hpn->thp', c_blk, old_state, precision=full_precision)
        result = result + jnp.exp(log_decay)[:, :, None] * enters[:, None, None] * carried
        result = result + skips[None, :, None] * x_blk
        last_seg = seg_blk[-1]
        tail_wts = jnp.exp(log_decay[-1][None, :] - log_decay) * (seg_blk == last_seg).astype(jnp.float32)[:, None] * dt_blk
        new_state = jnp.einsum('sh,shp,sn->hpn', tail_wts, x_blk, b_blk, precision=full_precision)
        keep_old = jnp.exp(log_decay[-1]) * (prev_seg == last_seg).astype(jnp.float32)
        new_state = new_state + keep_old[:, None, None] * old_state
        return ((new_state, last_seg), result)
    start_state = (jnp.zeros((head_count, head_dim, state_dim), jnp.float32), jnp.array(-1, jnp.int32))
    _, outputs = lax.scan(jax.checkpoint(block_step), start_state, (x_blocks, dt_blocks, b_blocks, c_blocks, seg_blocks))
    return outputs.reshape(row_count, head_count * head_dim)

def mixer_branch(projected, kernel, shift_bias, gate, rates, biases, skips, seg_ids, valid):
    inner_dim = gate.shape[0]
    conv_dim = shift_bias.shape[0]
    state_dim = (conv_dim - inner_dim) // 2
    gate_in = projected[:, :inner_dim]
    conv_in = projected[:, inner_dim:inner_dim + conv_dim]
    dt_raw = projected[:, inner_dim + conv_dim:]
    activ = jax.nn.silu(convolve(conv_in, kernel, shift_bias, seg_ids))
    x_act = activ[:, :inner_dim]
    b_mat = activ[:, inner_dim:inner_dim + state_dim]
    c_mat = activ[:, inner_dim + state_dim:]
    steps_dt = jax.nn.softplus(dt_raw + biases[None, :])
    decay_rate = -jnp.exp(rates)
    scanned = state_scan(x_act, steps_dt, decay_rate, b_mat, c_mat, skips, seg_ids)
    gated = scanned * jax.nn.silu(gate_in)
    scale = lax.rsqrt(lax.optimization_barrier(jnp.mean(gated * gated, axis=1, keepdims=True)) + EPS)
    return gated * scale * gate[None, :] * valid[:, None]

def reference(hidden_in, lengths, norm_gain, in_proj, conv_weight, conv_bias, gate_gain, out_proj, decay_log, step_bias, skip_gain, grad_out):
    gain_float = norm_gain.astype(jnp.float32)
    kernel_float = conv_weight.astype(jnp.float32)
    bias_float = conv_bias.astype(jnp.float32)
    gate_float = gate_gain.astype(jnp.float32)

    def per_device(totals, block):
        x_block, cot_block, lens_row = block
        seg_ids, valid = segment_ids(lens_row, TOK_DEV)
        x_float = x_block.astype(jnp.float32)
        normed32, norm_back = jax.vjp(pre_norm, x_float, gain_float)
        normed = normed32.astype(jnp.bfloat16)
        projected = jnp.dot(normed, in_proj, preferred_element_type=jnp.float32)

        def branch(proj_in, kernel, shift_bias, gate, rates, biases, skips):
            return mixer_branch(proj_in, kernel, shift_bias, gate, rates, biases, skips, seg_ids, valid)
        mixed32, branch_back = jax.vjp(branch, projected, kernel_float, bias_float, gate_float, decay_log, step_bias, skip_gain)
        mixed = mixed32.astype(jnp.bfloat16)
        output = (x_float + jnp.dot(mixed, out_proj, preferred_element_type=jnp.float32)).astype(jnp.bfloat16)
        grad_mixed = jnp.dot(cot_block, out_proj.T, preferred_element_type=jnp.float32)
        grad_proj, grad_kernel, grad_shift, grad_gate, grad_rates, grad_biases, grad_skips = branch_back(grad_mixed)
        proj_low = grad_proj.astype(jnp.bfloat16)
        grad_normed = jnp.dot(proj_low, in_proj.T, preferred_element_type=jnp.float32)
        grad_x, grad_gain = norm_back(grad_normed)
        grad_rows = cot_block.astype(jnp.float32) + grad_x
        terms = (grad_gain, jnp.dot(normed.T, proj_low, preferred_element_type=jnp.float32), grad_kernel, grad_shift, grad_gate, jnp.dot(mixed.T, cot_block, preferred_element_type=jnp.float32), grad_rates, grad_biases, grad_skips)
        totals = jax.tree.map(lambda left, right: left + right, totals, terms)
        return (totals, (output, grad_rows))
    start_totals = (jnp.zeros((D,), jnp.float32), jnp.zeros((D, E), jnp.float32), jnp.zeros((CONV, K), jnp.float32), jnp.zeros((CONV,), jnp.float32), jnp.zeros((DI,), jnp.float32), jnp.zeros((DI, D), jnp.float32), jnp.zeros((H,), jnp.float32), jnp.zeros((H,), jnp.float32), jnp.zeros((H,), jnp.float32))
    x_blocks = hidden_in.reshape(SHARDS, TOK_DEV, D)
    cot_blocks = grad_out.reshape(SHARDS, TOK_DEV, D)
    final, (outputs, grad_rows) = lax.scan(per_device, start_totals, (x_blocks, cot_blocks, lengths))
    return (outputs.reshape(TOKENS, D), grad_rows.reshape(TOKENS, D), final[0], final[1], final[2], final[3], final[4], final[5], final[6], final[7], final[8])
```

```python
import functools
import math

import jax
import jax.numpy as jnp
from jax import lax
from jax.experimental import pallas as pl
from jax.experimental.pallas import tpu as pltpu
from jax.sharding import PartitionSpec as P

EPS = 1e-05
F32 = jnp.float32
BF16 = jnp.bfloat16
EXACT = lax.Precision.HIGHEST
LANES = 128


def nn(a, b):
    return lax.dot_general(a, b, (((1,), (0,)), ((), ())), preferred_element_type=F32)


def nt(a, b):
    return lax.dot_general(a, b, (((1,), (1,)), ((), ())), preferred_element_type=F32)


def tn(a, b):
    return lax.dot_general(a, b, (((0,), (0,)), ((), ())), preferred_element_type=F32)


def iota(shape, dim):
    return lax.broadcasted_iota(jnp.int32, shape, dim)


def segments(pos, ends):
    total = jnp.zeros(pos.shape, jnp.int32)
    for end in ends:
        total = total + (pos >= end).astype(jnp.int32)
    return total


def block_ends(lens_ref, block, count):
    ends, total = [], 0
    for slot in range(count):
        total = total + lens_ref[block, slot]
        ends.append(total)
    return ends


def keep_masks(rows, ends, taps):
    pos = iota((rows, LANES), 0)
    seg = segments(pos, ends)
    keeps = []
    for off in range(1, taps):
        same = (segments(pos - off, ends) == seg) & (pos >= off)
        keeps.append(same.astype(F32))
    valid = (seg < len(ends)).astype(F32)
    return keeps, valid


def conv_tile(u, weights, bias, keeps, taps):
    pre = bias + u * weights[taps - 1 : taps, :]
    for off in range(1, taps):
        pre = pre + pltpu.roll(u, off, 0) * keeps[off - 1] * weights[taps - 1 - off : taps - off, :]
    return pre


def softplus(v):
    return jnp.maximum(v, 0.0) + jnp.log1p(jnp.exp(-jnp.abs(v)))


def split(a):
    hi = a.astype(BF16)
    return hi, (a - hi.astype(F32)).astype(BF16)


def three(product, a, b):
    ah, al = split(a)
    bh, bl = split(b)
    return product(ah, bh) + (product(ah, bl) + product(al, bh))


class Sizes:
    pass


def fwd_kernel(sz, lens_ref, x_ref, go_ref, wzx_ref, wtl_ref, wo_ref, gain_ref, cw_ref, cb_ref, gate_ref, head_ref, rank_ref,
               nrm_ref, pzx_ref, ptl_ref, y_ref, gm_ref, q_ref):
    b = pl.program_id(0)
    rows, cs, st = sz.rows, sz.cs, sz.state
    tiles = cs // LANES
    ends = block_ends(lens_ref, b, sz.seqs)
    xb = x_ref[0].astype(F32)
    mean = jnp.mean(xb * xb, axis=1, keepdims=True)
    nrm = (xb * lax.rsqrt(mean + EPS) * gain_ref[...]).astype(BF16)
    nrm_ref[0] = nrm
    pzx = nn(nrm, wzx_ref[...])
    ptl = nn(nrm, wtl_ref[...])
    gm = nt(go_ref[0], wo_ref[...])
    pzx_ref[0] = pzx
    ptl_ref[0] = ptl
    gm_ref[0] = gm
    keeps, valid = keep_masks(rows, ends, sz.taps)

    def act(u, at):
        w = cw_ref[:, at : at + LANES]
        return jax.nn.silu(conv_tile(u, w, cb_ref[:, at : at + LANES], keeps, sz.taps))

    bm = act(ptl[:, 0:st], cs)
    cm = act(ptl[:, st : 2 * st], cs + st)
    raw = pltpu.roll(ptl[:, 2 * st : 2 * st + LANES], rank_ref[0], 1)
    dt = softplus(raw + head_ref[0:1, :])
    rate = -jnp.exp(head_ref[1:2, :])
    tri = (iota((rows, rows), 0) >= iota((rows, rows), 1))
    log_decay = jnp.dot(tri.astype(F32), dt * rate, precision=EXACT, preferred_element_type=F32)
    log_t = log_decay.T
    same = (segments(iota((rows, rows), 0), ends) == segments(iota((rows, rows), 1), ends)) & tri
    drop = jnp.where(same, 0.0, -jnp.inf)
    inner = three(nt, cm, bm)
    low = iota((rows, LANES), 1) < sz.hd
    q1 = jnp.zeros((rows, LANES), F32)
    q2 = jnp.zeros((rows, LANES), F32)
    for j in range(tiles):
        at = j * LANES
        xa = act(pzx[:, cs + at : cs + at + LANES], at)
        dt2 = jnp.where(low, dt[:, 2 * j : 2 * j + 1], dt[:, 2 * j + 1 : 2 * j + 2])
        xd = xa * dt2
        parts = []
        for e in range(2):
            h = 2 * j + e
            spread = log_decay[:, h : h + 1] - log_t[h : h + 1, :]
            f = (jnp.exp(spread + drop) * inner).astype(BF16)
            mine = low if e == 0 else jnp.logical_not(low)
            parts.append(nn(f, jnp.where(mine, xd, 0.0).astype(BF16)))
        y = parts[0] + parts[1] + xa * gate_ref[1:2, at : at + LANES]
        y_ref[0, :, at : at + LANES] = y
        zt = pzx[:, at : at + LANES]
        gated = y * (zt * jax.nn.sigmoid(zt))
        q1 = q1 + gated * gated
        q2 = q2 + gated * gm[:, at : at + LANES] * gate_ref[0:1, at : at + LANES]
    q2 = q2 * valid
    lane = iota((rows, LANES), 1)
    stats = jnp.where(lane == 0, jnp.sum(q1, axis=1, keepdims=True), jnp.sum(q2, axis=1, keepdims=True)).T
    q_ref[0] = stats[0:8, :]


def bwd_kernel(sz, lens_ref, nrm_ref, x_ref, go_ref, pzx_ref, ptl_ref, y_ref, gm_ref, q_ref, wzx_ref, wtl_ref, wo_ref, cw_ref,
               cb_ref, gate_ref, head_ref, rank_ref, mix_ref, hid_ref, dp_ref, dt_ref, gn_ref, small_ref):
    b = pl.program_id(0)
    rows, cs, st, taps = sz.rows, sz.cs, sz.state, sz.taps
    tiles = cs // LANES
    ends = block_ends(lens_ref, b, sz.seqs)
    keeps, valid = keep_masks(rows, ends, taps)
    at_gate, at_conv, at_head, at_gain = sz.at_gate, sz.at_conv, sz.at_head, sz.at_gain

    @pl.when(b == 0)
    def _():
        small_ref[...] = jnp.zeros(small_ref.shape, F32)

    def colsum(v):
        return jnp.sum(v, axis=0, keepdims=True)

    def conv_pre(u, at):
        return conv_tile(u, cw_ref[:, at : at + LANES], cb_ref[:, at : at + LANES], keeps, taps)

    def silu_pair(v):
        s = jax.nn.sigmoid(v)
        return v * s, s * (1.0 + v * (1.0 - s))

    def conv_back(u, dact, dsilu, at):
        dpre = dact * dsilu
        tile = at // LANES
        row = at_conv + tile * 8 if tile < tiles else sz.at_bc + (tile - tiles) * 8
        back = dpre * cw_ref[taps - 1 : taps, at : at + LANES]
        small_ref[row + taps - 1 : row + taps, :] += colsum(dpre * u)
        small_ref[row + taps : row + taps + 1, :] += colsum(dpre)
        for off in range(1, taps):
            kept = dpre * keeps[off - 1]
            tap = taps - 1 - off
            small_ref[row + tap : row + tap + 1, :] += colsum(kept * pltpu.roll(u, off, 0))
            back = back + pltpu.roll(kept, rows - off, 0) * cw_ref[tap : tap + 1, at : at + LANES]
        return back

    ub, uc = ptl_ref[0, :, 0:st], ptl_ref[0, :, st : 2 * st]
    bm, bslope = silu_pair(conv_pre(ub, cs))
    cm, cslope = silu_pair(conv_pre(uc, cs + st))
    raw = pltpu.roll(ptl_ref[0, :, 2 * st : 2 * st + LANES], rank_ref[0], 1) + head_ref[0:1, :]
    dt = softplus(raw)
    rate = -jnp.exp(head_ref[1:2, :])
    tri = (iota((rows, rows), 0) >= iota((rows, rows), 1))
    log_decay = jnp.dot(tri.astype(F32), dt * rate, precision=EXACT, preferred_element_type=F32)
    log_t = log_decay.T
    upper = (iota((rows, rows), 1) >= iota((rows, rows), 0))
    same = (segments(iota((rows, rows), 0), ends) == segments(iota((rows, rows), 1), ends)) & upper
    drop = jnp.where(same, 0.0, -jnp.inf)
    inner_t = three(nt, bm, cm)
    low = iota((rows, LANES), 1) < sz.hd
    lane = iota((rows, LANES), 1)

    q1 = jnp.broadcast_to(q_ref[0, 0:1, :], (LANES, rows)).T
    q2 = jnp.broadcast_to(q_ref[0, 1:2, :], (LANES, rows)).T
    scale = lax.rsqrt(q1 / sz.di + EPS)
    pull = scale * scale * scale * q2 / sz.di

    dcb = jnp.zeros((rows, rows), F32)
    ddt = jnp.zeros((rows, LANES), F32)
    cols = jnp.zeros((rows, LANES), F32)
    rowsums = jnp.zeros((LANES, rows), F32)
    lane_row = iota((LANES, rows), 0)
    for j in range(tiles):
        at = j * LANES
        tile = slice(at, at + LANES)
        zt = pzx_ref[0, :, tile]
        y = y_ref[0, :, tile]
        gm = gm_ref[0, :, tile] * valid
        gate = gate_ref[0:1, tile]
        sz_, zslope = silu_pair(zt)
        gated = y * sz_
        unit = gated * scale
        mix_ref[0, :, tile] = (unit * gate * valid).astype(BF16)
        small_ref[at_gate + j : at_gate + j + 1, :] += colsum(gm * unit)
        dgated = scale * gm * gate - gated * pull
        dp_ref[0, :, tile] = (dgated * y * zslope).astype(BF16)
        dy = dgated * sz_
        ux = pzx_ref[0, :, cs + at : cs + at + LANES]
        xa, xslope = silu_pair(conv_pre(ux, at))
        small_ref[at_head + 3 + j : at_head + 4 + j, :] += colsum(dy * xa)
        dt2 = jnp.where(low, dt[:, 2 * j : 2 * j + 1], dt[:, 2 * j + 1 : 2 * j + 2])
        xd = xa * dt2
        dxd = []
        for e in range(2):
            h = 2 * j + e
            mine = low if e == 0 else jnp.logical_not(low)
            decay = jnp.exp(log_t[h : h + 1, :] - log_decay[:, h : h + 1] + drop)
            df = three(nt, jnp.where(mine, xd, 0.0), dy) * decay
            dcb = dcb + df
            p = df * inner_t
            cols = jnp.where(lane == h, jnp.sum(p, axis=1, keepdims=True), cols)
            rowsums = jnp.where(lane_row == h, colsum(p), rowsums)
            dxd.append(nn((decay * inner_t).astype(BF16), jnp.where(mine, dy, 0.0).astype(BF16)))
        dxd = dxd[0] + dxd[1]
        both = dxd * xa
        ddt = jnp.where(lane == 2 * j, jnp.sum(jnp.where(low, both, 0.0), axis=1, keepdims=True), ddt)
        ddt = jnp.where(lane == 2 * j + 1, jnp.sum(jnp.where(low, 0.0, both), axis=1, keepdims=True), ddt)
        dx = dxd * dt2 + dy * gate_ref[1:2, tile]
        dp_ref[0, :, cs + at : cs + at + LANES] = conv_back(ux, dx, xslope, at).astype(BF16)

    ga = jnp.dot(upper.astype(F32), rowsums.T - cols, precision=EXACT, preferred_element_type=F32)
    ddt = ddt + ga * rate
    small_ref[at_head : at_head + 1, :] += rate * colsum(ga * dt)
    draw = jnp.where(lane < sz.nh, ddt * jax.nn.sigmoid(raw), 0.0)
    small_ref[at_head + 1 : at_head + 2, :] += colsum(draw)
    dt_ref[0, :, 2 * st : 2 * st + LANES] = pltpu.roll(draw, rank_ref[1], 1).astype(BF16)
    dcb = dcb.astype(BF16)
    db = nn(dcb, cm.astype(BF16))
    dc = tn(dcb, bm.astype(BF16))
    dt_ref[0, :, 0:st] = conv_back(ub, db, bslope, cs).astype(BF16)
    dt_ref[0, :, st : 2 * st] = conv_back(uc, dc, cslope, cs + st).astype(BF16)

    hid_ref[0] = nn(mix_ref[0], wo_ref[...]).astype(BF16)
    gn = nt(dp_ref[0], wzx_ref[...]) + nt(dt_ref[0], wtl_ref[...])
    gn_ref[0] = gn.astype(BF16)
    xb = x_ref[0].astype(F32)
    xhat = xb * lax.rsqrt(jnp.mean(xb * xb, axis=1, keepdims=True) + EPS)
    sums = colsum(gn * xhat)
    for k in range(sz.d // LANES):
        small_ref[at_gain + k : at_gain + k + 1, :] += sums[:, k * LANES : (k + 1) * LANES]


def up8(count):
    return -(-count // 8) * 8


def small_layout(sz):
    tiles = sz.cs // LANES
    sz.at_gain = 0
    sz.at_bc = up8(sz.d // LANES)
    sz.common = sz.at_bc + 2 * sz.state // LANES * 8
    sz.at_conv = sz.common
    sz.at_gate = sz.at_conv + tiles * 8
    sz.at_head = sz.at_gate + up8(tiles)
    sz.small_rows = sz.at_head + up8(3 + tiles)


def run_fwd(sz, lens, ranks, x_all, go_all, wzx, wtl, wo, gain, cw, cb, gate, head):
    t, rows, d, cs, tl = sz.t, sz.rows, sz.d, sz.cs, sz.tl
    whole = lambda a: pl.BlockSpec(a.shape, lambda b, *_: (0,) * a.ndim)
    block = lambda width: pl.BlockSpec((1, rows, width), lambda b, *_: (b, 0, 0))
    smem = pl.BlockSpec(memory_space=pltpu.SMEM)
    kernel = functools.partial(fwd_kernel, sz)
    return pl.pallas_call(
        kernel,
        grid=(t,),
        in_specs=[smem, block(d), block(d), whole(wzx), whole(wtl), whole(wo), whole(gain), whole(cw), whole(cb), whole(gate), whole(head), smem],
        out_specs=[block(d), block(2 * cs), block(tl), block(cs), block(cs), pl.BlockSpec((1, 8, rows), lambda b: (b, 0, 0))],
        out_shape=[
            jax.ShapeDtypeStruct((t, rows, d), BF16),
            jax.ShapeDtypeStruct((t, rows, 2 * cs), F32),
            jax.ShapeDtypeStruct((t, rows, tl), F32),
            jax.ShapeDtypeStruct((t, rows, cs), F32),
            jax.ShapeDtypeStruct((t, rows, cs), F32),
            jax.ShapeDtypeStruct((t, 8, rows), F32),
        ],
        compiler_params=pltpu.CompilerParams(vmem_limit_bytes=60 << 20),
        name="fwd",
    )(lens, x_all, go_all, wzx, wtl, wo, gain, cw, cb, gate, head, ranks)


def run_bwd(sz, lens, ranks, nrm, x_all, go_all, pzx, ptl, y, gm, q, wzx, wtl, wo, cw, cb, gate, head):
    t, rows, d, cs, tl = sz.t, sz.rows, sz.d, sz.cs, sz.tl
    whole = lambda a: pl.BlockSpec(a.shape, lambda b, *_: (0,) * a.ndim)
    block = lambda width: pl.BlockSpec((1, rows, width), lambda b, *_: (b, 0, 0))
    smem = pl.BlockSpec(memory_space=pltpu.SMEM)
    kernel = functools.partial(bwd_kernel, sz)
    return pl.pallas_call(
        kernel,
        grid=(t,),
        in_specs=[smem, block(d), block(d), block(d), block(2 * cs), block(tl), block(cs), block(cs), pl.BlockSpec((1, 8, rows), lambda b: (b, 0, 0)),
                  whole(wzx), whole(wtl), whole(wo), whole(cw), whole(cb), whole(gate), whole(head), smem],
        out_specs=[block(cs), block(d), block(2 * cs), block(tl), block(d), pl.BlockSpec((sz.small_rows, LANES), lambda b: (0, 0))],
        out_shape=[
            jax.ShapeDtypeStruct((t, rows, cs), BF16),
            jax.ShapeDtypeStruct((t, rows, d), BF16),
            jax.ShapeDtypeStruct((t, rows, 2 * cs), BF16),
            jax.ShapeDtypeStruct((t, rows, tl), BF16),
            jax.ShapeDtypeStruct((t, rows, d), BF16),
            jax.ShapeDtypeStruct((sz.small_rows, LANES), F32),
        ],
        compiler_params=pltpu.CompilerParams(vmem_limit_bytes=60 << 20),
        name="bwd",
    )(lens, nrm, x_all, go_all, pzx, ptl, y, gm, q, wzx, wtl, wo, cw, cb, gate, head, ranks)


def device_of(sz, g, t):
    return (lax.div(g, sz.z) * sz.fi + lax.div(t, 2), lax.rem(g, sz.z) * 2 + lax.rem(t, 2))


def index_of(sz, g, t):
    f, p = device_of(sz, g, t)
    return f * sz.p + p


class Place:
    def __init__(self, sz):
        f, p = lax.axis_index("fsdp"), lax.axis_index("dp")
        fi, z = lax.rem(f, sz.fi), lax.div(p, 2)
        self.c = lax.rem(p, 2)
        self.g = lax.div(f, sz.fi) * sz.z + z
        self.t = fi * 2 + self.c
        self.i = f * sz.p + p
        u, v = lax.rem(fi, 2), lax.div(fi, 2)
        across, along = v * 2 + 1 - u, (1 - v) * 2 + u
        self.fi = fi
        self.fa = across * (1 - self.c) + along * self.c
        self.fb = along * (1 - self.c) + across * self.c
        self.fd = sz.fi - 1 - fi
        self.other = 1 - self.c


def remote(sz, src, dst, send, recv, g, t):
    return pltpu.make_async_remote_copy(
        src_ref=src, dst_ref=dst, send_sem=send, recv_sem=recv, device_id=device_of(sz, g, t), device_id_type=pl.DeviceIdType.MESH
    )


def landed(ref, sem):
    pltpu.make_async_copy(ref, ref, sem).wait()


def greet_all(sz, me):
    barrier = pltpu.get_barrier_semaphore()

    @pl.loop(1, sz.n)
    def _(step):
        there = lax.rem(me.i + step, sz.n)
        pl.semaphore_signal(barrier, inc=1, device_id=(lax.div(there, sz.p), lax.rem(there, sz.p)), device_id_type=pl.DeviceIdType.MESH)

    pl.semaphore_wait(barrier, sz.n - 1)


class PlaneGather:
    def __init__(self, sz, me, parts, own, view, send, recv):
        self.sz, self.me, self.parts, self.own, self.view, self.send, self.recv = sz, me, parts, own, view, send, recv
        m = me
        self.a, self.b, self.d = m.fa * 2 + m.c, m.fb * 2 + m.c, m.fd * 2 + m.c
        self.pair = m.fi * 2 + m.other

    def copy(self, kind, slot, part, target, own=False):
        src = self.own(part) if own else self.view(slot, part)
        return remote(self.sz, src, self.view(slot, part), self.send.at[kind, part], self.recv.at[slot, part], self.me.g, target)

    def copies(self, part):
        m = self.me
        yield self.copy(0, m.t, part, self.a, True)
        yield self.copy(1, m.t, part, self.b, True)
        yield self.copy(2, m.t, part, self.pair, True)
        yield self.copy(3, self.a, part, self.b)
        yield self.copy(4, self.a, part, self.pair)
        yield self.copy(5, self.b, part, self.pair)
        yield self.copy(6, self.d, part, self.pair)

    def arrived(self, slot, part):
        landed(self.view(slot, part), self.recv.at[slot, part])

    def start(self):
        for part in range(self.parts):
            for copy in list(self.copies(part))[:3]:
                copy.start()

    def relay(self):
        for part in range(self.parts):
            _, _, _, on, first, second, _ = self.copies(part)
            self.arrived(self.a, part)
            on.start()
            first.start()
            self.arrived(self.b, part)
            second.start()

    def relay_far(self):
        for part in range(self.parts):
            self.arrived(self.d, part)
            list(self.copies(part))[6].start()

    def finish(self):
        for part in range(self.parts):
            for fi in (self.me.fi, self.me.fa, self.me.fb, self.me.fd):
                self.arrived(fi * 2 + self.me.other, part)
            for copy in self.copies(part):
                copy.wait_send()


def gather_kernel(sz, x, go, win, tail, wout, sm, X, GO, WZX, WTL, WO, SM, vx, vg, vw, vt, vo, vs, xsend, xrecv, gsend, grecv, wsend, wrecv,
                  asend, arecv, zsend, zrecv, tsend, trecv, osend, orecv, ssend, srecv, lsem):
    me = Place(sz)
    cs, rows, G, T = sz.cs, sz.rows, sz.g, sz.t
    greet_all(sz, me)

    @pl.loop(1, sz.n)
    def _(step):
        there = lax.rem(me.i + step, sz.n)
        pltpu.make_async_remote_copy(
            src_ref=sm, dst_ref=SM.at[me.i], send_sem=ssend.at[0], recv_sem=srecv.at[0],
            device_id=(lax.div(there, sz.p), lax.rem(there, sz.p)), device_id_type=pl.DeviceIdType.MESH,
        ).start()

    def slices(t):
        return [
            (win.at[:, pl.ds(pl.multiple_of(half * sz.di + t * cs, LANES), cs)], half) for half in range(2)
        ]

    def exchange(step):
        there = lax.rem(me.t + step, T)
        return [
            remote(sz, src, WZX.at[me.i, :, pl.ds(half * cs, cs)], asend.at[step, half], arecv.at[me.t, half], me.g, there)
            for src, half in slices(there)
        ]

    for step in range(1, T):
        for copy in exchange(step):
            copy.start()

    def tail_copy(step):
        there = lax.rem(me.g + step, G)
        return remote(sz, tail, WTL.at[me.i], tsend.at[step], trecv.at[me.g], there, me.t)

    for step in range(1, G):
        tail_copy(step).start()

    owner_t, piece = lax.div(me.i, G), lax.rem(me.i, G)

    def out_copy(g):
        return remote(sz, wout, WO.at[piece], osend.at[g], orecv.at[piece], g, owner_t)

    def is_self(g):
        return (owner_t == me.t) & (me.g == g)

    for g in range(G):
        @pl.when(jnp.logical_not(is_self(g)))
        def _(g=g):
            out_copy(g).start()

    gx = PlaneGather(sz, me, sz.parts, lambda k: x.at[pl.ds(k * sz.part_rows, sz.part_rows)],
                     lambda s, k: X.at[s, pl.ds(k * sz.part_rows, sz.part_rows)], xsend, xrecv)
    gg = PlaneGather(sz, me, sz.parts, lambda k: go.at[pl.ds(k * sz.part_rows, sz.part_rows)],
                     lambda s, k: GO.at[s, pl.ds(k * sz.part_rows, sz.part_rows)], gsend, grecv)
    gt = PlaneGather(sz, me, G, lambda k: WTL.at[index_of(sz, k, me.t)], lambda s, k: WTL.at[index_of(sz, k, s)], wsend, wrecv)
    gx.start()

    mine = slices(me.t)
    ins = [
        pltpu.make_async_copy(mine[0][0], vw.at[:, 0:cs], lsem.at[0]),
        pltpu.make_async_copy(mine[1][0], vw.at[:, cs:], lsem.at[1]),
        pltpu.make_async_copy(tail, vt, lsem.at[2]),
        pltpu.make_async_copy(sm, vs, lsem.at[3]),
        pltpu.make_async_copy(x, vx, lsem.at[4]),
        pltpu.make_async_copy(go, vg, lsem.at[5]),
    ]
    for copy in ins:
        copy.start()
    for copy in ins:
        copy.wait()
    outs = [
        pltpu.make_async_copy(vw, WZX.at[me.i], lsem.at[0]),
        pltpu.make_async_copy(vt, WTL.at[me.i], lsem.at[1]),
        pltpu.make_async_copy(vs, SM.at[me.i], lsem.at[2]),
        pltpu.make_async_copy(vx, X.at[me.t], lsem.at[3]),
        pltpu.make_async_copy(vg, GO.at[me.t], lsem.at[4]),
    ]
    for copy in outs:
        copy.start()
    for copy in outs:
        copy.wait()

    @pl.when(owner_t == me.t)
    def _():
        copy = pltpu.make_async_copy(wout, vo, lsem.at[6])
        copy.start()
        copy.wait()
        copy = pltpu.make_async_copy(vo, WO.at[piece], lsem.at[6])
        copy.start()
        copy.wait()

    for step in range(1, G):
        there = lax.rem(me.g + step, G)
        landed(WTL.at[index_of(sz, there, me.t)], trecv.at[there])
    gt.start()
    for step in range(1, T):
        there = lax.rem(me.t + step, T)
        for half in range(2):
            landed(WZX.at[index_of(sz, me.g, there), :, pl.ds(half * cs, cs)], arecv.at[there, half])

    def line(step, fi, up):
        plane = me.g - step if up else me.g + step
        have = (plane >= 0) if up else (plane < G)
        more = (me.g < G - 1) if up else (me.g > 0)
        plane = jnp.clip(plane, 0, G - 1)
        block = WZX.at[pl.ds(index_of(sz, plane, jnp.int32(2 * fi)), 2)]
        nxt = jnp.clip(me.g + 1 if up else me.g - 1, 0, G - 1)
        copy = remote(sz, block, block, zsend.at[int(up), plane, fi], zrecv.at[plane, fi], nxt, me.t)
        return have, more, block, copy, plane

    def advance(step):
        for fi in range(sz.fi):
            for up in (True, False):
                have, more, block, copy, plane = line(step, fi, up)
                if step > 0:
                    @pl.when(have)
                    def _(block=block, plane=plane, fi=fi):
                        landed(block, zrecv.at[plane, fi])
                if step < G - 1:
                    @pl.when(have & more)
                    def _(copy=copy):
                        copy.start()

    advance(0)
    gx.relay()
    gg.start()
    gt.relay()
    advance(1)
    gx.relay_far()
    gt.relay_far()
    gg.relay()
    for step in range(2, G):
        advance(step)
    gg.relay_far()
    gx.finish()
    gt.finish()
    gg.finish()
    for k in range(G):
        @pl.when(t_differs(sz, me, k))
        def _(k=k):
            landed(WO.at[k], orecv.at[k])
    for g in range(G):
        @pl.when(jnp.logical_not(is_self(g)))
        def _(g=g):
            out_copy(g).wait_send()
    for step in range(1, T):
        for copy in exchange(step):
            copy.wait_send()
    for step in range(1, G):
        tail_copy(step).wait_send()
    for step in range(G - 1):
        for fi in range(sz.fi):
            for up in (True, False):
                have, more, _, copy, _ = line(step, fi, up)

                @pl.when(have & more)
                def _(copy=copy):
                    copy.wait_send()
    landed(SM.at[pl.ds(0, sz.n - 1)], srecv.at[0])
    landed(SM.at[pl.ds(0, sz.n - 1)], ssend.at[0])


def t_differs(sz, me, k):
    return me.t * sz.g + k != me.i


def run_gather(sz, x, go, win, tail, wout, sm):
    n, g, t, rows, d, cs, tl, parts = sz.n, sz.g, sz.t, sz.rows, sz.d, sz.cs, sz.tl, sz.parts
    dn, on = win.shape[0], wout.shape[0]
    any_ = pl.BlockSpec(memory_space=pl.ANY)
    dma = pltpu.SemaphoreType.DMA
    return pl.pallas_call(
        functools.partial(gather_kernel, sz),
        in_specs=[any_] * 6,
        out_specs=[any_] * 6,
        out_shape=[
            jax.ShapeDtypeStruct((t, rows, d), BF16),
            jax.ShapeDtypeStruct((t, rows, d), BF16),
            jax.ShapeDtypeStruct((n, dn, 2 * cs), BF16),
            jax.ShapeDtypeStruct((n, dn, tl), BF16),
            jax.ShapeDtypeStruct((g, on, d), BF16),
            jax.ShapeDtypeStruct((n,) + sm.shape, F32),
        ],
        scratch_shapes=[
            pltpu.VMEM((rows, d), BF16), pltpu.VMEM((rows, d), BF16), pltpu.VMEM((dn, 2 * cs), BF16), pltpu.VMEM((dn, tl), BF16),
            pltpu.VMEM((on, d), BF16), pltpu.VMEM(sm.shape, F32),
            dma((7, parts)), dma((t, parts)), dma((7, parts)), dma((t, parts)), dma((7, g)), dma((t, g)),
            dma((t, 2)), dma((t, 2)), dma((2, g, sz.fi)), dma((g, sz.fi)), dma((g,)), dma((g,)), dma((g,)), dma((g,)), dma((1,)), dma((1,)), dma((8,)),
        ],
        compiler_params=pltpu.CompilerParams(collective_id=0, has_side_effects=True),
        name="gather",
    )(x, go, win, tail, wout, sm)


def stats_kernel(sz, q, out, held, send, recv):
    me = Place(sz)
    barrier = pltpu.get_barrier_semaphore()
    for step in range(1, sz.t):
        f, p = device_of(sz, me.g, lax.rem(me.t + step, sz.t))
        pl.semaphore_signal(barrier, inc=1, device_id=(f, p), device_id_type=pl.DeviceIdType.MESH)
    pl.semaphore_wait(barrier, sz.t - 1)

    def copy(step):
        return remote(sz, q, held.at[me.t], send.at[step], recv.at[me.t], me.g, lax.rem(me.t + step, sz.t))

    for step in range(1, sz.t):
        copy(step).start()
    total = q[...]
    for step in range(1, sz.t):
        there = lax.rem(me.t + step, sz.t)
        landed(held.at[there], recv.at[there])
        total = total + held[there]
    out[...] = total
    for step in range(1, sz.t):
        copy(step).wait_send()


def run_stats(sz, q):
    vmem = pl.BlockSpec(memory_space=pltpu.VMEM)
    dma = pltpu.SemaphoreType.DMA
    return pl.pallas_call(
        functools.partial(stats_kernel, sz),
        in_specs=[vmem],
        out_specs=vmem,
        out_shape=jax.ShapeDtypeStruct(q.shape, F32),
        scratch_shapes=[pltpu.VMEM((sz.t,) + q.shape, F32), dma((sz.t,)), dma((sz.t,))],
        compiler_params=pltpu.CompilerParams(collective_id=1, has_side_effects=True),
        name="stats",
    )(q)


def reduce_kernel(sz, hp, gp, dwzx, dwtl, dwo, sm, hsum, gsum, gin, gtl, gout, gsm, hs, gs, r0h, r0g, r1h, r1g, r2h, r2g, rz, sz_, ro, rt, st, rtz, ra,
                  rs1, s1, rs2, p0send, p0recv, p1send, p1recv, p2send, p2recv, zsend, zrecv, asend, arecv, osend, orecv, tsend, trecv, uzsend, uzrecv,
                  s1send, s1recv, s2send, s2recv, usend, urecv):
    me = Place(sz)
    cs, rows, G, T, FI = sz.cs, sz.rows, sz.g, sz.t, sz.fi
    parts, pr = sz.rparts, sz.rows // sz.rparts
    greet_all(sz, me)

    def up32(v):
        return v.astype(F32)

    def s1_copy(step):
        return remote(sz, sm, rs1.at[me.g], s1send.at[step], s1recv.at[me.g], lax.rem(me.g + step, G), me.t)

    for step in range(1, G):
        s1_copy(step).start()

    arrays = [(hp, hs, r0h, r1h, r2h, hsum), (gp, gs, r0g, r1g, r2g, gsum)]
    order = (me.fa, me.fd, me.fb, me.fi)

    def p0_copy(k, which, part):
        src, _, r0 = arrays[k][:3]
        fi = order[which]
        rows_ = pl.ds(part * pr, pr)
        return remote(sz, src.at[fi * 2 + me.other, rows_], r0.at[fi, rows_], p0send.at[k, which, part], p0recv.at[k, fi, part], me.g, me.fi * 2 + me.other)

    for k in range(2):
        for which in range(4):
            for part in range(parts):
                p0_copy(k, which, part).start()

    def t_copy(step, g):
        there = lax.rem(me.t + step, T)
        return remote(sz, dwtl.at[index_of(sz, g, there)], rt.at[me.t, g], tsend.at[step, g], trecv.at[me.t, g], me.g, there)

    for step in range(1, T):
        for g in range(G):
            t_copy(step, g).start()

    def z_copy(step, fi):
        there = lax.rem(me.g + step, G)
        return remote(sz, dwzx.at[pl.ds(index_of(sz, there, jnp.int32(2 * fi)), 2)], rz.at[me.g, pl.ds(2 * fi, 2)], zsend.at[step, fi], zrecv.at[me.g, fi],
                      there, me.t)

    for step in range(1, G):
        for fi in range(FI):
            z_copy(step, fi).start()

    def o_copy(k):
        owner = me.t * G + k
        f, p = lax.div(owner, sz.p), lax.rem(owner, sz.p)
        return pltpu.make_async_remote_copy(src_ref=dwo.at[k], dst_ref=ro.at[me.g], send_sem=osend.at[k], recv_sem=orecv.at[me.g],
                                            device_id=(f, p), device_id_type=pl.DeviceIdType.MESH)

    for k in range(G):
        @pl.when(t_differs(sz, me, k))
        def _(k=k):
            o_copy(k).start()

    def p1_copy(k, which, part):
        _, s, _, r1 = arrays[k][:4]
        rows_ = pl.ds(part * pr, pr)
        return remote(sz, s.at[which, rows_], r1.at[which, rows_], p1send.at[k, which, part], p1recv.at[k, which, part], me.g, me.fa * 2 + me.c)

    def p2_copy(k, part):
        _, s, _, _, r2 = arrays[k][:5]
        rows_ = pl.ds(part * pr, pr)
        return remote(sz, s.at[2, rows_], r2.at[rows_], p2send.at[k, part], p2recv.at[k, part], me.g, me.fb * 2 + me.c)

    for k in range(2):
        src, s, r0, r1, r2, out = arrays[k]
        for which in range(4):
            fi = order[which]
            for part in range(parts):
                rows_ = pl.ds(part * pr, pr)
                landed(r0.at[fi, rows_], p0recv.at[k, fi, part])
                both = up32(src[fi * 2 + me.c, rows_]) + up32(r0[fi, rows_])
                if which < 2:
                    s[which, rows_] = both.astype(BF16)
                    p1_copy(k, which, part).start()
                elif which == 2:
                    s[2, rows_] = both.astype(BF16)
                else:
                    out[rows_] = both

    for step in range(1, T):
        for g in range(G):
            there = lax.rem(me.t + step, T)
            landed(rt.at[there, g], trecv.at[there, g])
    for g in range(G):
        total = up32(dwtl[index_of(sz, g, me.t)])
        for step in range(1, T):
            total = total + up32(rt[lax.rem(me.t + step, T), g])
        st[g] = total.astype(BF16)

    def uz_copy(step):
        there = lax.rem(me.g + step, G)
        return remote(sz, st.at[there], rtz.at[me.g], uzsend.at[step], uzrecv.at[me.g], there, me.t)

    for step in range(1, G):
        uz_copy(step).start()

    total = sm[...]
    for step in range(1, G):
        there = lax.rem(me.g + step, G)
        landed(rs1.at[there], s1recv.at[there])
        total = total + rs1[there]
    s1[...] = total
    rs2[me.t] = total

    def s2_copy(step):
        return remote(sz, s1, rs2.at[me.t], s2send.at[step], s2recv.at[me.t], me.g, lax.rem(me.t + step, T))

    for step in range(1, T):
        s2_copy(step).start()

    for k in range(2):
        src, s, r0, r1, r2, out = arrays[k]
        for part in range(parts):
            rows_ = pl.ds(part * pr, pr)
            landed(r1.at[1, rows_], p1recv.at[k, 1, part])
            s[2, rows_] = (up32(s[2, rows_]) + up32(r1[1, rows_])).astype(BF16)
            p2_copy(k, part).start()

    for fi in range(FI):
        for step in range(1, G):
            there = lax.rem(me.g + step, G)
            landed(rz.at[there, pl.ds(2 * fi, 2)], zrecv.at[there, fi])
        for c in range(2):
            total = up32(dwzx[index_of(sz, me.g, jnp.int32(2 * fi + c))])
            for step in range(1, G):
                total = total + up32(rz[lax.rem(me.g + step, G), 2 * fi + c])
            sz_[2 * fi + c] = total.astype(BF16)

    def a_copy(step):
        there = lax.rem(me.t + step, T)
        return remote(sz, sz_.at[there], ra.at[me.t], asend.at[step], arecv.at[me.t], me.g, there)

    for step in range(1, T):
        a_copy(step).start()
    ra[me.t] = sz_[me.t]

    total = jnp.zeros(gout.shape, F32)
    mine = lax.div(me.i, G) == me.t

    @pl.when(mine)
    def _():
        gout[...] = up32(dwo[lax.rem(me.i, G)])

    @pl.when(jnp.logical_not(mine))
    def _():
        gout[...] = jnp.zeros(gout.shape, F32)

    for g in range(G):
        other = jnp.logical_not(mine & (me.g == g))

        @pl.when(other)
        def _(g=g):
            landed(ro.at[g], orecv.at[g])
            gout[...] += up32(ro[g])

    total = up32(st[me.g])
    for step in range(1, G):
        there = lax.rem(me.g + step, G)
        landed(rtz.at[there], uzrecv.at[there])
        total = total + up32(rtz[there])
    gtl[...] = total

    for k in range(2):
        src, s, r0, r1, r2, out = arrays[k]
        for part in range(parts):
            rows_ = pl.ds(part * pr, pr)
            landed(r1.at[0, rows_], p1recv.at[k, 0, part])
            landed(r2.at[rows_], p2recv.at[k, part])
            out[rows_] = out[rows_] + up32(r1[0, rows_]) + up32(r2[rows_])

    for step in range(1, T):
        there = lax.rem(me.t + step, T)
        landed(ra.at[there], arecv.at[there])
        landed(rs2.at[there], s2recv.at[there])
    for t in range(T):
        gin[:, t * cs : (t + 1) * cs] = up32(ra[t, :, 0:cs])
        gin[:, sz.di + t * cs : sz.di + (t + 1) * cs] = up32(ra[t, :, cs:])
    total = rs2[0, 0 : sz.common]
    for t in range(1, T):
        total = total + rs2[t, 0 : sz.common]
    gsm[0 : sz.common] = total
    width = sz.small_rows - sz.common
    for t in range(T):
        gsm[sz.common + t * width : sz.common + (t + 1) * width] = rs2[t, sz.common :]

    for step in range(1, G):
        s1_copy(step).wait_send()
        uz_copy(step).wait_send()
        for fi in range(FI):
            z_copy(step, fi).wait_send()
    for step in range(1, T):
        s2_copy(step).wait_send()
        a_copy(step).wait_send()
        for g in range(G):
            t_copy(step, g).wait_send()
    for k in range(2):
        for part in range(parts):
            for which in range(4):
                p0_copy(k, which, part).wait_send()
            for which in range(2):
                p1_copy(k, which, part).wait_send()
            p2_copy(k, part).wait_send()
    for k in range(G):
        @pl.when(t_differs(sz, me, k))
        def _(k=k):
            o_copy(k).wait_send()


def run_reduce(sz, hp, gp, dwzx, dwtl, dwo, sm):
    n, g, t, rows, d, cs, tl, parts, fi = sz.n, sz.g, sz.t, sz.rows, sz.d, sz.cs, sz.tl, sz.rparts, sz.fi
    dn, on = dwzx.shape[1], dwo.shape[1]
    vmem = pl.BlockSpec(memory_space=pltpu.VMEM)
    dma = pltpu.SemaphoreType.DMA
    v = lambda *s: pltpu.VMEM(s, BF16)
    sr = sz.small_rows
    total_rows = sz.common + t * (sr - sz.common)
    return pl.pallas_call(
        functools.partial(reduce_kernel, sz),
        in_specs=[vmem] * 6,
        out_specs=[vmem] * 6,
        out_shape=[
            jax.ShapeDtypeStruct((rows, d), F32),
            jax.ShapeDtypeStruct((rows, d), F32),
            jax.ShapeDtypeStruct((dn, 2 * sz.di), F32),
            jax.ShapeDtypeStruct((dn, tl), F32),
            jax.ShapeDtypeStruct((on, d), F32),
            jax.ShapeDtypeStruct((total_rows, LANES), F32),
        ],
        scratch_shapes=[
            v(3, rows, d), v(3, rows, d), v(fi, rows, d), v(fi, rows, d), v(2, rows, d), v(2, rows, d), v(rows, d), v(rows, d),
            v(g, t, dn, 2 * cs), v(t, dn, 2 * cs), v(g, on, d), v(t, g, dn, tl), v(g, dn, tl), v(g, dn, tl), v(t, dn, 2 * cs),
            pltpu.VMEM((g, sr, LANES), F32), pltpu.VMEM((sr, LANES), F32), pltpu.VMEM((t, sr, LANES), F32),
            dma((2, 4, parts)), dma((2, fi, parts)), dma((2, 2, parts)), dma((2, 2, parts)), dma((2, parts)), dma((2, parts)),
            dma((g, fi)), dma((g, fi)), dma((t,)), dma((t,)), dma((g,)), dma((g,)), dma((t, g)), dma((t, g)), dma((g,)), dma((g,)),
            dma((g,)), dma((g,)), dma((t,)), dma((t,)), dma((1,)), dma((1,)),
        ],
        compiler_params=pltpu.CompilerParams(collective_id=2, has_side_effects=True, vmem_limit_bytes=63 << 20),
        name="reduce",
    )(hp, gp, dwzx, dwtl, dwo, sm)


def sizes(mesh, hidden, lengths, in_proj, conv_weight, gate_gain, decay_log):
    sz = Sizes()
    sz.f, sz.p = mesh.shape["fsdp"], mesh.shape["dp"]
    sz.n = sz.f * sz.p
    sz.rows, sz.d = hidden.shape
    sz.seqs = lengths.shape[1]
    sz.conv, sz.taps = conv_weight.shape[0] * sz.n, conv_weight.shape[1]
    sz.di = gate_gain.shape[0] * sz.n
    sz.state = (sz.conv - sz.di) // 2
    sz.heads = decay_log.shape[0]
    sz.hd = sz.di // sz.heads
    sz.fi = math.gcd(sz.f, sz.di // (2 * LANES))
    sz.t = 2 * sz.fi
    sz.z = sz.p // 2
    sz.g = sz.f // sz.fi * sz.z
    sz.cs, sz.nh = sz.di // sz.t, sz.heads // sz.t
    sz.tail = in_proj.shape[1] - 2 * sz.di
    sz.tl = -(-sz.tail // LANES) * LANES
    sz.parts, sz.rparts = 2, 2
    sz.part_rows = sz.rows // sz.parts
    small_layout(sz)
    return sz


def widen(a, rows, lanes):
    return jnp.pad(a, ((0, rows - a.shape[0]), (0, lanes - a.shape[1])))


def local(mesh, hidden_in, lengths, norm_gain, in_proj, conv_weight, conv_bias, gate_gain, out_proj, decay_log, step_bias, skip_gain, grad_out):
    sz = sizes(mesh, hidden_in, lengths, in_proj, conv_weight, gate_gain, decay_log)
    n, t, cs, di = sz.n, sz.t, sz.cs, sz.di
    f, p = lax.axis_index("fsdp"), lax.axis_index("dp")
    fo, fi, z, c = f // sz.fi, f % sz.fi, p // 2, p % 2
    rank, index = fi * 2 + c, f * sz.p + p
    dn, cn, kn = norm_gain.shape[0], conv_bias.shape[0], gate_gain.shape[0]

    small = [norm_gain, conv_weight.reshape(-1), conv_bias, gate_gain, lengths[0]]
    flat = jnp.concatenate([a.astype(F32) for a in small])
    lanes = -(-flat.shape[0] // (8 * LANES)) * 8 * LANES
    sm = jnp.pad(flat, (0, lanes - flat.shape[0])).reshape(-1, LANES)
    tail = jnp.pad(in_proj[:, 2 * di :], ((0, 0), (0, sz.tl - sz.tail)))
    x_all, go_all, wzx, wtl, wo, sm_all = run_gather(sz, hidden_in, grad_out, in_proj, tail, out_proj, sm)
    flat = sm_all.reshape(n, lanes)
    cuts = [0]
    for a in small:
        cuts.append(cuts[-1] + a.size)
    gain, cw, cb, gate, lens = (flat[:, lo:hi] for lo, hi in zip(cuts[:-1], cuts[1:]))
    gain = gain.reshape(1, sz.d)
    cw = cw.reshape(sz.conv, sz.taps)
    cb, gate = cb.reshape(-1), gate.reshape(-1)
    here = lambda a, width: lax.dynamic_slice_in_dim(a, rank * width, width)
    cw = widen(jnp.concatenate([here(cw, cs), cw[di:]]).T, 8, cs + 2 * sz.state)
    cb = jnp.concatenate([here(cb, cs), cb[di:]])[None]
    gate = widen(jnp.stack([here(gate, cs), jnp.repeat(here(skip_gain, sz.nh), sz.hd)]), 8, cs)
    head = widen(jnp.stack([here(step_bias, sz.nh), here(decay_log, sz.nh)]), 8, LANES)
    lens = lens.reshape(sz.f // sz.fi, sz.fi, sz.z, 2, sz.seqs)[fo, :, z].reshape(t, sz.seqs).astype(jnp.int32)
    ranks = jnp.stack([(LANES - sz.nh * rank) % LANES, sz.nh * rank]).astype(jnp.int32)
    wzx, wtl, wo = wzx.reshape(sz.d, 2 * cs), wtl.reshape(sz.d, sz.tl), wo.reshape(cs, sz.d)

    nrm, pzx, ptl, y, gm, q = run_fwd(sz, lens, ranks, x_all, go_all, wzx, wtl, wo, gain, cw, cb, gate, head)
    q = run_stats(sz, q)
    mix, hid, dzx, dtl, gn, small = run_bwd(sz, lens, ranks, nrm, x_all, go_all, pzx, ptl, y, gm, q, wzx, wtl, wo, cw, cb, gate, head)

    tall = lambda a: a.reshape(t * sz.rows, a.shape[2])
    dwzx = tn(tall(nrm), tall(dzx)).astype(BF16).reshape(n, dn, 2 * cs)
    dwtl = tn(tall(nrm), tall(dtl)).astype(BF16).reshape(n, dn, sz.tl)
    dwo = tn(tall(mix), tall(go_all)).astype(BF16).reshape(sz.g, cs // sz.g, sz.d)
    hsum, gsum, gin, gtl, gout, gsm = run_reduce(sz, hid, gn, dwzx, dwtl, dwo, small)

    x = hidden_in.astype(F32)
    hidden_out = (x + hsum).astype(BF16)
    scale = lax.rsqrt(jnp.mean(x * x, axis=1, keepdims=True) + EPS)
    dxhat = gsum * gain
    inner = jnp.mean(dxhat * x, axis=1, keepdims=True)
    grad_in = grad_out.astype(F32) + scale * (dxhat - x * (scale * scale * inner))
    grad_in_proj = jnp.concatenate([gin, gtl[:, : sz.tail]], axis=1)

    own = lambda a, width: lax.dynamic_slice_in_dim(a, index * width, width)
    common, slices = gsm[: sz.common], gsm[sz.common :].reshape(t, -1, LANES)
    at = lambda place: place - sz.common
    grad_norm_gain = own(common[: sz.d // LANES].reshape(-1), dn)
    conv_x = slices[:, : at(sz.at_gate)].reshape(-1, 8, LANES)
    conv = jnp.concatenate([conv_x, common[sz.at_bc :].reshape(-1, 8, LANES)])
    conv = conv[:, : sz.taps + 1].transpose(0, 2, 1).reshape(sz.conv, sz.taps + 1)
    conv = own(conv, cn)
    tiles = cs // LANES
    grad_gate = own(slices[:, at(sz.at_gate) : at(sz.at_gate) + tiles].reshape(-1), kn)
    heads = slices[:, at(sz.at_head) :]
    grad_decay = heads[:, 0, : sz.nh].reshape(-1)
    grad_bias = heads[:, 1, : sz.nh].reshape(-1)
    grad_skip = jnp.sum(heads[:, 3 : 3 + tiles].reshape(sz.heads, sz.hd), axis=1)
    return (hidden_out, grad_in, grad_norm_gain, grad_in_proj, conv[:, : sz.taps], conv[:, sz.taps], grad_gate, gout, grad_decay, grad_bias, grad_skip)


def solution(mesh):
    both = ("fsdp", "dp")
    wide, flat, free = P(both, None), P(both), P()
    in_specs = (wide, wide, flat, wide, wide, flat, flat, wide, free, free, free, wide)
    out_specs = (wide, wide, flat, wide, wide, flat, flat, wide, free, free, free)
    return jax.shard_map(functools.partial(local, mesh), mesh=mesh, in_specs=in_specs, out_specs=out_specs, check_vma=False)
```

```python
import functools
import math

import jax
import jax.numpy as jnp
from jax import lax
from jax.experimental import pallas as pl
from jax.experimental.pallas import tpu as pltpu
from jax.sharding import PartitionSpec as P

EPS = 1e-05
F32 = jnp.float32
BF16 = jnp.bfloat16
EXACT = lax.Precision.HIGHEST
LANES = 128


def nn(a, b):
    return lax.dot_general(a, b, (((1,), (0,)), ((), ())), preferred_element_type=F32)


def nt(a, b):
    return lax.dot_general(a, b, (((1,), (1,)), ((), ())), preferred_element_type=F32)


def tn(a, b):
    return lax.dot_general(a, b, (((0,), (0,)), ((), ())), preferred_element_type=F32)


def iota(shape, dim):
    return lax.broadcasted_iota(jnp.int32, shape, dim)


def conv_tile(u, weights, bias, keeps, taps):
    pre = bias + u * weights[taps - 1 : taps, :]
    for off in range(1, taps):
        pre = pre + pltpu.roll(u, off, 0) * keeps[off - 1] * weights[taps - 1 - off : taps - off, :]
    return pre


def softplus(v):
    return jnp.maximum(v, 0.0) + jnp.log1p(jnp.exp(-jnp.abs(v)))


def split(a):
    hi = a.astype(BF16)
    return hi, (a - hi.astype(F32)).astype(BF16)


def three(product, a, b):
    ah, al = split(a)
    bh, bl = split(b)
    return product(ah, bh) + (product(ah, bl) + product(al, bh))


class Sizes:
    pass


def up8(count):
    return -(-count // 8) * 8


def small_layout(sz):
    tiles = sz.cs // LANES
    sz.at_gain = 0
    sz.at_bc = up8(sz.d // LANES)
    sz.common = sz.at_bc + 2 * sz.state // LANES * 8
    sz.at_conv = sz.common
    sz.at_gate = sz.at_conv + tiles * 8
    sz.at_head = sz.at_gate + up8(tiles)
    sz.small_rows = sz.at_head + up8(3 + tiles)


def device_of(sz, g, t):
    return (lax.div(g, sz.z) * sz.fi + lax.div(t, 2), lax.rem(g, sz.z) * 2 + lax.rem(t, 2))


def index_of(sz, g, t):
    f, p = device_of(sz, g, t)
    return f * sz.p + p


class Place:
    def __init__(self, sz):
        f, p = lax.axis_index("fsdp"), lax.axis_index("dp")
        fi, z = lax.rem(f, sz.fi), lax.div(p, 2)
        self.c = lax.rem(p, 2)
        self.g = lax.div(f, sz.fi) * sz.z + z
        self.t = fi * 2 + self.c
        self.i = f * sz.p + p
        u, v = lax.rem(fi, 2), lax.div(fi, 2)
        across, along = v * 2 + 1 - u, (1 - v) * 2 + u
        self.fi = fi
        self.fa = across * (1 - self.c) + along * self.c
        self.fb = along * (1 - self.c) + across * self.c
        self.fd = sz.fi - 1 - fi
        self.other = 1 - self.c


def remote(sz, src, dst, send, recv, g, t):
    return pltpu.make_async_remote_copy(
        src_ref=src, dst_ref=dst, send_sem=send, recv_sem=recv, device_id=device_of(sz, g, t), device_id_type=pl.DeviceIdType.MESH
    )


def landed(ref, sem):
    pltpu.make_async_copy(ref, ref, sem).wait()


def greet_all(sz, me):
    barrier = pltpu.get_barrier_semaphore()

    @pl.loop(1, sz.n)
    def _(step):
        there = lax.rem(me.i + step, sz.n)
        pl.semaphore_signal(barrier, inc=1, device_id=(lax.div(there, sz.p), lax.rem(there, sz.p)), device_id_type=pl.DeviceIdType.MESH)

    pl.semaphore_wait(barrier, sz.n - 1)


def greet_near(sz, me):
    barrier = pltpu.get_barrier_semaphore()
    near = [(me.g, lax.rem(me.t + step, sz.t)) for step in range(1, sz.t)] + [(lax.rem(me.g + step, sz.g), me.t) for step in range(1, sz.g)]
    for g, t in near:
        pl.semaphore_signal(barrier, inc=1, device_id=device_of(sz, g, t), device_id_type=pl.DeviceIdType.MESH)
    pl.semaphore_wait(barrier, len(near))


class PlaneGather:
    def __init__(self, sz, me, parts, own, views, gauge, bulk, send, recv):
        self.sz, self.me, self.parts, self.own, self.views, self.gauge, self.bulk, self.send, self.recv = sz, me, parts, own, views, gauge, bulk, send, recv
        self.a, self.b, self.d = me.fa * 2 + me.c, me.fb * 2 + me.c, me.fd * 2 + me.c
        self.pair = me.fi * 2 + me.other

    def push(self, kind, part):
        slot = (self.me.t, self.me.t, self.me.t, self.a, self.a, self.b, self.d)[kind]
        target = (self.a, self.b, self.pair, self.b, self.pair, self.pair, self.pair)[kind]
        views = self.views(slot, part)
        for src, dst in zip(self.own(part) if kind < 3 else views, views):
            remote(self.sz, src, dst, self.send.at[0], self.recv.at[slot, part], self.me.g, target).start()

    def arrived(self, slot, part):
        landed(self.gauge, self.recv.at[slot, part])

    def start(self, part):
        for kind in range(3):
            self.push(kind, part)

    def relay(self, part):
        self.arrived(self.a, part)
        self.push(3, part)
        self.push(4, part)
        self.arrived(self.b, part)
        self.push(5, part)

    def relay_far(self, part):
        self.arrived(self.d, part)
        self.push(6, part)

    def sent(self):
        landed(self.bulk, self.send.at[0])


def t_differs(sz, me, k):
    return me.t * sz.g + k != me.i


def select_rows(sz, packed, channel, per):
    n = packed.shape[0]
    wide = channel.shape[1]
    owner = jnp.floor((channel + 0.5) * (1.0 / per))
    place = channel - owner * per
    pick = (iota((LANES, wide), 0).astype(F32) == place).astype(BF16)
    spread = nn(packed.reshape(n * 8, LANES).astype(BF16), pick).reshape(n, 8, wide)
    over = lambda v, by: jnp.floor((v + 0.5) * (1.0 / by))
    spot = iota((n, 8, LANES), 0).astype(F32)
    rank = over(spot, sz.g)
    plane = spot - sz.g * rank
    fi, fo = over(rank, 2), over(plane, sz.z)
    device = ((fo * sz.fi + fi) * sz.z + plane - sz.z * fo) * 2 + rank - 2 * fi
    total = jnp.zeros((8, wide), F32)
    parts = []
    for at in range(0, wide, LANES):
        hit = device == owner[None, :, at : at + LANES]
        parts.append(jnp.sum(jnp.where(hit, spread[:, :, at : at + LANES], 0.0), axis=0))
    return jnp.concatenate(parts, axis=1)


def lanes_of(wide):
    return iota((1, wide), 1).astype(F32)


def slot_of(me, k):
    flip = lambda bit, other: bit + other - 2 * bit * other
    v, u, c = lax.div(me.t, 4), lax.rem(lax.div(me.t, 2), 2), me.c
    kv, ku, kc = lax.div(k, 4), lax.rem(lax.div(k, 2), 2), lax.rem(k, 2)
    return (flip(v, kv) * 2 + flip(u, ku)) * 2 + flip(c, kc)


def ends_of(row, count):
    ends, total = [], jnp.zeros((1, 1), F32)
    for slot in range(count):
        total = total + row[:, slot : slot + 1]
        ends.append(total)
    return ends


def segments(pos, ends):
    total = jnp.zeros(pos.shape, F32)
    for end in ends:
        total = total + (pos >= end).astype(F32)
    return total


def masks(rows, ends, taps):
    pos = iota((rows, LANES), 0).astype(F32)
    seg = segments(pos, ends)
    keeps = []
    for off in range(1, taps):
        same = (segments(pos - off, ends) == seg) & (pos >= off)
        keeps.append(same.astype(F32))
    valid = (seg < len(ends)).astype(F32)
    seg_row = segments(lanes_of(rows), ends)
    same = jnp.concatenate([(seg == seg_row[:, at : at + LANES]) for at in range(0, rows, LANES)], axis=1)
    return keeps, valid, same


def triangle(rows):
    return iota((rows, rows), 0) >= iota((rows, rows), 1)


def front_kernel(sz, x, go, win, tail, wout, norm, cw, cb, gate, lens, decay, bias, skip,
                 NRM, GO, PX, PT, PZ, Y, GM, WX, WZ, WT, WO, Q, PAR, HEAD, TILE,
                 xv, nv, gov, px, pt, pz, yv, gmv, wxv, wzv, wtv, wov, pack, smv, par, head, qv, qr, tilev,
                 xsend, xrecv, gsend, grecv, wsend, wrecv, axsend, axrecv, azsend, azrecv, zxsend, zxrecv, zzsend, zzrecv,
                 tsend, trecv, osend, orecv, ssend, srecv, qsend, qrecv, lsem, esem, wsem):
    me = Place(sz)
    cs, rows, G, T, st, taps = sz.cs, sz.rows, sz.g, sz.t, sz.state, sz.taps
    tiles = cs // LANES
    pack[...] = jnp.zeros(pack.shape, F32)
    dn, cn, kn = norm.shape[1], cb.shape[1], gate.shape[1]
    pack[0:taps, 0:cn] = cw[...].astype(F32)
    pack[taps : taps + 1, 0:cn] = cb[...].astype(F32)
    pack[taps + 1 : taps + 2, 0:kn] = gate[...].astype(F32)
    pack[taps + 2 : taps + 3, 0:dn] = norm[...].astype(F32)
    pack[taps + 3 : taps + 4, 0 : sz.seqs] = lens[...].astype(F32)
    (greet_near if sz.aligned else greet_all)(sz, me)

    tile_of = lambda g, t: smv.at[t * G + g]

    def pack_line(step):
        return remote(sz, pack, tile_of(me.g, me.t), ssend.at[0], srecv.at[0], lax.rem(me.g + step, G), me.t)

    def pack_plane(step):
        mine = smv.at[pl.ds(me.t * G, G)]
        return remote(sz, mine, mine, ssend.at[1], srecv.at[1], me.g, lax.rem(me.t + step, T))

    def columns(half, t):
        return win.at[:, pl.ds(pl.multiple_of(half * sz.di + t * cs, LANES), cs)]

    def exchange(half, step):
        there = lax.rem(me.t + step, T)
        wv, send, recv = ((wzv, azsend, azrecv), (wxv, axsend, axrecv))[half]
        return remote(sz, columns(half, there), wv.at[me.i], send.at[0], recv.at[0], me.g, there)

    def tail_copy(step):
        there = lax.rem(me.g + step, G)
        return remote(sz, tail, wtv.at[me.i], tsend.at[0], trecv.at[0], there, me.t)

    for step in range(1, G):
        tail_copy(step).start()
        pack_line(step).start()
    for step in range(1, T):
        exchange(1, step).start()

    part = lambda ref, k: ref.at[pl.ds(k * sz.part_rows, sz.part_rows)]
    gx = PlaneGather(sz, me, sz.parts, lambda k: [part(x, k)], lambda s, k: [part(xv.at[s], k)], part(xv.at[0], 0), xv.at[pl.ds(0, T - 1)], xsend, xrecv)
    gg = PlaneGather(sz, me, sz.parts, lambda k: [part(go, k)], lambda s, k: [part(gov.at[s], k)], part(gov.at[0], 0), gov.at[pl.ds(0, T - 1)], gsend, grecv)
    tails_of = lambda s, k: [wtv.at[index_of(sz, jnp.int32(g), s)] for g in range(G)]
    gt = PlaneGather(sz, me, 1, lambda k: tails_of(me.t, k), tails_of, wtv.at[pl.ds(0, G)], wtv.at[pl.ds(0, (T - 1) * G)], wsend, wrecv)

    owner_t, piece = lax.div(me.i, G), lax.rem(me.i, G)

    def out_copy(g):
        return remote(sz, wout, wov.at[piece], osend.at[2, g], orecv.at[piece], g, owner_t)

    def out_targets():
        planes = (me.g,) if sz.aligned else tuple(range(G))
        for g in planes:
            elsewhere = (owner_t != me.t) | (me.g != g)
            yield elsewhere, (lambda g=g: out_copy(jnp.int32(0) + g))

    def out_line(step, half, up):
        plane = me.g - step if up else me.g + step
        first = 2 * plane - me.c * sz.z
        have = (plane >= 0 if up else plane < G) & (first >= 0) & (first < G)
        more = (me.g < G - 1) if up else (me.g > 0)
        k = jnp.clip(first, 0, G - 2) + half
        nxt = jnp.clip(me.g + 1 if up else me.g - 1, 0, G - 1)
        copy = lambda: remote(sz, wov.at[k], wov.at[k], osend.at[int(up), k], orecv.at[k], nxt, me.t)
        return have, more, k, copy

    def out_advance(step):
        for half in range(2):
            if step == 0:
                have, _, k, _ = out_line(0, half, True)

                @pl.when(have & t_differs(sz, me, k))
                def _(k=k):
                    landed(wov.at[k], orecv.at[k])
            for up in (True, False):
                have, more, k, copy = out_line(step, half, up)
                if step > 0:
                    @pl.when(have)
                    def _(k=k):
                        landed(wov.at[k], orecv.at[k])
                if step < G - 1:
                    @pl.when(have & more)
                    def _(copy=copy):
                        copy().start()

    def out_steps(*steps):
        if sz.aligned:
            for step in steps:
                out_advance(step)

    for elsewhere, copy in out_targets():
        @pl.when(elsewhere)
        def _(copy=copy):
            copy().start()

    ins = [
        pltpu.make_async_copy(columns(1, me.t), wxv.at[me.i], lsem.at[0]),
        pltpu.make_async_copy(columns(0, me.t), wzv.at[me.i], lsem.at[1]),
        pltpu.make_async_copy(tail, wtv.at[me.i], lsem.at[2]),
        pltpu.make_async_copy(pack, tile_of(me.g, me.t), lsem.at[3]),
        pltpu.make_async_copy(x, xv.at[me.t], lsem.at[4]),
        pltpu.make_async_copy(go, gov.at[me.t], lsem.at[5]),
    ]
    for copy in ins:
        copy.start()
    for copy in ins:
        copy.wait()

    @pl.when(owner_t == me.t)
    def _():
        copy = pltpu.make_async_copy(wout, wov.at[piece], lsem.at[6])
        copy.start()
        copy.wait()

    head[...] = jnp.zeros(head.shape, F32)
    head[0:1, 0 : sz.heads] = bias[...]
    head[1:2, 0 : sz.heads] = decay[...]
    head[2:3, 0 : sz.heads] = skip[...]
    lead = lax.rem(LANES - sz.nh * me.t, LANES)
    head[...] = pltpu.roll(head[...], lead, 1)

    landed(smv.at[pl.ds(0, G - 1)], srecv.at[0])
    landed(wtv.at[pl.ds(0, G - 1)], trecv.at[0])
    for step in range(1, T):
        pack_plane(step).start()
    gt.start(0)
    gx.start(0)

    def arrive(half):
        wv, _, recv = ((wzv, azsend, azrecv), (wxv, axsend, axrecv))[half]
        landed(wv.at[pl.ds(0, T - 1)], recv.at[0])

    def line(half, step, up):
        wv, send, recv = ((wzv, zzsend, zzrecv), (wxv, zxsend, zxrecv))[half]
        plane = me.g - step if up else me.g + step
        have = (plane >= 0) if up else (plane < G)
        more = (me.g < G - 1) if up else (me.g > 0)
        plane = jnp.clip(plane, 0, G - 1)
        nxt = jnp.clip(me.g + 1 if up else me.g - 1, 0, G - 1)

        def push():
            for fi in range(sz.fi):
                block = wv.at[pl.ds(index_of(sz, plane, jnp.int32(2 * fi)), 2)]
                remote(sz, block, block, send.at[int(up), plane], recv.at[plane], nxt, me.t).start()

        return have, more, plane, push, wv.at[pl.ds(0, T)], send, recv

    def advance(half, step):
        for up in (True, False):
            have, more, plane, push, gauge, _, recv = line(half, step, up)
            if step > 0:
                @pl.when(have)
                def _(gauge=gauge, recv=recv, plane=plane):
                    landed(gauge, recv.at[plane])
            if step < G - 1:
                pl.when(have & more)(push)

    arrive(1)
    advance(1, 0)
    gt.relay(0)
    for step in range(1, T):
        exchange(0, step).start()
    for p in range(1, sz.parts):
        gx.start(p)
    advance(1, 1)
    landed(smv.at[pl.ds(0, (T - 1) * G)], srecv.at[1])
    packed = smv[...]
    ch = lanes_of(cs + 2 * st)
    start_ch = (me.t * cs).astype(F32)
    ch = jnp.where(ch < cs, ch + start_ch, ch + (sz.di - cs))
    par[:, 0 : cs + 2 * st] = select_rows(sz, packed, ch, cn)
    picked = select_rows(sz, packed, lanes_of(cs) + start_ch, kn)
    par[taps + 1 : taps + 2, 0:cs] = picked[taps + 1 : taps + 2]
    gains = select_rows(sz, packed, lanes_of(sz.d), dn)
    par[taps + 2 : taps + 3, 0 : sz.d] = gains[taps + 2 : taps + 3]

    def normalize(k):
        slot = slot_of(me, k)
        xb = xv[slot].astype(F32)
        mean = jnp.mean(xb * xb, axis=1, keepdims=True)
        nv[slot] = (xb * lax.rsqrt(mean + EPS) * par[taps + 2 : taps + 3, 0 : sz.d]).astype(BF16)
        pltpu.make_async_copy(nv.at[slot], NRM.at[slot], esem.at[0]).start()

    def wait_pair(gather, k):
        slot = slot_of(me, k)
        for p in range(sz.parts):
            gather.arrived(slot, p)

    normalize(jnp.int32(0))
    wait_pair(gx, jnp.int32(1))
    normalize(jnp.int32(1))
    gx.relay(0)
    for step in range(2, G - 1):
        advance(1, step)
    arrive(0)
    advance(0, 0)
    gt.relay_far(0)
    advance(1, G - 1)
    for p in range(1, sz.parts):
        gx.relay(p)
    for p in range(sz.parts):
        gg.start(p)
    for fi in (me.fi, me.fa, me.fb, me.fd):
        gt.arrived(fi * 2 + me.other, 0)

    low = iota((rows, LANES), 1) < sz.hd
    tri = triangle(rows)
    half_rows = rows // 2

    def scan(k):
        slot = slot_of(me, k)

        @pl.when((k > 2) & (lax.rem(k, 2) == 1))
        def _():
            wait_pair(gx, k)

        @pl.when(k > 1)
        def _():
            normalize(k)

        keeps, _, same = masks(rows, ends_of(smv[slot * G + me.g, taps + 3 : taps + 4, :], sz.seqs), taps)
        nrm = nv[slot]
        pxv = nn(nrm, wxv[...].reshape(sz.d, cs))
        ptl = nn(nrm, wtv[...].reshape(sz.d, sz.tl))
        px[slot] = pxv
        pt[slot] = ptl
        pltpu.make_async_copy(px.at[slot], PX.at[slot], esem.at[1]).start()
        pltpu.make_async_copy(pt.at[slot], PT.at[slot], esem.at[2]).start()

        def act(u, at):
            return jax.nn.silu(conv_tile(u, par[0:taps, at : at + LANES], par[taps : taps + 1, at : at + LANES], keeps, taps))

        bm = act(ptl[:, 0:st], cs)
        cm = act(ptl[:, st : 2 * st], cs + st)
        raw = pltpu.roll(ptl[:, 2 * st : 2 * st + LANES], lead, 1)
        dt = softplus(raw + head[0:1, :])
        rate = -jnp.exp(head[1:2, :])
        log_decay = jnp.dot(tri.astype(F32), dt * rate, precision=EXACT, preferred_element_type=F32)
        log_t = log_decay.T
        drop = jnp.where(same & tri, 0.0, -jnp.inf)
        inner = three(nt, cm, bm)
        for j in range(tiles):
            at = j * LANES
            xa = act(pxv[:, at : at + LANES], at)
            dt2 = jnp.where(low, dt[:, 2 * j : 2 * j + 1], dt[:, 2 * j + 1 : 2 * j + 2])
            xd = xa * dt2
            tops, bottoms = [], []
            for e in range(2):
                h = 2 * j + e
                mine = low if e == 0 else jnp.logical_not(low)
                xm = jnp.where(mine, xd, 0.0).astype(BF16)
                for r, wide, into in ((slice(0, half_rows), half_rows, tops), (slice(half_rows, rows), rows, bottoms)):
                    spread = log_decay[r, h : h + 1] - log_t[h : h + 1, 0:wide]
                    f = (jnp.exp(spread + drop[r, 0:wide]) * inner[r, 0:wide]).astype(BF16)
                    into.append(nn(f, xm[0:wide]))
            y = jnp.concatenate([tops[0] + tops[1], bottoms[0] + bottoms[1]], axis=0)
            skip2 = jnp.where(low[0:1], head[2:3, 2 * j : 2 * j + 1], head[2:3, 2 * j + 1 : 2 * j + 2])
            yv[slot, :, at : at + LANES] = y + xa * skip2
        pltpu.make_async_copy(yv.at[slot], Y.at[slot], esem.at[3]).start()

    def between(k, *steps):
        @pl.when(k)
        def _():
            for step in steps:
                step()

    whole = [(wxv, WX), (wtv, WT), (par, PAR), (head, HEAD), (wzv, WZ), (wov, WO), (tilev, TILE)]

    def save(*picked):
        for k in picked:
            pltpu.make_async_copy(*whole[k], wsem.at[k]).start()

    save(0, 1, 2, 3)

    @pl.loop(0, T)
    def _(k):
        between(k == 1, lambda: advance(0, 1), lambda: out_steps(0))
        between(k == 2, lambda: gx.relay_far(0))
        between(k == 4, lambda: [gx.relay_far(p) for p in range(1, sz.parts)], lambda: [advance(0, step) for step in range(2, G - 1)])
        between(k == 5, lambda: gg.relay(0))
        between(k == 6, lambda: [gg.relay(p) for p in range(1, sz.parts)], lambda: out_steps(1))
        between(k == 7, lambda: advance(0, G - 1))
        scan(k)

    out_steps(*range(2, G - 1))
    save(4)

    @pl.loop(0, T)
    def _(k):
        slot = slot_of(me, k)
        pz[slot] = nn(nv[slot], wzv[...].reshape(sz.d, cs))
        pltpu.make_async_copy(pz.at[slot], PZ.at[slot], esem.at[4]).start()

    for p in range(sz.parts):
        gg.relay_far(p)
    out_steps(G - 1)
    if not sz.aligned:
        for k in range(G):
            @pl.when(t_differs(sz, me, k))
            def _(k=k):
                landed(wov.at[k], orecv.at[k])

    save(5)

    @pl.loop(0, T)
    def _(k):
        slot = slot_of(me, k)

        between(lax.rem(k, 2) == 1, lambda: wait_pair(gg, k))
        pos = iota((rows, LANES), 0).astype(F32)
        seg = segments(pos, ends_of(smv[slot * G + me.g, taps + 3 : taps + 4, :], sz.seqs))
        valid = (seg < sz.seqs).astype(F32)
        tilev[slot] = smv[slot * G + me.g]
        zt = pz[slot]
        gm = nt(gov[slot], wov[...].reshape(cs, sz.d))
        gmv[slot] = gm
        pltpu.make_async_copy(gmv.at[slot], GM.at[slot], esem.at[5]).start()
        pltpu.make_async_copy(gov.at[slot], GO.at[slot], esem.at[6]).start()
        q1 = jnp.zeros((rows, LANES), F32)
        q2 = jnp.zeros((rows, LANES), F32)
        for j in range(tiles):
            tile = slice(j * LANES, (j + 1) * LANES)
            gated = yv[slot, :, tile] * (zt[:, tile] * jax.nn.sigmoid(zt[:, tile]))
            q1 = q1 + gated * gated
            q2 = q2 + gated * gm[:, tile] * par[taps + 1 : taps + 2, tile]
        q2 = q2 * valid
        lane = iota((rows, LANES), 1)
        stats = jnp.where(lane == 0, jnp.sum(q1, axis=1, keepdims=True), jnp.sum(q2, axis=1, keepdims=True)).T
        qv[pl.ds(slot, 1), :] = stats[0:1, :]
        qv[pl.ds(T + slot, 1), :] = stats[1:2, :]

    save(6)

    def q_copy(step):
        return remote(sz, qv, qr.at[me.t], qsend.at[0], qrecv.at[0], me.g, lax.rem(me.t + step, T))

    for step in range(1, T):
        q_copy(step).start()

    landed(qr.at[pl.ds(0, T - 1)], qrecv.at[0])
    total = qv[...]
    for step in range(1, T):
        total = total + qr[lax.rem(me.t + step, T)]
    Q[...] = total

    landed(qr.at[pl.ds(0, T - 1)], qsend.at[0])
    landed(wxv.at[pl.ds(0, T - 1)], axsend.at[0])
    landed(wzv.at[pl.ds(0, T - 1)], azsend.at[0])
    landed(wtv.at[pl.ds(0, G - 1)], tsend.at[0])
    landed(smv.at[pl.ds(0, G - 1)], ssend.at[0])
    landed(smv.at[pl.ds(0, (T - 1) * G)], ssend.at[1])
    for gather in (gx, gg, gt):
        gather.sent()
    for elsewhere, copy in out_targets():
        @pl.when(elsewhere)
        def _(copy=copy):
            copy().wait_send()
    if sz.aligned:
        for step in range(G - 1):
            for half in range(2):
                for up in (True, False):
                    have, more, _, copy = out_line(step, half, up)

                    @pl.when(have & more)
                    def _(copy=copy):
                        copy().wait_send()
    for half in range(2):
        for step in range(G - 1):
            for up in (True, False):
                have, more, plane, _, gauge, send, _ = line(half, step, up)

                @pl.when(have & more)
                def _(gauge=gauge, send=send, plane=plane, up=up):
                    landed(gauge, send.at[int(up), plane])
    for k, (src, dst) in enumerate(whole):
        pltpu.make_async_copy(src, dst, wsem.at[k]).wait()
    for a, (src, dst) in enumerate([(nv, NRM), (px, PX), (pt, PT), (yv, Y), (pz, PZ), (gmv, GM), (gov, GO)]):
        pltpu.make_async_copy(src, dst, esem.at[a]).wait()


def run_front(sz, x, go, win, tail, wout, norm, cw, cb, gate, lens, decay, bias, skip):
    n, g, t, rows, d, cs, tl, parts, fi = sz.n, sz.g, sz.t, sz.rows, sz.d, sz.cs, sz.tl, sz.parts, sz.fi
    dn, on = win.shape[0], wout.shape[0]
    any_ = pl.BlockSpec(memory_space=pl.ANY)
    vmem = pl.BlockSpec(memory_space=pltpu.VMEM)
    dma = pltpu.SemaphoreType.DMA
    shapes = dict(
        nrm=((t, rows, d), BF16), go=((t, rows, d), BF16), px=((t, rows, cs), F32), pt=((t, rows, tl), F32), pz=((t, rows, cs), F32),
        y=((t, rows, cs), F32), gm=((t, rows, cs), F32), wx=((n, dn, cs), BF16), wz=((n, dn, cs), BF16), wt=((n, dn, tl), BF16),
        wo=((g, on, d), BF16), q=((2 * t, rows), F32), par=((8, d), F32), head=((8, LANES), F32), tile=((t, 8, LANES), F32),
    )
    out = lambda *names: [jax.ShapeDtypeStruct(*shapes[name]) for name in names]
    scr = lambda *names: [pltpu.VMEM(*shapes[name]) for name in names]
    return pl.pallas_call(
        functools.partial(front_kernel, sz),
        in_specs=[any_] * 5 + [vmem] * 8,
        out_specs=[any_] * 11 + [vmem] + [any_] * 3,
        out_shape=out("nrm", "go", "px", "pt", "pz", "y", "gm", "wx", "wz", "wt", "wo", "q", "par", "head", "tile"),
        scratch_shapes=scr("nrm", "nrm", "go", "px", "pt", "pz", "y", "gm", "wx", "wz", "wt", "wo")
        + [pltpu.VMEM((8, LANES), F32), pltpu.VMEM((n, 8, LANES), F32)]
        + scr("par", "head", "q")
        + [pltpu.VMEM((t, 2 * t, rows), F32), pltpu.VMEM((t, 8, LANES), F32)]
        + [dma((1,)), dma((t, parts)), dma((1,)), dma((t, parts)), dma((1,)), dma((t, 1)), dma((1,)), dma((1,)), dma((1,)), dma((1,)),
           dma((2, g)), dma((g,)), dma((2, g)), dma((g,)), dma((1,)), dma((1,)), dma((3, g)), dma((g,)), dma((2,)), dma((2,)),
           dma((1,)), dma((1,)), dma((7,)), dma((7,)), dma((7,))],
        compiler_params=pltpu.CompilerParams(collective_id=0, has_side_effects=True, vmem_limit_bytes=63 << 20),
        name="front",
    )(x, go, win, tail, wout, norm, cw, cb, gate, lens, decay, bias, skip)


def bwd_kernel(sz, nrm_ref, px_ref, pt_ref, pz_ref, y_ref, gm_ref, q_ref, wx_ref, wz_ref, wt_ref, wo_ref, par_ref, head_ref, tile_ref,
               mix_ref, hid_ref, dz_ref, dx_ref, dt_ref, gn_ref, small_ref):
    b = pl.program_id(0)
    me = Place(sz)
    rows, cs, st, taps = sz.rows, sz.cs, sz.state, sz.taps
    tiles = cs // LANES
    keeps, valid, same = masks(rows, ends_of(tile_ref[0, taps + 3 : taps + 4, :], sz.seqs), taps)
    at_gate, at_conv, at_head, at_gain = sz.at_gate, sz.at_conv, sz.at_head, sz.at_gain
    lead = lax.rem(LANES - sz.nh * me.t, LANES)

    @pl.when(b == 0)
    def _():
        small_ref[...] = jnp.zeros(small_ref.shape, F32)

    def colsum(v):
        return jnp.sum(v, axis=0, keepdims=True)

    def conv_pre(u, at):
        return conv_tile(u, par_ref[0:taps, at : at + LANES], par_ref[taps : taps + 1, at : at + LANES], keeps, taps)

    def silu_pair(v):
        s = jax.nn.sigmoid(v)
        return v * s, s * (1.0 + v * (1.0 - s))

    def conv_back(u, dact, dsilu, at):
        dpre = dact * dsilu
        tile = at // LANES
        row = at_conv + tile * 8 if tile < tiles else sz.at_bc + (tile - tiles) * 8
        back = dpre * par_ref[taps - 1 : taps, at : at + LANES]
        small_ref[row + taps - 1 : row + taps, :] += colsum(dpre * u)
        small_ref[row + taps : row + taps + 1, :] += colsum(dpre)
        for off in range(1, taps):
            kept = dpre * keeps[off - 1]
            tap = taps - 1 - off
            small_ref[row + tap : row + tap + 1, :] += colsum(kept * pltpu.roll(u, off, 0))
            back = back + pltpu.roll(kept, rows - off, 0) * par_ref[tap : tap + 1, at : at + LANES]
        return back

    ub, uc = pt_ref[0, :, 0:st], pt_ref[0, :, st : 2 * st]
    bm, bslope = silu_pair(conv_pre(ub, cs))
    cm, cslope = silu_pair(conv_pre(uc, cs + st))
    raw = pltpu.roll(pt_ref[0, :, 2 * st : 2 * st + LANES], lead, 1) + head_ref[0:1, :]
    dt = softplus(raw)
    rate = -jnp.exp(head_ref[1:2, :])
    log_decay = jnp.dot(triangle(rows).astype(F32), dt * rate, precision=EXACT, preferred_element_type=F32)
    log_t = log_decay.T
    upper = iota((rows, rows), 1) >= iota((rows, rows), 0)
    drop = jnp.where(same & upper, 0.0, -jnp.inf)
    inner_t = three(nt, bm, cm)
    low = iota((rows, LANES), 1) < sz.hd
    lane = iota((rows, LANES), 1)
    q1 = jnp.broadcast_to(q_ref[pl.ds(b, 1), :], (LANES, rows)).T
    q2 = jnp.broadcast_to(q_ref[pl.ds(sz.t + b, 1), :], (LANES, rows)).T
    scale = lax.rsqrt(q1 / sz.di + EPS)
    pull = scale * scale * scale * q2 / sz.di

    dcb = jnp.zeros((rows, rows), F32)
    ddt = jnp.zeros((rows, LANES), F32)
    cols = jnp.zeros((rows, LANES), F32)
    rowsums = jnp.zeros((LANES, rows), F32)
    lane_row = iota((LANES, rows), 0)
    for j in range(tiles):
        at = j * LANES
        tile = slice(at, at + LANES)
        zt = pz_ref[0, :, tile]
        y = y_ref[0, :, tile]
        gm = gm_ref[0, :, tile] * valid
        gate = par_ref[taps + 1 : taps + 2, tile]
        sz_, zslope = silu_pair(zt)
        gated = y * sz_
        unit = gated * scale
        mix_ref[0, :, tile] = (unit * gate * valid).astype(BF16)
        small_ref[at_gate + j : at_gate + j + 1, :] += colsum(gm * unit)
        dgated = scale * gm * gate - gated * pull
        dz_ref[0, :, tile] = (dgated * y * zslope).astype(BF16)
        dy = dgated * sz_
        ux = px_ref[0, :, tile]
        xa, xslope = silu_pair(conv_pre(ux, at))
        small_ref[at_head + 3 + j : at_head + 4 + j, :] += colsum(dy * xa)
        dt2 = jnp.where(low, dt[:, 2 * j : 2 * j + 1], dt[:, 2 * j + 1 : 2 * j + 2])
        xd = xa * dt2
        dxd = []
        for e in range(2):
            h = 2 * j + e
            mine = low if e == 0 else jnp.logical_not(low)
            decay = jnp.exp(log_t[h : h + 1, :] - log_decay[:, h : h + 1] + drop)
            df = three(nt, jnp.where(mine, xd, 0.0), dy) * decay
            dcb = dcb + df
            p = df * inner_t
            cols = jnp.where(lane == h, jnp.sum(p, axis=1, keepdims=True), cols)
            rowsums = jnp.where(lane_row == h, colsum(p), rowsums)
            dxd.append(nn((decay * inner_t).astype(BF16), jnp.where(mine, dy, 0.0).astype(BF16)))
        dxd = dxd[0] + dxd[1]
        both = dxd * xa
        ddt = jnp.where(lane == 2 * j, jnp.sum(jnp.where(low, both, 0.0), axis=1, keepdims=True), ddt)
        ddt = jnp.where(lane == 2 * j + 1, jnp.sum(jnp.where(low, 0.0, both), axis=1, keepdims=True), ddt)
        skip2 = jnp.where(low[0:1], head_ref[2:3, 2 * j : 2 * j + 1], head_ref[2:3, 2 * j + 1 : 2 * j + 2])
        dx = dxd * dt2 + dy * skip2
        dx_ref[0, :, tile] = conv_back(ux, dx, xslope, at).astype(BF16)

    ga = jnp.dot(upper.astype(F32), rowsums.T - cols, precision=EXACT, preferred_element_type=F32)
    ddt = ddt + ga * rate
    small_ref[at_head : at_head + 1, :] += rate * colsum(ga * dt)
    draw = jnp.where(lane < sz.nh, ddt * jax.nn.sigmoid(raw), 0.0)
    small_ref[at_head + 1 : at_head + 2, :] += colsum(draw)
    dt_ref[0, :, 2 * st : 2 * st + LANES] = pltpu.roll(draw, sz.nh * me.t, 1).astype(BF16)
    dcb = dcb.astype(BF16)
    db = nn(dcb, cm.astype(BF16))
    dc = tn(dcb, bm.astype(BF16))
    dt_ref[0, :, 0:st] = conv_back(ub, db, bslope, cs).astype(BF16)
    dt_ref[0, :, st : 2 * st] = conv_back(uc, dc, cslope, cs + st).astype(BF16)

    hid_ref[0] = nn(mix_ref[0], wo_ref[...]).astype(BF16)
    gn = nt(dz_ref[0], wz_ref[...]) + nt(dx_ref[0], wx_ref[...]) + nt(dt_ref[0], wt_ref[...])
    gn_ref[0] = gn.astype(BF16)
    sums = colsum(gn * nrm_ref[0].astype(F32)) / par_ref[taps + 2 : taps + 3, 0 : sz.d]
    for k in range(sz.d // LANES):
        small_ref[at_gain + k : at_gain + k + 1, :] += sums[:, k * LANES : (k + 1) * LANES]


def run_bwd(sz, nrm, px, pt, pz, y, gm, q, wx, wz, wt, wo, par, head, tile):
    t, rows, d, cs, tl = sz.t, sz.rows, sz.d, sz.cs, sz.tl
    whole = lambda a: pl.BlockSpec(a.shape, lambda b: (0,) * a.ndim)
    block = lambda width: pl.BlockSpec((1, rows, width), lambda b: (b, 0, 0))
    return pl.pallas_call(
        functools.partial(bwd_kernel, sz),
        grid=(t,),
        in_specs=[block(d), block(cs), block(tl), block(cs), block(cs), block(cs), whole(q), whole(wx), whole(wz), whole(wt), whole(wo), whole(par),
                  whole(head), pl.BlockSpec((1, 8, LANES), lambda b: (b, 0, 0))],
        out_specs=[block(cs), block(d), block(cs), block(cs), block(tl), block(d), pl.BlockSpec((sz.small_rows, LANES), lambda b: (0, 0))],
        out_shape=[
            jax.ShapeDtypeStruct((t, rows, cs), BF16),
            jax.ShapeDtypeStruct((t, rows, d), BF16),
            jax.ShapeDtypeStruct((t, rows, cs), BF16),
            jax.ShapeDtypeStruct((t, rows, cs), BF16),
            jax.ShapeDtypeStruct((t, rows, tl), BF16),
            jax.ShapeDtypeStruct((t, rows, d), BF16),
            jax.ShapeDtypeStruct((sz.small_rows, LANES), F32),
        ],
        compiler_params=pltpu.CompilerParams(vmem_limit_bytes=60 << 20),
        name="bwd",
    )(nrm, px, pt, pz, y, gm, q, wx, wz, wt, wo, par, head, tile)


def reduce_kernel(sz, hp, gp, dwzx, dwtl, dwo, sm, hsum, gsum, gin, gtl, gout, gsm, hs, gs, r0h, r0g, r1h, r1g, r2h, r2g, rz, sz_, ro, rt, st, rtz, ra,
                  rs1, s1, rs2, p0send, p0recv, p1send, p1recv, p2send, p2recv, zsend, zrecv, asend, arecv, osend, orecv, tsend, trecv, uzsend, uzrecv,
                  s1send, s1recv, s2send, s2recv, usend, urecv):
    me = Place(sz)
    cs, rows, G, T, FI = sz.cs, sz.rows, sz.g, sz.t, sz.fi
    parts, pr = sz.rparts, sz.rows // sz.rparts
    greet_all(sz, me)

    def up32(v):
        return v.astype(F32)

    def s1_copy(step):
        return remote(sz, sm, rs1.at[me.g], s1send.at[step], s1recv.at[me.g], lax.rem(me.g + step, G), me.t)

    for step in range(1, G):
        s1_copy(step).start()

    arrays = [(hp, hs, r0h, r1h, r2h, hsum), (gp, gs, r0g, r1g, r2g, gsum)]
    order = (me.fa, me.fd, me.fb, me.fi)

    def p0_copy(k, which, part):
        src, _, r0 = arrays[k][:3]
        fi = order[which]
        rows_ = pl.ds(part * pr, pr)
        return remote(sz, src.at[fi * 2 + me.other, rows_], r0.at[fi, rows_], p0send.at[k, which, part], p0recv.at[k, fi, part], me.g, me.fi * 2 + me.other)

    for k in range(2):
        for which in range(4):
            for part in range(parts):
                p0_copy(k, which, part).start()

    def t_copy(step, g):
        there = lax.rem(me.t + step, T)
        return remote(sz, dwtl.at[index_of(sz, g, there)], rt.at[me.t, g], tsend.at[step, g], trecv.at[me.t, g], me.g, there)

    for step in range(1, T):
        for g in range(G):
            t_copy(step, g).start()

    def z_copy(step, fi):
        there = lax.rem(me.g + step, G)
        return remote(sz, dwzx.at[pl.ds(index_of(sz, there, jnp.int32(2 * fi)), 2)], rz.at[me.g, pl.ds(2 * fi, 2)], zsend.at[step, fi], zrecv.at[me.g, fi],
                      there, me.t)

    for step in range(1, G):
        for fi in range(FI):
            z_copy(step, fi).start()

    def o_copy(k):
        owner = me.t * G + k
        f, p = lax.div(owner, sz.p), lax.rem(owner, sz.p)
        return pltpu.make_async_remote_copy(src_ref=dwo.at[k], dst_ref=ro.at[me.g], send_sem=osend.at[k], recv_sem=orecv.at[me.g],
                                            device_id=(f, p), device_id_type=pl.DeviceIdType.MESH)

    for k in range(G):
        @pl.when(t_differs(sz, me, k))
        def _(k=k):
            o_copy(k).start()

    def p1_copy(k, which, part):
        _, s, _, r1 = arrays[k][:4]
        rows_ = pl.ds(part * pr, pr)
        return remote(sz, s.at[which, rows_], r1.at[which, rows_], p1send.at[k, which, part], p1recv.at[k, which, part], me.g, me.fa * 2 + me.c)

    def p2_copy(k, part):
        _, s, _, _, r2 = arrays[k][:5]
        rows_ = pl.ds(part * pr, pr)
        return remote(sz, s.at[2, rows_], r2.at[rows_], p2send.at[k, part], p2recv.at[k, part], me.g, me.fb * 2 + me.c)

    for k in range(2):
        src, s, r0, r1, r2, out = arrays[k]
        for which in range(4):
            fi = order[which]
            for part in range(parts):
                rows_ = pl.ds(part * pr, pr)
                landed(r0.at[fi, rows_], p0recv.at[k, fi, part])
                both = up32(src[fi * 2 + me.c, rows_]) + up32(r0[fi, rows_])
                if which < 2:
                    s[which, rows_] = both.astype(BF16)
                    p1_copy(k, which, part).start()
                elif which == 2:
                    s[2, rows_] = both.astype(BF16)
                else:
                    out[rows_] = both

    for step in range(1, T):
        for g in range(G):
            there = lax.rem(me.t + step, T)
            landed(rt.at[there, g], trecv.at[there, g])
    for g in range(G):
        total = up32(dwtl[index_of(sz, g, me.t)])
        for step in range(1, T):
            total = total + up32(rt[lax.rem(me.t + step, T), g])
        st[g] = total.astype(BF16)

    def uz_copy(step):
        there = lax.rem(me.g + step, G)
        return remote(sz, st.at[there], rtz.at[me.g], uzsend.at[step], uzrecv.at[me.g], there, me.t)

    for step in range(1, G):
        uz_copy(step).start()

    total = sm[...]
    for step in range(1, G):
        there = lax.rem(me.g + step, G)
        landed(rs1.at[there], s1recv.at[there])
        total = total + rs1[there]
    s1[...] = total
    rs2[me.t] = total

    def s2_copy(step):
        return remote(sz, s1, rs2.at[me.t], s2send.at[step], s2recv.at[me.t], me.g, lax.rem(me.t + step, T))

    for step in range(1, T):
        s2_copy(step).start()

    for k in range(2):
        src, s, r0, r1, r2, out = arrays[k]
        for part in range(parts):
            rows_ = pl.ds(part * pr, pr)
            landed(r1.at[1, rows_], p1recv.at[k, 1, part])
            s[2, rows_] = (up32(s[2, rows_]) + up32(r1[1, rows_])).astype(BF16)
            p2_copy(k, part).start()

    for fi in range(FI):
        for step in range(1, G):
            there = lax.rem(me.g + step, G)
            landed(rz.at[there, pl.ds(2 * fi, 2)], zrecv.at[there, fi])
        for c in range(2):
            total = up32(dwzx[index_of(sz, me.g, jnp.int32(2 * fi + c))])
            for step in range(1, G):
                total = total + up32(rz[lax.rem(me.g + step, G), 2 * fi + c])
            sz_[2 * fi + c] = total.astype(BF16)

    def a_copy(step):
        there = lax.rem(me.t + step, T)
        return remote(sz, sz_.at[there], ra.at[me.t], asend.at[step], arecv.at[me.t], me.g, there)

    for step in range(1, T):
        a_copy(step).start()
    ra[me.t] = sz_[me.t]

    total = jnp.zeros(gout.shape, F32)
    mine = lax.div(me.i, G) == me.t

    @pl.when(mine)
    def _():
        gout[...] = up32(dwo[lax.rem(me.i, G)])

    @pl.when(jnp.logical_not(mine))
    def _():
        gout[...] = jnp.zeros(gout.shape, F32)

    for g in range(G):
        other = jnp.logical_not(mine & (me.g == g))

        @pl.when(other)
        def _(g=g):
            landed(ro.at[g], orecv.at[g])
            gout[...] += up32(ro[g])

    total = up32(st[me.g])
    for step in range(1, G):
        there = lax.rem(me.g + step, G)
        landed(rtz.at[there], uzrecv.at[there])
        total = total + up32(rtz[there])
    gtl[...] = total

    for k in range(2):
        src, s, r0, r1, r2, out = arrays[k]
        for part in range(parts):
            rows_ = pl.ds(part * pr, pr)
            landed(r1.at[0, rows_], p1recv.at[k, 0, part])
            landed(r2.at[rows_], p2recv.at[k, part])
            out[rows_] = out[rows_] + up32(r1[0, rows_]) + up32(r2[rows_])

    for step in range(1, T):
        there = lax.rem(me.t + step, T)
        landed(ra.at[there], arecv.at[there])
        landed(rs2.at[there], s2recv.at[there])
    for t in range(T):
        gin[:, t * cs : (t + 1) * cs] = up32(ra[t, :, 0:cs])
        gin[:, sz.di + t * cs : sz.di + (t + 1) * cs] = up32(ra[t, :, cs:])
    total = rs2[0, 0 : sz.common]
    for t in range(1, T):
        total = total + rs2[t, 0 : sz.common]
    gsm[0 : sz.common] = total
    width = sz.small_rows - sz.common
    for t in range(T):
        gsm[sz.common + t * width : sz.common + (t + 1) * width] = rs2[t, sz.common :]

    for step in range(1, G):
        s1_copy(step).wait_send()
        uz_copy(step).wait_send()
        for fi in range(FI):
            z_copy(step, fi).wait_send()
    for step in range(1, T):
        s2_copy(step).wait_send()
        a_copy(step).wait_send()
        for g in range(G):
            t_copy(step, g).wait_send()
    for k in range(2):
        for part in range(parts):
            for which in range(4):
                p0_copy(k, which, part).wait_send()
            for which in range(2):
                p1_copy(k, which, part).wait_send()
            p2_copy(k, part).wait_send()
    for k in range(G):
        @pl.when(t_differs(sz, me, k))
        def _(k=k):
            o_copy(k).wait_send()


def run_reduce(sz, hp, gp, dwzx, dwtl, dwo, sm):
    n, g, t, rows, d, cs, tl, parts, fi = sz.n, sz.g, sz.t, sz.rows, sz.d, sz.cs, sz.tl, sz.rparts, sz.fi
    dn, on = dwzx.shape[1], dwo.shape[1]
    vmem = pl.BlockSpec(memory_space=pltpu.VMEM)
    dma = pltpu.SemaphoreType.DMA
    v = lambda *s: pltpu.VMEM(s, BF16)
    sr = sz.small_rows
    total_rows = sz.common + t * (sr - sz.common)
    return pl.pallas_call(
        functools.partial(reduce_kernel, sz),
        in_specs=[vmem] * 6,
        out_specs=[vmem] * 6,
        out_shape=[
            jax.ShapeDtypeStruct((rows, d), F32),
            jax.ShapeDtypeStruct((rows, d), F32),
            jax.ShapeDtypeStruct((dn, 2 * sz.di), F32),
            jax.ShapeDtypeStruct((dn, tl), F32),
            jax.ShapeDtypeStruct((on, d), F32),
            jax.ShapeDtypeStruct((total_rows, LANES), F32),
        ],
        scratch_shapes=[
            v(3, rows, d), v(3, rows, d), v(fi, rows, d), v(fi, rows, d), v(2, rows, d), v(2, rows, d), v(rows, d), v(rows, d),
            v(g, t, dn, 2 * cs), v(t, dn, 2 * cs), v(g, on, d), v(t, g, dn, tl), v(g, dn, tl), v(g, dn, tl), v(t, dn, 2 * cs),
            pltpu.VMEM((g, sr, LANES), F32), pltpu.VMEM((sr, LANES), F32), pltpu.VMEM((t, sr, LANES), F32),
            dma((2, 4, parts)), dma((2, fi, parts)), dma((2, 2, parts)), dma((2, 2, parts)), dma((2, parts)), dma((2, parts)),
            dma((g, fi)), dma((g, fi)), dma((t,)), dma((t,)), dma((g,)), dma((g,)), dma((t, g)), dma((t, g)), dma((g,)), dma((g,)),
            dma((g,)), dma((g,)), dma((t,)), dma((t,)), dma((1,)), dma((1,)),
        ],
        compiler_params=pltpu.CompilerParams(collective_id=2, has_side_effects=True, vmem_limit_bytes=63 << 20),
        name="reduce",
    )(hp, gp, dwzx, dwtl, dwo, sm)


def sizes(mesh, hidden, lengths, in_proj, conv_weight, gate_gain, decay_log):
    sz = Sizes()
    sz.f, sz.p = mesh.shape["fsdp"], mesh.shape["dp"]
    sz.n = sz.f * sz.p
    sz.rows, sz.d = hidden.shape
    sz.seqs = lengths.shape[1]
    sz.conv, sz.taps = conv_weight.shape[0] * sz.n, conv_weight.shape[1]
    sz.di = gate_gain.shape[0] * sz.n
    sz.state = (sz.conv - sz.di) // 2
    sz.heads = decay_log.shape[0]
    sz.hd = sz.di // sz.heads
    sz.fi = math.gcd(sz.f, sz.di // (2 * LANES))
    sz.t = 2 * sz.fi
    sz.z = sz.p // 2
    sz.g = sz.f // sz.fi * sz.z
    sz.aligned = sz.f == sz.fi
    sz.cs, sz.nh = sz.di // sz.t, sz.heads // sz.t
    sz.tail = in_proj.shape[1] - 2 * sz.di
    sz.tl = -(-sz.tail // LANES) * LANES
    sz.parts, sz.rparts = 2, 2
    sz.part_rows = sz.rows // sz.parts
    small_layout(sz)
    return sz


def local(mesh, hidden_in, lengths, norm_gain, in_proj, conv_weight, conv_bias, gate_gain, out_proj, decay_log, step_bias, skip_gain, grad_out):
    sz = sizes(mesh, hidden_in, lengths, in_proj, conv_weight, gate_gain, decay_log)
    n, t, cs, di = sz.n, sz.t, sz.cs, sz.di
    f, p = lax.axis_index("fsdp"), lax.axis_index("dp")
    index = f * sz.p + p
    dn, cn, kn = norm_gain.shape[0], conv_bias.shape[0], gate_gain.shape[0]

    tail = jnp.pad(in_proj[:, 2 * di :], ((0, 0), (0, sz.tl - sz.tail)))
    row = lambda a: a.reshape(1, -1)
    nrm, go_all, px, pt, pz, y, gm, wx, wz, wt, wo, q, par, head, tile = run_front(
        sz, hidden_in, grad_out, in_proj, tail, out_proj, row(norm_gain), conv_weight.T, row(conv_bias), row(gate_gain), lengths,
        row(decay_log), row(step_bias), row(skip_gain))
    wx, wz, wt, wo = wx.reshape(sz.d, cs), wz.reshape(sz.d, cs), wt.reshape(sz.d, sz.tl), wo.reshape(cs, sz.d)
    gain = par[sz.taps + 2 : sz.taps + 3]
    mix, hid, dz, dx, dtl, gn, small = run_bwd(sz, nrm, px, pt, pz, y, gm, q, wx, wz, wt, wo, par, head, tile)

    tall = lambda a: a.reshape(t * sz.rows, a.shape[2])
    dwzx = jnp.concatenate([tn(tall(nrm), tall(a)).astype(BF16) for a in (dz, dx)], axis=1).reshape(n, dn, 2 * cs)
    dwtl = tn(tall(nrm), tall(dtl)).astype(BF16).reshape(n, dn, sz.tl)
    dwo = tn(tall(mix), tall(go_all)).astype(BF16).reshape(sz.g, cs // sz.g, sz.d)
    hsum, gsum, gin, gtl, gout, gsm = run_reduce(sz, hid, gn, dwzx, dwtl, dwo, small)

    x = hidden_in.astype(F32)
    hidden_out = (x + hsum).astype(BF16)
    scale = lax.rsqrt(jnp.mean(x * x, axis=1, keepdims=True) + EPS)
    dxhat = gsum * gain
    inner = jnp.mean(dxhat * x, axis=1, keepdims=True)
    grad_in = grad_out.astype(F32) + scale * (dxhat - x * (scale * scale * inner))
    grad_in_proj = jnp.concatenate([gin, gtl[:, : sz.tail]], axis=1)

    own = lambda a, width: lax.dynamic_slice_in_dim(a, index * width, width)
    common, slices = gsm[: sz.common], gsm[sz.common :].reshape(t, -1, LANES)
    at = lambda place: place - sz.common
    grad_norm_gain = own(common[: sz.d // LANES].reshape(-1), dn)
    conv_x = slices[:, : at(sz.at_gate)].reshape(-1, 8, LANES)
    conv = jnp.concatenate([conv_x, common[sz.at_bc :].reshape(-1, 8, LANES)])
    conv = conv[:, : sz.taps + 1].transpose(0, 2, 1).reshape(sz.conv, sz.taps + 1)
    conv = own(conv, cn)
    tiles = cs // LANES
    grad_gate = own(slices[:, at(sz.at_gate) : at(sz.at_gate) + tiles].reshape(-1), kn)
    heads = slices[:, at(sz.at_head) :]
    grad_decay = heads[:, 0, : sz.nh].reshape(-1)
    grad_bias = heads[:, 1, : sz.nh].reshape(-1)
    grad_skip = jnp.sum(heads[:, 3 : 3 + tiles].reshape(sz.heads, sz.hd), axis=1)
    return (hidden_out, grad_in, grad_norm_gain, grad_in_proj, conv[:, : sz.taps], conv[:, sz.taps], grad_gate, gout, grad_decay, grad_bias, grad_skip)


def solution(mesh):
    both = ("fsdp", "dp")
    wide, flat, free = P(both, None), P(both), P()
    in_specs = (wide, wide, flat, wide, wide, flat, flat, wide, free, free, free, wide)
    out_specs = (wide, wide, flat, wide, wide, flat, flat, wide, free, free, free)
    return jax.shard_map(functools.partial(local, mesh), mesh=mesh, in_specs=in_specs, out_specs=out_specs, check_vma=False)
```

```python
import functools
import math

import jax
import jax.numpy as jnp
from jax import lax
from jax.experimental import pallas as pl
from jax.experimental.pallas import tpu as pltpu
from jax.sharding import PartitionSpec as P

EPS = 1e-05
F32 = jnp.float32
BF16 = jnp.bfloat16
EXACT = lax.Precision.HIGHEST
LANES = 128


def nn(a, b):
    return lax.dot_general(a, b, (((1,), (0,)), ((), ())), preferred_element_type=F32)


def nt(a, b):
    return lax.dot_general(a, b, (((1,), (1,)), ((), ())), preferred_element_type=F32)


def tn(a, b):
    return lax.dot_general(a, b, (((0,), (0,)), ((), ())), preferred_element_type=F32)


def iota(shape, dim):
    return lax.broadcasted_iota(jnp.int32, shape, dim)


def conv_tile(u, weights, bias, keeps, taps):
    pre = bias + u * weights[taps - 1 : taps, :]
    for off in range(1, taps):
        pre = pre + pltpu.roll(u, off, 0) * keeps[off - 1] * weights[taps - 1 - off : taps - off, :]
    return pre


def softplus(v):
    return jnp.maximum(v, 0.0) + jnp.log1p(jnp.exp(-jnp.abs(v)))


def split(a):
    hi = a.astype(BF16)
    return hi, (a - hi.astype(F32)).astype(BF16)


def three(product, a, b):
    ah, al = split(a)
    bh, bl = split(b)
    return product(ah, bh) + (product(ah, bl) + product(al, bh))


class Sizes:
    pass


def up8(count):
    return -(-count // 8) * 8


def small_layout(sz):
    tiles = sz.cs // LANES
    sz.at_bc = 0
    sz.common = 2 * sz.state // LANES * 8
    sz.at_conv = sz.common
    sz.at_gate = sz.at_conv + tiles * 8
    sz.at_head = sz.at_gate + up8(tiles)
    sz.small_rows = sz.at_head + up8(3 + tiles)


def device_of(sz, g, t):
    return (lax.div(g, sz.z) * sz.fi + lax.div(t, 2), lax.rem(g, sz.z) * 2 + lax.rem(t, 2))


def index_of(sz, g, t):
    f, p = device_of(sz, g, t)
    return f * sz.p + p


class Place:
    def __init__(self, sz):
        f, p = lax.axis_index("fsdp"), lax.axis_index("dp")
        fi, z = lax.rem(f, sz.fi), lax.div(p, 2)
        self.c = lax.rem(p, 2)
        self.g = lax.div(f, sz.fi) * sz.z + z
        self.t = fi * 2 + self.c
        self.i = f * sz.p + p
        u, v = lax.rem(fi, 2), lax.div(fi, 2)
        across, along = v * 2 + 1 - u, (1 - v) * 2 + u
        self.fi = fi
        self.fa = across * (1 - self.c) + along * self.c
        self.fb = along * (1 - self.c) + across * self.c
        self.fd = sz.fi - 1 - fi
        self.other = 1 - self.c


def remote(sz, src, dst, send, recv, g, t):
    return pltpu.make_async_remote_copy(
        src_ref=src, dst_ref=dst, send_sem=send, recv_sem=recv, device_id=device_of(sz, g, t), device_id_type=pl.DeviceIdType.MESH
    )


def landed(ref, sem):
    pltpu.make_async_copy(ref, ref, sem).wait()


def greet_all(sz, me):
    barrier = pltpu.get_barrier_semaphore()

    @pl.loop(1, sz.n)
    def _(step):
        there = lax.rem(me.i + step, sz.n)
        pl.semaphore_signal(barrier, inc=1, device_id=(lax.div(there, sz.p), lax.rem(there, sz.p)), device_id_type=pl.DeviceIdType.MESH)

    pl.semaphore_wait(barrier, sz.n - 1)


def greet_near(sz, me):
    barrier = pltpu.get_barrier_semaphore()
    near = [(me.g, lax.rem(me.t + step, sz.t)) for step in range(1, sz.t)] + [(lax.rem(me.g + step, sz.g), me.t) for step in range(1, sz.g)]
    for g, t in near:
        pl.semaphore_signal(barrier, inc=1, device_id=device_of(sz, g, t), device_id_type=pl.DeviceIdType.MESH)
    pl.semaphore_wait(barrier, len(near))


class PlaneGather:
    def __init__(self, sz, me, parts, own, views, gauge, bulk, send, recv):
        self.sz, self.me, self.parts, self.own, self.views, self.gauge, self.bulk, self.send, self.recv = sz, me, parts, own, views, gauge, bulk, send, recv
        self.a, self.b, self.d = me.fa * 2 + me.c, me.fb * 2 + me.c, me.fd * 2 + me.c
        self.pair = me.fi * 2 + me.other

    def push(self, kind, part):
        slot = (self.me.t, self.me.t, self.me.t, self.a, self.a, self.b, self.d)[kind]
        target = (self.a, self.b, self.pair, self.b, self.pair, self.pair, self.pair)[kind]
        views = self.views(slot, part)
        for src, dst in zip(self.own(part) if kind < 3 else views, views):
            remote(self.sz, src, dst, self.send.at[0], self.recv.at[slot, part], self.me.g, target).start()

    def arrived(self, slot, part):
        landed(self.gauge, self.recv.at[slot, part])

    def start(self, part):
        for kind in range(3):
            self.push(kind, part)

    def relay(self, part):
        self.arrived(self.a, part)
        self.push(3, part)
        self.push(4, part)
        self.arrived(self.b, part)
        self.push(5, part)

    def relay_far(self, part):
        self.arrived(self.d, part)
        self.push(6, part)

    def sent(self):
        landed(self.bulk, self.send.at[0])


def t_differs(sz, me, k):
    return me.t * sz.g + k != me.i


def select_rows(sz, packed, channel, per):
    n = packed.shape[0]
    wide = channel.shape[1]
    owner = jnp.floor((channel + 0.5) * (1.0 / per))
    place = channel - owner * per
    pick = (iota((LANES, wide), 0).astype(F32) == place).astype(BF16)
    spread = nn(packed.reshape(n * 8, LANES).astype(BF16), pick).reshape(n, 8, wide)
    over = lambda v, by: jnp.floor((v + 0.5) * (1.0 / by))
    spot = iota((n, 8, LANES), 0).astype(F32)
    rank = over(spot, sz.g)
    plane = spot - sz.g * rank
    fi, fo = over(rank, 2), over(plane, sz.z)
    device = ((fo * sz.fi + fi) * sz.z + plane - sz.z * fo) * 2 + rank - 2 * fi
    total = jnp.zeros((8, wide), F32)
    parts = []
    for at in range(0, wide, LANES):
        hit = device == owner[None, :, at : at + LANES]
        parts.append(jnp.sum(jnp.where(hit, spread[:, :, at : at + LANES], 0.0), axis=0))
    return jnp.concatenate(parts, axis=1)


def lanes_of(wide):
    return iota((1, wide), 1).astype(F32)


def slot_of(me, k):
    flip = lambda bit, other: bit + other - 2 * bit * other
    v, u, c = lax.div(me.t, 4), lax.rem(lax.div(me.t, 2), 2), me.c
    kv, ku, kc = lax.div(k, 4), lax.rem(lax.div(k, 2), 2), lax.rem(k, 2)
    return (flip(v, kv) * 2 + flip(u, ku)) * 2 + flip(c, kc)


def ends_of(row, count):
    ends, total = [], jnp.zeros((1, 1), F32)
    for slot in range(count):
        total = total + row[:, slot : slot + 1]
        ends.append(total)
    return ends


def segments(pos, ends):
    total = jnp.zeros(pos.shape, F32)
    for end in ends:
        total = total + (pos >= end).astype(F32)
    return total


def masks(rows, ends, taps):
    pos = iota((rows, LANES), 0).astype(F32)
    seg = segments(pos, ends)
    keeps = []
    for off in range(1, taps):
        same = (segments(pos - off, ends) == seg) & (pos >= off)
        keeps.append(same.astype(F32))
    valid = (seg < len(ends)).astype(F32)
    seg_row = segments(lanes_of(rows), ends)
    same = jnp.concatenate([(seg == seg_row[:, at : at + LANES]) for at in range(0, rows, LANES)], axis=1)
    return keeps, valid, same


def triangle(rows):
    return iota((rows, rows), 0) >= iota((rows, rows), 1)


def front_kernel(sz, x, go, win, tail, wout, norm, cw, cb, gate, lens, decay, bias, skip,
                 NT, GO, PX, PT, PZ, Y, GM, WX, WZ, WT, WO, Q, PAR, HEAD, TILE,
                 xv, nv, gov, px, pt, pz, yv, gmv, wxv, wzv, wtv, wov, pack, smv, par, head, qv, qr, tilev, flip,
                 xsend, xrecv, gsend, grecv, wsend, wrecv, axsend, axrecv, azsend, azrecv, zxsend, zxrecv, zzsend, zzrecv,
                 tsend, trecv, osend, orecv, ssend, srecv, qsend, qrecv, lsem, esem, wsem):
    me = Place(sz)
    cs, rows, G, T, st, taps = sz.cs, sz.rows, sz.g, sz.t, sz.state, sz.taps
    tiles = cs // LANES
    pack[...] = jnp.zeros(pack.shape, F32)
    dn, cn, kn = norm.shape[1], cb.shape[1], gate.shape[1]
    pack[0:taps, 0:cn] = cw[...].astype(F32)
    pack[taps : taps + 1, 0:cn] = cb[...].astype(F32)
    pack[taps + 1 : taps + 2, 0:kn] = gate[...].astype(F32)
    pack[taps + 2 : taps + 3, 0:dn] = norm[...].astype(F32)
    pack[taps + 3 : taps + 4, 0 : sz.seqs] = lens[...].astype(F32)
    (greet_near if sz.aligned else greet_all)(sz, me)

    tile_of = lambda g, t: smv.at[t * G + g]

    def pack_line(step):
        return remote(sz, pack, tile_of(me.g, me.t), ssend.at[0], srecv.at[0], lax.rem(me.g + step, G), me.t)

    def pack_plane(step):
        mine = smv.at[pl.ds(me.t * G, G)]
        return remote(sz, mine, mine, ssend.at[1], srecv.at[1], me.g, lax.rem(me.t + step, T))

    def columns(half, t):
        return win.at[:, pl.ds(pl.multiple_of(half * sz.di + t * cs, LANES), cs)]

    def exchange(half, step):
        there = lax.rem(me.t + step, T)
        wv, send, recv = ((wzv, azsend, azrecv), (wxv, axsend, axrecv))[half]
        return remote(sz, columns(half, there), wv.at[me.i], send.at[0], recv.at[0], me.g, there)

    def tail_copy(step):
        there = lax.rem(me.g + step, G)
        return remote(sz, tail, wtv.at[me.i], tsend.at[0], trecv.at[0], there, me.t)

    for step in range(1, G):
        tail_copy(step).start()
        pack_line(step).start()
    for step in range(1, T):
        exchange(1, step).start()

    part = lambda ref, k: ref.at[pl.ds(k * sz.part_rows, sz.part_rows)]
    gx = PlaneGather(sz, me, sz.parts, lambda k: [part(x, k)], lambda s, k: [part(xv.at[s], k)], part(xv.at[0], 0), xv.at[pl.ds(0, T - 1)], xsend, xrecv)
    gg = PlaneGather(sz, me, sz.parts, lambda k: [part(go, k)], lambda s, k: [part(gov.at[s], k)], part(gov.at[0], 0), gov.at[pl.ds(0, T - 1)], gsend, grecv)
    tails_of = lambda s, k: [wtv.at[index_of(sz, jnp.int32(g), s)] for g in range(G)]
    gt = PlaneGather(sz, me, 1, lambda k: tails_of(me.t, k), tails_of, wtv.at[pl.ds(0, G)], wtv.at[pl.ds(0, (T - 1) * G)], wsend, wrecv)

    owner_t, piece = lax.div(me.i, G), lax.rem(me.i, G)

    def out_copy(g):
        return remote(sz, wout, wov.at[piece], osend.at[2, g], orecv.at[piece], g, owner_t)

    def out_targets():
        planes = (me.g,) if sz.aligned else tuple(range(G))
        for g in planes:
            elsewhere = (owner_t != me.t) | (me.g != g)
            yield elsewhere, (lambda g=g: out_copy(jnp.int32(0) + g))

    def out_line(step, half, up):
        plane = me.g - step if up else me.g + step
        first = 2 * plane - me.c * sz.z
        have = (plane >= 0 if up else plane < G) & (first >= 0) & (first < G)
        more = (me.g < G - 1) if up else (me.g > 0)
        k = jnp.clip(first, 0, G - 2) + half
        nxt = jnp.clip(me.g + 1 if up else me.g - 1, 0, G - 1)
        copy = lambda: remote(sz, wov.at[k], wov.at[k], osend.at[int(up), k], orecv.at[k], nxt, me.t)
        return have, more, k, copy

    def out_advance(step):
        for half in range(2):
            if step == 0:
                have, _, k, _ = out_line(0, half, True)

                @pl.when(have & t_differs(sz, me, k))
                def _(k=k):
                    landed(wov.at[k], orecv.at[k])
            for up in (True, False):
                have, more, k, copy = out_line(step, half, up)
                if step > 0:
                    @pl.when(have)
                    def _(k=k):
                        landed(wov.at[k], orecv.at[k])
                if step < G - 1:
                    @pl.when(have & more)
                    def _(copy=copy):
                        copy().start()

    def out_steps(*steps):
        if sz.aligned:
            for step in steps:
                out_advance(step)

    for elsewhere, copy in out_targets():
        @pl.when(elsewhere)
        def _(copy=copy):
            copy().start()

    ins = [
        pltpu.make_async_copy(columns(1, me.t), wxv.at[me.i], lsem.at[0]),
        pltpu.make_async_copy(columns(0, me.t), wzv.at[me.i], lsem.at[1]),
        pltpu.make_async_copy(tail, wtv.at[me.i], lsem.at[2]),
        pltpu.make_async_copy(pack, tile_of(me.g, me.t), lsem.at[3]),
        pltpu.make_async_copy(x, xv.at[me.t], lsem.at[4]),
        pltpu.make_async_copy(go, gov.at[me.t], lsem.at[5]),
    ]
    for copy in ins:
        copy.start()
    for copy in ins:
        copy.wait()

    @pl.when(owner_t == me.t)
    def _():
        copy = pltpu.make_async_copy(wout, wov.at[piece], lsem.at[6])
        copy.start()
        copy.wait()

    head[...] = jnp.zeros(head.shape, F32)
    head[0:1, 0 : sz.heads] = bias[...]
    head[1:2, 0 : sz.heads] = decay[...]
    head[2:3, 0 : sz.heads] = skip[...]
    lead = lax.rem(LANES - sz.nh * me.t, LANES)
    head[...] = pltpu.roll(head[...], lead, 1)

    landed(smv.at[pl.ds(0, G - 1)], srecv.at[0])
    landed(wtv.at[pl.ds(0, G - 1)], trecv.at[0])
    for step in range(1, T):
        pack_plane(step).start()
    gt.start(0)
    gx.start(0)

    def arrive(half):
        wv, _, recv = ((wzv, azsend, azrecv), (wxv, axsend, axrecv))[half]
        landed(wv.at[pl.ds(0, T - 1)], recv.at[0])

    def line(half, step, up):
        wv, send, recv = ((wzv, zzsend, zzrecv), (wxv, zxsend, zxrecv))[half]
        plane = me.g - step if up else me.g + step
        have = (plane >= 0) if up else (plane < G)
        more = (me.g < G - 1) if up else (me.g > 0)
        plane = jnp.clip(plane, 0, G - 1)
        nxt = jnp.clip(me.g + 1 if up else me.g - 1, 0, G - 1)

        def push():
            for fi in range(sz.fi):
                block = wv.at[pl.ds(index_of(sz, plane, jnp.int32(2 * fi)), 2)]
                remote(sz, block, block, send.at[int(up), plane], recv.at[plane], nxt, me.t).start()

        return have, more, plane, push, wv.at[pl.ds(0, T)], send, recv

    def advance(half, step):
        for up in (True, False):
            have, more, plane, push, gauge, _, recv = line(half, step, up)
            if step > 0:
                @pl.when(have)
                def _(gauge=gauge, recv=recv, plane=plane):
                    landed(gauge, recv.at[plane])
            if step < G - 1:
                pl.when(have & more)(push)

    arrive(1)
    advance(1, 0)
    gt.relay(0)
    for step in range(1, T):
        exchange(0, step).start()
    for p in range(1, sz.parts):
        gx.start(p)
    advance(1, 1)
    landed(smv.at[pl.ds(0, (T - 1) * G)], srecv.at[1])
    packed = smv[...]
    ch = lanes_of(cs + 2 * st)
    start_ch = (me.t * cs).astype(F32)
    ch = jnp.where(ch < cs, ch + start_ch, ch + (sz.di - cs))
    par[:, 0 : cs + 2 * st] = select_rows(sz, packed, ch, cn)
    picked = select_rows(sz, packed, lanes_of(cs) + start_ch, kn)
    par[taps + 1 : taps + 2, 0:cs] = picked[taps + 1 : taps + 2]
    gains = select_rows(sz, packed, lanes_of(sz.d), dn)
    par[taps + 2 : taps + 3, 0 : sz.d] = gains[taps + 2 : taps + 3]

    def normalize(k):
        slot = slot_of(me, k)
        xb = xv[slot].astype(F32)
        mean = jnp.mean(xb * xb, axis=1, keepdims=True)
        nrm = (xb * lax.rsqrt(mean + EPS) * par[taps + 2 : taps + 3, 0 : sz.d]).astype(BF16)
        nv[slot] = nrm
        flip[...] = nrm.T
        turn = pltpu.make_async_copy(flip, NT.at[:, pl.ds(pl.multiple_of(slot * rows, LANES), rows)], esem.at[0])
        turn.start()
        turn.wait()

    def wait_pair(gather, k):
        slot = slot_of(me, k)
        for p in range(sz.parts):
            gather.arrived(slot, p)

    normalize(jnp.int32(0))
    wait_pair(gx, jnp.int32(1))
    normalize(jnp.int32(1))
    gx.relay(0)
    for step in range(2, G - 1):
        advance(1, step)
    arrive(0)
    advance(0, 0)
    gt.relay_far(0)
    advance(1, G - 1)
    for p in range(1, sz.parts):
        gx.relay(p)
    for p in range(sz.parts):
        gg.start(p)
    for fi in (me.fi, me.fa, me.fb, me.fd):
        gt.arrived(fi * 2 + me.other, 0)

    low = iota((rows, LANES), 1) < sz.hd
    tri = triangle(rows)
    half_rows = rows // 2

    def scan(k):
        slot = slot_of(me, k)

        @pl.when((k > 2) & (lax.rem(k, 2) == 1))
        def _():
            wait_pair(gx, k)

        @pl.when(k > 1)
        def _():
            normalize(k)

        keeps, _, same = masks(rows, ends_of(smv[slot * G + me.g, taps + 3 : taps + 4, :], sz.seqs), taps)
        nrm = nv[slot]
        pxv = nn(nrm, wxv[...].reshape(sz.d, cs))
        ptl = nn(nrm, wtv[...].reshape(sz.d, sz.tl))
        px[slot] = pxv
        pt[slot] = ptl
        pltpu.make_async_copy(px.at[slot], PX.at[slot], esem.at[1]).start()
        pltpu.make_async_copy(pt.at[slot], PT.at[slot], esem.at[2]).start()

        def act(u, at):
            return jax.nn.silu(conv_tile(u, par[0:taps, at : at + LANES], par[taps : taps + 1, at : at + LANES], keeps, taps))

        bm = act(ptl[:, 0:st], cs)
        cm = act(ptl[:, st : 2 * st], cs + st)
        raw = pltpu.roll(ptl[:, 2 * st : 2 * st + LANES], lead, 1)
        dt = softplus(raw + head[0:1, :])
        rate = -jnp.exp(head[1:2, :])
        log_decay = jnp.dot(tri.astype(F32), dt * rate, precision=EXACT, preferred_element_type=F32)
        log_t = log_decay.T
        drop = jnp.where(same & tri, 0.0, -jnp.inf)
        inner = three(nt, cm, bm)
        for j in range(tiles):
            at = j * LANES
            xa = act(pxv[:, at : at + LANES], at)
            dt2 = jnp.where(low, dt[:, 2 * j : 2 * j + 1], dt[:, 2 * j + 1 : 2 * j + 2])
            xd = xa * dt2
            tops, bottoms = [], []
            for e in range(2):
                h = 2 * j + e
                mine = low if e == 0 else jnp.logical_not(low)
                xm = jnp.where(mine, xd, 0.0).astype(BF16)
                for r, wide, into in ((slice(0, half_rows), half_rows, tops), (slice(half_rows, rows), rows, bottoms)):
                    spread = log_decay[r, h : h + 1] - log_t[h : h + 1, 0:wide]
                    f = (jnp.exp(spread + drop[r, 0:wide]) * inner[r, 0:wide]).astype(BF16)
                    into.append(nn(f, xm[0:wide]))
            y = jnp.concatenate([tops[0] + tops[1], bottoms[0] + bottoms[1]], axis=0)
            skip2 = jnp.where(low[0:1], head[2:3, 2 * j : 2 * j + 1], head[2:3, 2 * j + 1 : 2 * j + 2])
            yv[slot, :, at : at + LANES] = y + xa * skip2
        pltpu.make_async_copy(yv.at[slot], Y.at[slot], esem.at[3]).start()

    def between(k, *steps):
        @pl.when(k)
        def _():
            for step in steps:
                step()

    whole = [(wxv, WX), (wtv, WT), (par, PAR), (head, HEAD), (wzv, WZ), (wov, WO), (tilev, TILE)]

    def save(*picked):
        for k in picked:
            pltpu.make_async_copy(*whole[k], wsem.at[k]).start()

    save(0, 1, 2, 3)

    @pl.loop(0, T)
    def _(k):
        between(k == 1, lambda: advance(0, 1), lambda: out_steps(0))
        between(k == 2, lambda: gx.relay_far(0))
        between(k == 4, lambda: [gx.relay_far(p) for p in range(1, sz.parts)], lambda: [advance(0, step) for step in range(2, G - 1)])
        between(k == 5, lambda: gg.relay(0))
        between(k == 6, lambda: [gg.relay(p) for p in range(1, sz.parts)], lambda: out_steps(1))
        between(k == 7, lambda: advance(0, G - 1))
        scan(k)

    out_steps(*range(2, G - 1))
    save(4)

    @pl.loop(0, T)
    def _(k):
        slot = slot_of(me, k)
        pz[slot] = nn(nv[slot], wzv[...].reshape(sz.d, cs))
        pltpu.make_async_copy(pz.at[slot], PZ.at[slot], esem.at[4]).start()

    for p in range(sz.parts):
        gg.relay_far(p)
    out_steps(G - 1)
    if not sz.aligned:
        for k in range(G):
            @pl.when(t_differs(sz, me, k))
            def _(k=k):
                landed(wov.at[k], orecv.at[k])

    save(5)

    @pl.loop(0, T)
    def _(k):
        slot = slot_of(me, k)

        between(lax.rem(k, 2) == 1, lambda: wait_pair(gg, k))
        pos = iota((rows, LANES), 0).astype(F32)
        seg = segments(pos, ends_of(smv[slot * G + me.g, taps + 3 : taps + 4, :], sz.seqs))
        valid = (seg < sz.seqs).astype(F32)
        tilev[slot] = smv[slot * G + me.g]
        zt = pz[slot]
        gm = nt(gov[slot], wov[...].reshape(cs, sz.d))
        gmv[slot] = gm
        pltpu.make_async_copy(gmv.at[slot], GM.at[slot], esem.at[5]).start()
        pltpu.make_async_copy(gov.at[slot], GO.at[slot], esem.at[6]).start()
        q1 = jnp.zeros((rows, LANES), F32)
        q2 = jnp.zeros((rows, LANES), F32)
        for j in range(tiles):
            tile = slice(j * LANES, (j + 1) * LANES)
            gated = yv[slot, :, tile] * (zt[:, tile] * jax.nn.sigmoid(zt[:, tile]))
            q1 = q1 + gated * gated
            q2 = q2 + gated * gm[:, tile] * par[taps + 1 : taps + 2, tile]
        q2 = q2 * valid
        lane = iota((rows, LANES), 1)
        stats = jnp.where(lane == 0, jnp.sum(q1, axis=1, keepdims=True), jnp.sum(q2, axis=1, keepdims=True)).T
        qv[pl.ds(slot, 1), :] = stats[0:1, :]
        qv[pl.ds(T + slot, 1), :] = stats[1:2, :]

    save(6)

    def q_copy(step):
        return remote(sz, qv, qr.at[me.t], qsend.at[0], qrecv.at[0], me.g, lax.rem(me.t + step, T))

    for step in range(1, T):
        q_copy(step).start()

    landed(qr.at[pl.ds(0, T - 1)], qrecv.at[0])
    total = qv[...]
    for step in range(1, T):
        total = total + qr[lax.rem(me.t + step, T)]
    Q[...] = total

    landed(qr.at[pl.ds(0, T - 1)], qsend.at[0])
    landed(wxv.at[pl.ds(0, T - 1)], axsend.at[0])
    landed(wzv.at[pl.ds(0, T - 1)], azsend.at[0])
    landed(wtv.at[pl.ds(0, G - 1)], tsend.at[0])
    landed(smv.at[pl.ds(0, G - 1)], ssend.at[0])
    landed(smv.at[pl.ds(0, (T - 1) * G)], ssend.at[1])
    for gather in (gx, gg, gt):
        gather.sent()
    for elsewhere, copy in out_targets():
        @pl.when(elsewhere)
        def _(copy=copy):
            copy().wait_send()
    if sz.aligned:
        for step in range(G - 1):
            for half in range(2):
                for up in (True, False):
                    have, more, _, copy = out_line(step, half, up)

                    @pl.when(have & more)
                    def _(copy=copy):
                        copy().wait_send()
    for half in range(2):
        for step in range(G - 1):
            for up in (True, False):
                have, more, plane, _, gauge, send, _ = line(half, step, up)

                @pl.when(have & more)
                def _(gauge=gauge, send=send, plane=plane, up=up):
                    landed(gauge, send.at[int(up), plane])
    for k, (src, dst) in enumerate(whole):
        pltpu.make_async_copy(src, dst, wsem.at[k]).wait()
    for a, (src, dst) in enumerate([(px, PX), (pt, PT), (yv, Y), (pz, PZ), (gmv, GM), (gov, GO)]):
        pltpu.make_async_copy(src, dst, esem.at[a + 1]).wait()


def run_front(sz, x, go, win, tail, wout, norm, cw, cb, gate, lens, decay, bias, skip):
    n, g, t, rows, d, cs, tl, parts, fi = sz.n, sz.g, sz.t, sz.rows, sz.d, sz.cs, sz.tl, sz.parts, sz.fi
    dn, on = win.shape[0], wout.shape[0]
    any_ = pl.BlockSpec(memory_space=pl.ANY)
    vmem = pl.BlockSpec(memory_space=pltpu.VMEM)
    dma = pltpu.SemaphoreType.DMA
    shapes = dict(
        nrm=((t, rows, d), BF16), nt=((d, t * rows), BF16), go=((t, rows, d), BF16), px=((t, rows, cs), F32), pt=((t, rows, tl), F32), pz=((t, rows, cs), F32),
        y=((t, rows, cs), F32), gm=((t, rows, cs), F32), wx=((n, dn, cs), BF16), wz=((n, dn, cs), BF16), wt=((n, dn, tl), BF16),
        wo=((g, on, d), BF16), q=((2 * t, rows), F32), par=((8, d), F32), head=((8, LANES), F32), tile=((t, 8, LANES), F32),
    )
    out = lambda *names: [jax.ShapeDtypeStruct(*shapes[name]) for name in names]
    scr = lambda *names: [pltpu.VMEM(*shapes[name]) for name in names]
    return pl.pallas_call(
        functools.partial(front_kernel, sz),
        in_specs=[any_] * 5 + [vmem] * 8,
        out_specs=[any_] * 11 + [vmem] + [any_] * 3,
        out_shape=out("nt", "go", "px", "pt", "pz", "y", "gm", "wx", "wz", "wt", "wo", "q", "par", "head", "tile"),
        scratch_shapes=scr("nrm", "nrm", "go", "px", "pt", "pz", "y", "gm", "wx", "wz", "wt", "wo")
        + [pltpu.VMEM((8, LANES), F32), pltpu.VMEM((n, 8, LANES), F32)]
        + scr("par", "head", "q")
        + [pltpu.VMEM((t, 2 * t, rows), F32), pltpu.VMEM((t, 8, LANES), F32), pltpu.VMEM((d, rows), BF16)]
        + [dma((1,)), dma((t, parts)), dma((1,)), dma((t, parts)), dma((1,)), dma((t, 1)), dma((1,)), dma((1,)), dma((1,)), dma((1,)),
           dma((2, g)), dma((g,)), dma((2, g)), dma((g,)), dma((1,)), dma((1,)), dma((3, g)), dma((g,)), dma((2,)), dma((2,)),
           dma((1,)), dma((1,)), dma((7,)), dma((7,)), dma((7,))],
        compiler_params=pltpu.CompilerParams(collective_id=0, has_side_effects=True, vmem_limit_bytes=67043328),
        name="front",
    )(x, go, win, tail, wout, norm, cw, cb, gate, lens, decay, bias, skip)


class LineReduce:
    def __init__(self, sz, me, own, recv, send_sem, recv_sem):
        self.sz, self.me, self.own, self.recv, self.send_sem, self.recv_sem = sz, me, own, recv, send_sem, recv_sem

    def leg(self, step, up):
        g, last = self.me.g, self.sz.g - 1
        late = step - g if up else step - (last - g)
        p = last - late if up else late
        moves = (late >= 0) & ((p > g) if up else (p < g))
        p = jnp.clip(p, 0, last)
        inner = (g > 0) if up else (g < last)
        nxt = jnp.clip(g + 1 if up else g - 1, 0, last)
        there = p if up else jnp.where(p == nxt, last + 1, p)
        copy = lambda: remote(self.sz, self.own.at[p], self.recv.at[there], self.send_sem.at[p], self.recv_sem.at[there], nxt, self.me.t)
        return p, moves, inner, copy

    def step(self, step):
        for up in (True, False):
            p, moves, inner, copy = self.leg(step, up)

            @pl.when(moves & inner)
            def _(p=p):
                landed(self.recv.at[p], self.recv_sem.at[p])
                self.own[p] = (self.own[p].astype(F32) + self.recv[p].astype(F32)).astype(BF16)

            @pl.when(moves)
            def _(copy=copy):
                copy().start()

    def total(self, acc):
        g = self.me.g
        acc[...] = self.own[g].astype(F32)
        for k, there in ((g, g > 0), (self.sz.g, g < self.sz.g - 1)):
            @pl.when(there)
            def _(k=k):
                landed(self.recv.at[k], self.recv_sem.at[k])
                acc[...] += self.recv[k].astype(F32)

    def sent(self):
        for step in range(self.sz.g - 1):
            for up in (True, False):
                _, moves, _, copy = self.leg(step, up)

                @pl.when(moves)
                def _(copy=copy):
                    copy().wait_send()


class PlaneReduce:
    def __init__(self, sz, me, stage, r0, s, r1, r2, out, sems):
        self.sz, self.me, self.stage, self.r0, self.s, self.r1, self.r2, self.out = sz, me, stage, r0, s, r1, r2, out
        self.send0, self.recv0, self.send1, self.recv1, self.send2, self.recv2 = sems

    def chip(self, w):
        m = self.me
        return jnp.where(w == 0, m.fa, jnp.where(w == 1, m.fd, jnp.where(w == 2, m.fb, m.fi)))

    def slot(self, k):
        w = lax.rem(k, 4)
        core = jnp.where(k < 4, self.me.other, self.me.c)
        return self.chip(w) * 2 + core

    def put0(self, w):
        return remote(self.sz, self.stage.at[w], self.r0.at[w], self.send0.at[w], self.recv0.at[w], self.me.g, self.me.fi * 2 + self.me.other)

    def put1(self, w):
        return remote(self.sz, self.s.at[w], self.r1.at[w], self.send1.at[w], self.recv1.at[w], self.me.g, self.me.fa * 2 + self.me.c)

    def put2(self):
        return remote(self.sz, self.s.at[2], self.r2, self.send2.at[0], self.recv2.at[0], self.me.g, self.me.fb * 2 + self.me.c)

    def block(self, k, value):
        w = lax.rem(k, 4)

        @pl.when(k < 4)
        def _():
            self.stage[w] = value.astype(BF16)
            self.put0(w).start()

        @pl.when(k >= 4)
        def _():
            there = jnp.where(w == 0, 2, jnp.where(w == 2, 0, w))
            landed(self.r0.at[there], self.recv0.at[there])
            total = value + self.r0[there].astype(F32)

            @pl.when(w < 3)
            def _():
                self.s[w] = total.astype(BF16)

            @pl.when(w < 2)
            def _():
                self.put1(w).start()

            @pl.when(w == 3)
            def _():
                self.out(total, False)

    def middle(self):
        landed(self.r1.at[1], self.recv1.at[1])
        self.s[2] = (self.s[2].astype(F32) + self.r1[1].astype(F32)).astype(BF16)
        self.put2().start()

    def finish(self):
        landed(self.r1.at[0], self.recv1.at[0])
        landed(self.r2, self.recv2.at[0])
        self.out(self.r1[0].astype(F32) + self.r2[...].astype(F32), True)

    def sent0(self):
        for w in range(4):
            self.put0(w).wait_send()

    def sent(self):
        for w in range(2):
            self.put1(w).wait_send()
        self.put2().wait_send()


def back_kernel(sz, NT, GO, PX, PT, PZ, Y, GM, WX, WZ, WT, WO, q_ref, par, head, tile_ref,
                HS, GS, RAZ, RAX, GTL, GOUT, GSM,
                nt_, gov, ra, rx, rt_, wx, wz, wt, wo, mix, dz, dtv, dyv, r0h, sh, r1h, r2h, r0g, r1g, r2g, gs,
                dwz, dwx, dwo, rzz, rzx, acc, szz, szx, raz, rax, ro, gout, rtt, st, rtz, gtl, small, rs1, s1, rs2, gsm,
                lsem, asem, bsem, h0s, h0r, h1s, h1r, h2s, h2r, g0s, g0r, g1s, g1r, g2s, g2r, zzs, zzr, zxs, zxr, os_, or_, as_, ar_, ts, tr, us, ur, ss, sr, wsem):
    me = Place(sz)
    rows, cs, st_dim, taps, T, G, d = sz.rows, sz.cs, sz.state, sz.taps, sz.t, sz.g, sz.d
    tiles = cs // LANES
    half = rows // 2
    barrier = pltpu.get_barrier_semaphore()

    @pl.loop(1, sz.n)
    def _(step):
        there = lax.rem(me.i + step, sz.n)
        pl.semaphore_signal(barrier, inc=1, device_id=(lax.div(there, sz.p), lax.rem(there, sz.p)), device_id_type=pl.DeviceIdType.MESH)

    stage = gov.at[pl.ds(0, 4)]
    dx = mix
    pieces = d // cs

    class Folded:
        def at(self, c):
            return ra.at[c // (pieces // 2), pl.ds(c % (pieces // 2) * rows, rows)]

        def put(self, value, more):
            for c in range(pieces):
                part = value[:, c * cs : (c + 1) * cs]
                self.at(c)[...] = self.at(c)[...] + part if more else part

    hid = PlaneReduce(sz, me, stage, r0h, sh, r1h, r2h, Folded().put, (h0s, h0r, h1s, h1r, h2s, h2r))
    def put_gs(value, more):
        gs[...] = gs[...] + value if more else value

    gn = PlaneReduce(sz, me, stage, r0g, gov.at[pl.ds(4, 3)], r1g, r2g, put_gs, (g0s, g0r, g1s, g1r, g2s, g2r))

    def fetch_a(k):
        slot, par_ = hid.slot(k), lax.rem(k, 2)
        return [pltpu.make_async_copy(src.at[slot], ra.at[par_, pl.ds(a * rows, rows)], asem.at[par_]) for a, src in enumerate((PZ, Y, GM))]

    def fetch_b(k):
        slot, par_ = gn.slot(k), lax.rem(k, 2)
        return [pltpu.make_async_copy(PX.at[slot], rx.at[par_], bsem.at[0, par_]), pltpu.make_async_copy(PT.at[slot], rt_.at[par_], bsem.at[1, par_])]

    for k in range(2):
        for copy in fetch_a(jnp.int32(k)):
            copy.start()
    loads = [pltpu.make_async_copy(src, dst, lsem.at[k]) for k, (src, dst) in enumerate(((NT, nt_), (WO, wo), (GO, gov), (WX, wx), (WZ, wz), (WT, wt)))]
    for copy in loads[:1]:
        copy.start()
    for copy in fetch_b(jnp.int32(0)):
        copy.start()
    small[...] = jnp.zeros(small.shape, F32)

    def colsum(v):
        return jnp.sum(v, axis=0, keepdims=True)

    def silu_pair(v):
        s = jax.nn.sigmoid(v)
        return v * s, s * (1.0 + v * (1.0 - s))

    @pl.loop(0, T)
    def _(k):
        slot, par_ = hid.slot(k), lax.rem(k, 2)

        @pl.when(k == T // 2)
        def _():
            for copy in loads[1:]:
                copy.start()

        landed(ra.at[par_, pl.ds(0, 3 * rows)], asem.at[par_])
        pos = iota((rows, LANES), 0).astype(F32)
        valid = (segments(pos, ends_of(tile_ref[slot, taps + 3 : taps + 4, :], sz.seqs)) < sz.seqs).astype(F32)
        q1 = jnp.broadcast_to(q_ref[pl.ds(slot, 1), :], (LANES, rows)).T
        q2 = jnp.broadcast_to(q_ref[pl.ds(T + slot, 1), :], (LANES, rows)).T
        scale = lax.rsqrt(q1 / sz.di + EPS)
        pull = scale * scale * scale * q2 / sz.di
        for j in range(tiles):
            tile = slice(j * LANES, (j + 1) * LANES)
            zt, y, gm = (ra[par_, a * rows : (a + 1) * rows, tile] for a in range(3))
            gm = gm * valid
            gate = par[taps + 1 : taps + 2, tile]
            up, slope = silu_pair(zt)
            gated = y * up
            unit = gated * scale
            mix[slot, :, tile] = (unit * gate * valid).astype(BF16)
            small[sz.at_gate + j : sz.at_gate + j + 1, :] += colsum(gm * unit)
            dgated = scale * gm * gate - gated * pull
            dz[slot, :, tile] = (dgated * y * slope).astype(BF16)
            dyv[slot, :, tile] = dgated * up

        @pl.when(k + 2 < T)
        def _():
            for copy in fetch_a(k + 2):
                copy.start()

    def weight_grad(values, into):
        dn = sz.d // sz.n
        for at in range(0, sz.n, sz.n // 4):
            span = sz.n // 4 * dn
            got = nn(nt_[at * dn : at * dn + span, :], values[...].reshape(T * rows, values.shape[2]))
            for i in range(at, at + sz.n // 4):
                f, p = i // sz.p, i % sz.p
                fo, fi, z, c = f // sz.fi, f % sz.fi, p // 2, p % 2
                into[fo * sz.z + z, fi * 2 + c, :, 0 : got.shape[1]] = got[(i - at) * dn : (i - at + 1) * dn].astype(BF16)

    line_z = LineReduce(sz, me, dwz.at[:, :, :, pl.ds(0, cs)], rzz, zzs, zzr)
    line_x = LineReduce(sz, me, dwx, rzx, zxs, zxr)
    loads[0].wait()
    weight_grad(dz, dwz)
    pl.semaphore_wait(barrier, sz.n - 1)
    line_z.step(0)
    loads[1].wait()

    loads[2].wait()

    def o_copy(k):
        owner = me.t * G + k
        return pltpu.make_async_remote_copy(src_ref=dwo.at[k], dst_ref=ro.at[me.g], send_sem=os_.at[k], recv_sem=or_.at[me.g],
                                            device_id=(lax.div(owner, sz.p), lax.rem(owner, sz.p)), device_id_type=pl.DeviceIdType.MESH)

    for at in range(0, d, d // 3):
        got = tn(mix[...].reshape(T * rows, cs), gov[:, :, at : at + d // 3].reshape(T * rows, d // 3))
        for k in range(G):
            dwo[k, :, at : at + d // 3] = got[k * (cs // G) : (k + 1) * (cs // G)].astype(BF16)
    def out_sends():
        for k in range(G):
            @pl.when(t_differs(sz, me, k))
            def _(k=k):
                o_copy(k).start()

    @pl.loop(0, T)
    def _(k):
        hid.block(k, nn(mix[hid.slot(k)], wo[...].reshape(cs, d)))

    for copy in loads[3:]:
        copy.wait()

    low = iota((rows, LANES), 1) < sz.hd
    lane = iota((rows, LANES), 1)
    lead = lax.rem(LANES - sz.nh * me.t, LANES)
    quads = ((slice(0, half), slice(0, rows)), (slice(half, rows), slice(half, rows)))

    def between(k, *steps):
        @pl.when(k)
        def _():
            for step in steps:
                step()

    def scan_back(k):
        slot, par_ = gn.slot(k), lax.rem(k, 2)

        @pl.when(k + 1 < T)
        def _():
            for copy in fetch_b(k + 1):
                copy.start()

        landed(rx.at[par_], bsem.at[0, par_])
        landed(rt_.at[par_], bsem.at[1, par_])
        keeps, _, same = masks(rows, ends_of(tile_ref[slot, taps + 3 : taps + 4, :], sz.seqs), taps)

        def conv_pre(u, at):
            return conv_tile(u, par[0:taps, at : at + LANES], par[taps : taps + 1, at : at + LANES], keeps, taps)

        def conv_back(u, dact, dsilu, at):
            dpre = dact * dsilu
            tile = at // LANES
            row = sz.at_conv + tile * 8 if tile < tiles else sz.at_bc + (tile - tiles) * 8
            back = dpre * par[taps - 1 : taps, at : at + LANES]
            small[row + taps - 1 : row + taps, :] += colsum(dpre * u)
            small[row + taps : row + taps + 1, :] += colsum(dpre)
            for off in range(1, taps):
                kept = dpre * keeps[off - 1]
                tap = taps - 1 - off
                small[row + tap : row + tap + 1, :] += colsum(kept * pltpu.roll(u, off, 0))
                back = back + pltpu.roll(kept, rows - off, 0) * par[tap : tap + 1, at : at + LANES]
            return back

        ub, uc = rt_[par_, :, 0:st_dim], rt_[par_, :, st_dim : 2 * st_dim]
        bm, bslope = silu_pair(conv_pre(ub, cs))
        cm, cslope = silu_pair(conv_pre(uc, cs + st_dim))
        raw = pltpu.roll(rt_[par_, :, 2 * st_dim : 2 * st_dim + LANES], lead, 1) + head[0:1, :]
        dt = softplus(raw)
        rate = -jnp.exp(head[1:2, :])
        log_decay = jnp.dot(triangle(rows).astype(F32), dt * rate, precision=EXACT, preferred_element_type=F32)
        log_t = log_decay.T
        upper = iota((rows, rows), 1) >= iota((rows, rows), 0)
        drop = jnp.where(same & upper, 0.0, -jnp.inf)
        inner_t = three(nt, bm, cm)
        dcb = [jnp.zeros((half, rows), F32), jnp.zeros((half, half), F32)]
        ddt = jnp.zeros((rows, LANES), F32)
        cols = jnp.zeros((rows, LANES), F32)
        rowsums = jnp.zeros((LANES, rows), F32)
        lane_row = iota((LANES, rows), 0)
        for j in range(tiles):
            at = j * LANES
            tile = slice(at, at + LANES)
            dy = dyv[slot, :, tile]
            ux = rx[par_, :, tile]
            xa, xslope = silu_pair(conv_pre(ux, at))
            small[sz.at_head + 3 + j : sz.at_head + 4 + j, :] += colsum(dy * xa)
            dt2 = jnp.where(low, dt[:, 2 * j : 2 * j + 1], dt[:, 2 * j + 1 : 2 * j + 2])
            xd = xa * dt2
            dyh, dyl = split(dy)
            tops = []
            for e in range(2):
                h = 2 * j + e
                mine = low if e == 0 else jnp.logical_not(low)
                xh, xl = split(jnp.where(mine, xd, 0.0))
                dym = jnp.where(mine, dy, 0.0).astype(BF16)
                parts, psums, tsum = [], [], []
                for quad, (r, c) in enumerate(quads):
                    decay = jnp.exp(log_t[h : h + 1, c] - log_decay[r, h : h + 1] + drop[r, c])
                    df = (nt(xh[r], dyh[c]) + (nt(xh[r], dyl[c]) + nt(xl[r], dyh[c]))) * decay
                    dcb[quad] = dcb[quad] + df
                    p = df * inner_t[r, c]
                    psums.append(jnp.sum(p, axis=1, keepdims=True))
                    tsum.append(colsum(p))
                    parts.append(nn((decay * inner_t[r, c]).astype(BF16), dym[c]))
                cols = jnp.where(lane == h, jnp.concatenate(psums, axis=0), cols)
                tsum = tsum[0] + jnp.concatenate([jnp.zeros((1, half), F32), tsum[1]], axis=1)
                rowsums = jnp.where(lane_row == h, tsum, rowsums)
                tops.append(jnp.concatenate(parts, axis=0))
            dxd = tops[0] + tops[1]
            both = dxd * xa
            ddt = jnp.where(lane == 2 * j, jnp.sum(jnp.where(low, both, 0.0), axis=1, keepdims=True), ddt)
            ddt = jnp.where(lane == 2 * j + 1, jnp.sum(jnp.where(low, 0.0, both), axis=1, keepdims=True), ddt)
            skip2 = jnp.where(low[0:1], head[2:3, 2 * j : 2 * j + 1], head[2:3, 2 * j + 1 : 2 * j + 2])
            dx[slot, :, tile] = conv_back(ux, dxd * dt2 + dy * skip2, xslope, at).astype(BF16)

        ga = jnp.dot(upper.astype(F32), rowsums.T - cols, precision=EXACT, preferred_element_type=F32)
        ddt = ddt + ga * rate
        small[sz.at_head : sz.at_head + 1, :] += rate * colsum(ga * dt)
        draw = jnp.where(lane < sz.nh, ddt * jax.nn.sigmoid(raw), 0.0)
        small[sz.at_head + 1 : sz.at_head + 2, :] += colsum(draw)
        dtv[slot, :, 2 * st_dim : 2 * st_dim + LANES] = pltpu.roll(draw, sz.nh * me.t, 1).astype(BF16)
        top, bottom = dcb[0].astype(BF16), dcb[1].astype(BF16)
        bb, cb = bm.astype(BF16), cm.astype(BF16)
        db = jnp.concatenate([nn(top, cb), nn(bottom, cb[half:])], axis=0)
        dc = tn(top, bb[:half]) + jnp.concatenate([jnp.zeros((half, st_dim), F32), tn(bottom, bb[half:])], axis=0)
        dtv[slot, :, 0:st_dim] = conv_back(ub, db, bslope, cs).astype(BF16)
        dtv[slot, :, st_dim : 2 * st_dim] = conv_back(uc, dc, cslope, cs + st_dim).astype(BF16)
        between(k == 0, hid.sent0)
        gn.block(k, nt(dz[slot], wz[...].reshape(d, cs)) + nt(dx[slot], wx[...].reshape(d, cs)) + nt(dtv[slot], wt[...].reshape(d, sz.tl)))

    @pl.loop(0, T)
    def _(k):
        between(k == 0, lambda: line_z.step(1))
        between(k == 1, lambda: [line_z.step(step) for step in range(2, G - 1)], out_sends)
        between(k == 3, hid.middle)
        between(k == 6, hid.finish)
        scan_back(k)

    weight_grad(dx, dwx)
    line_x.step(0)
    line_z.total(acc)
    szz[...] = acc[...].astype(BF16)

    def hand(sums, into, k):
        for step in range(1, T):
            there = lax.rem(me.t + step, T)
            remote(sz, sums.at[there], into.at[me.t], as_.at[k], ar_.at[k], me.g, there).start()
        into[me.t] = sums[me.t]

    hand(szz, raz, 0)
    line_z.sent()
    dwt = dwz.at[:, :, :, pl.ds(0, sz.tl)]
    weight_grad(dtv, dwz)

    def t_copy(step):
        there = lax.rem(me.t + step, T)
        return [remote(sz, dwt.at[g, there], rtt.at[me.t, g], ts.at[0], tr.at[0], me.g, there) for g in range(G)]

    for step in range(1, T):
        for copy in t_copy(step):
            copy.start()

    for j in range(tiles):
        spot = iota((LANES, LANES), 1) == 2 * j + (iota((LANES, LANES), 0) >= sz.hd).astype(jnp.int32)
        part = jnp.dot(small[sz.at_head + 3 + j : sz.at_head + 4 + j, :], spot.astype(F32), precision=EXACT, preferred_element_type=F32)
        small[sz.at_head + 2 : sz.at_head + 3, :] += part
    s_line = lambda step: remote(sz, small, rs1.at[me.g], ss.at[0], sr.at[0], lax.rem(me.g + step, G), me.t)
    for step in range(1, G):
        s_line(step).start()

    saves = [pltpu.make_async_copy(Folded().at(c), HS.at[:, pl.ds(c * cs, cs)], wsem.at[7 + c]) for c in range(pieces)]
    for copy in saves:
        copy.start()
    gn.middle()
    line_x.step(1)

    mine = lax.div(me.i, G) == me.t

    @pl.when(mine)
    def _():
        gout[...] = dwo[lax.rem(me.i, G)].astype(F32)

    @pl.when(jnp.logical_not(mine))
    def _():
        gout[...] = jnp.zeros(gout.shape, F32)

    for g in range(G):
        @pl.when(jnp.logical_not(mine & (me.g == g)))
        def _(g=g):
            landed(ro.at[g], or_.at[g])
            gout[...] += ro[g].astype(F32)

    saves.append(pltpu.make_async_copy(gout, GOUT, wsem.at[1]))
    saves[-1].start()
    landed(rs1.at[pl.ds(0, G - 1)], sr.at[0])
    total = small[...]
    for step in range(1, G):
        total = total + rs1[lax.rem(me.g + step, G)]
    s1[...] = total
    rs2[me.t] = total
    s_plane = lambda step: remote(sz, s1, rs2.at[me.t], ss.at[1], sr.at[1], me.g, lax.rem(me.t + step, T))
    for step in range(1, T):
        s_plane(step).start()

    for step in range(2, G - 1):
        line_x.step(step)
    landed(rtt.at[pl.ds(0, T - 1)], tr.at[0])
    for g in range(G):
        total = dwt[g, me.t].astype(F32)
        for step in range(1, T):
            total = total + rtt[lax.rem(me.t + step, T), g].astype(F32)
        st[g] = total.astype(BF16)
    t_line = lambda step: remote(sz, st.at[lax.rem(me.g + step, G)], rtz.at[me.g], us.at[0], ur.at[0], lax.rem(me.g + step, G), me.t)
    for step in range(1, G):
        t_line(step).start()
    gn.finish()
    saves.append(pltpu.make_async_copy(gs, GS, wsem.at[2]))
    saves[-1].start()
    landed(rs2.at[pl.ds(0, T - 1)], sr.at[1])
    total = rs2[0, 0 : sz.common]
    for t in range(1, T):
        total = total + rs2[t, 0 : sz.common]
    gsm[0 : sz.common] = total
    width = sz.small_rows - sz.common
    for t in range(T):
        gsm[sz.common + t * width : sz.common + (t + 1) * width] = rs2[t, sz.common :]
    saves.append(pltpu.make_async_copy(gsm, GSM, wsem.at[3]))
    saves[-1].start()

    line_x.total(acc)
    szx[...] = acc[...].astype(BF16)
    hand(szx, rax, 1)
    landed(raz.at[pl.ds(0, T - 1)], ar_.at[0])
    saves.append(pltpu.make_async_copy(raz, RAZ, wsem.at[4]))
    saves[-1].start()
    landed(rtz.at[pl.ds(0, G - 1)], ur.at[0])
    total = st[me.g].astype(F32)
    for step in range(1, G):
        total = total + rtz[lax.rem(me.g + step, G)].astype(F32)
    gtl[...] = total
    saves.append(pltpu.make_async_copy(gtl, GTL, wsem.at[5]))
    saves[-1].start()
    landed(rax.at[pl.ds(0, T - 1)], ar_.at[1])
    saves.append(pltpu.make_async_copy(rax, RAX, wsem.at[6]))
    saves[-1].start()

    hid.sent()
    gn.sent0()
    gn.sent()
    line_x.sent()
    for k in range(G):
        @pl.when(t_differs(sz, me, k))
        def _(k=k):
            o_copy(k).wait_send()
    for k in range(2):
        landed(raz.at[pl.ds(0, T - 1)], as_.at[k])
    landed(rtt.at[pl.ds(0, T - 1)], ts.at[0])
    landed(rtz.at[pl.ds(0, G - 1)], us.at[0])
    landed(rs1.at[pl.ds(0, G - 1)], ss.at[0])
    landed(rs2.at[pl.ds(0, T - 1)], ss.at[1])
    for copy in saves:
        copy.wait()


def run_back(sz, nt, go, px, pt, pz, y, gm, wx, wz, wt, wo, q, par, head, tile):
    n, g, t, rows, d, cs, tl = sz.n, sz.g, sz.t, sz.rows, sz.d, sz.cs, sz.tl
    dn, on = d // n, sz.di // n
    any_ = pl.BlockSpec(memory_space=pl.ANY)
    vmem = pl.BlockSpec(memory_space=pltpu.VMEM)
    dma = pltpu.SemaphoreType.DMA
    b = lambda *s: pltpu.VMEM(s, BF16)
    f = lambda *s: pltpu.VMEM(s, F32)
    sr = sz.small_rows
    total_rows = sz.common + t * (sr - sz.common)
    plane = lambda: [dma((4,)), dma((4,)), dma((2,)), dma((2,)), dma((1,)), dma((1,))]
    return pl.pallas_call(
        functools.partial(back_kernel, sz),
        in_specs=[any_] * 11 + [vmem] * 4,
        out_specs=[any_] * 7,
        out_shape=[
            jax.ShapeDtypeStruct((rows, d), F32),
            jax.ShapeDtypeStruct((rows, d), F32),
            jax.ShapeDtypeStruct((t, dn, cs), BF16),
            jax.ShapeDtypeStruct((t, dn, cs), BF16),
            jax.ShapeDtypeStruct((dn, tl), F32),
            jax.ShapeDtypeStruct((on, d), F32),
            jax.ShapeDtypeStruct((total_rows, LANES), F32),
        ],
        scratch_shapes=[
            b(d, t * rows), b(t, rows, d), f(2, max(3 * rows, -(-d // (2 * cs)) * rows), cs), f(2, rows, cs), f(2, rows, tl), b(n, dn, cs), b(n, dn, cs), b(n, dn, tl), b(g, on, d),
            b(t, rows, cs), b(t, rows, cs), b(t, rows, tl), f(t, rows, cs),
            b(4, rows, d), b(3, rows, d), b(2, rows, d), b(rows, d), b(4, rows, d), b(2, rows, d), b(rows, d), f(rows, d),
            b(g, t, dn, max(cs, tl)), b(g, t, dn, cs), b(g, on, d), b(g + 1, t, dn, cs), b(g + 1, t, dn, cs), f(t, dn, cs),
            b(t, dn, cs), b(t, dn, cs), b(t, dn, cs), b(t, dn, cs), b(g, on, d), f(on, d), b(t, g, dn, tl), b(g, dn, tl), b(g, dn, tl), f(dn, tl),
            f(sr, LANES), f(g, sr, LANES), f(sr, LANES), f(t, sr, LANES), f(total_rows, LANES),
            dma((6,)), dma((2,)), dma((2, 2)), *plane(), *plane(), dma((g,)), dma((g + 1,)), dma((g,)), dma((g + 1,)), dma((g,)), dma((g,)),
            dma((2,)), dma((2,)), dma((1,)), dma((1,)), dma((1,)), dma((1,)), dma((2,)), dma((2,)), dma((7 + d // cs,)),
        ],
        compiler_params=pltpu.CompilerParams(collective_id=1, has_side_effects=True, vmem_limit_bytes=67043328),
        name="back",
    )(nt, go, px, pt, pz, y, gm, wx, wz, wt, wo, q, par, head, tile)


def finish_kernel(sz, HS, GS, X, GO, RAZ, RAX, GTL, GOUT, gsm, WIN, norm, par, HID, GIN, gnorm, GW, gcw, gcb, ggate, GWO, gdecay, gbias, gskip,
                  hs, gs, x, go, raz, rax, gtl, gout, win, hidden, gin, gw, sem):
    me = Place(sz)
    cs, T, taps = sz.cs, sz.t, sz.taps
    tiles = cs // LANES
    width = sz.small_rows - sz.common
    loads = [pltpu.make_async_copy(src, dst, sem.at[k]) for k, (src, dst) in enumerate(
        ((X, x), (HS, hs), (GS, gs), (GO, go), (GOUT, gout), (WIN, win), (RAZ, raz), (RAX, rax), (GTL, gtl)))]
    for copy in loads:
        copy.start()
    saves = [pltpu.make_async_copy(src, dst, sem.at[9 + k]) for k, (src, dst) in enumerate(((hidden, HID), (gin, GIN), (gout, GWO), (gw, GW)))]
    loads[0].wait()
    loads[1].wait()
    xb = x[...].astype(F32)
    hidden[...] = (xb + hs[...]).astype(BF16)
    saves[0].start()
    loads[2].wait()
    loads[3].wait()
    scale = lax.rsqrt(jnp.mean(xb * xb, axis=1, keepdims=True) + EPS)
    dxhat = gs[...] * par[taps + 2 : taps + 3, 0 : sz.d]
    inner = jnp.mean(dxhat * xb, axis=1, keepdims=True)
    gin[...] = go[...].astype(F32) + scale * (dxhat - xb * (scale * scale * inner))
    saves[1].start()
    loads[4].wait()
    saves[2].start()
    for copy in loads[5:]:
        copy.wait()
    dot = jnp.zeros((gw.shape[0], LANES), F32)
    for side, ref in ((0, raz), (1, rax)):
        for t in range(T):
            at = side * sz.di + t * cs
            piece = ref[t].astype(F32)
            gw[:, at : at + cs] = piece
            both = piece * win[:, at : at + cs].astype(F32)
            for j in range(tiles):
                dot = dot + both[:, j * LANES : (j + 1) * LANES]
    at = 2 * sz.di
    gw[:, at:] = gtl[:, 0 : sz.tail]
    saves[3].start()
    last = jnp.sum(gtl[:, 0 : sz.tail] * win[:, at:].astype(F32), axis=1, keepdims=True)
    dot = jnp.sum(dot, axis=1, keepdims=True) + last
    gnorm[...] = jnp.broadcast_to(dot, (dot.shape[0], LANES)).T[0:1, :] / norm[...].astype(F32)

    def window(row_of, rows, per):
        first = lax.div(me.i * per, LANES)
        off = lax.rem(me.i * per, LANES)
        wide = jnp.concatenate([gsm[pl.ds(row_of(first), rows), :], gsm[pl.ds(row_of(first + 1), rows), :]], axis=1)
        return pltpu.roll(wide, lax.rem(2 * LANES - off, 2 * LANES), 1)

    def conv_row(q):
        q = jnp.clip(q, 0, T * tiles + 2 * sz.state // LANES - 1)
        inside = sz.common + lax.div(q, tiles) * width + 8 * lax.rem(q, tiles)
        return pl.multiple_of(jnp.where(q < T * tiles, inside, sz.at_bc + 8 * (q - T * tiles)), 8)

    def gate_row(q):
        q = jnp.clip(q, 0, T * tiles - 1)
        return sz.common + lax.div(q, tiles) * width + sz.at_gate - sz.common + lax.rem(q, tiles)

    conv = window(conv_row, 8, gcb.shape[1])
    gcw[...] = conv[0:taps, 0 : gcw.shape[1]]
    gcb[...] = conv[taps : taps + 1, 0 : gcb.shape[1]]

    def spread(q):
        return jnp.broadcast_to(gsm[pl.ds(gate_row(q), 1), :], (8, LANES))

    first, off = lax.div(me.i * ggate.shape[1], LANES), lax.rem(me.i * ggate.shape[1], LANES)
    wide = jnp.concatenate([spread(first), spread(first + 1)], axis=1)
    ggate[...] = pltpu.roll(wide, lax.rem(2 * LANES - off, 2 * LANES), 1)[0:1, 0 : ggate.shape[1]]
    for t in range(T):
        row = sz.common + t * width + sz.at_head - sz.common
        for k, ref in enumerate((gdecay, gbias, gskip)):
            ref[:, t * sz.nh : (t + 1) * sz.nh] = gsm[row + k : row + k + 1, 0 : sz.nh]
    for copy in saves:
        copy.wait()


def run_finish(sz, hs, gs, x, go, raz, rax, gtl, gout, gsm, win, norm, par, kn, cn):
    vmem, any_ = pl.BlockSpec(memory_space=pltpu.VMEM), pl.BlockSpec(memory_space=pltpu.HBM)
    o = lambda *s: jax.ShapeDtypeStruct(s, F32)
    dn = win.shape[0]
    same = lambda a: pltpu.VMEM(a.shape, a.dtype)
    return pl.pallas_call(
        functools.partial(finish_kernel, sz),
        in_specs=[any_] * 8 + [vmem, any_, vmem, vmem],
        out_specs=[any_, any_, vmem, any_, vmem, vmem, vmem, any_, vmem, vmem, vmem],
        out_shape=[jax.ShapeDtypeStruct(x.shape, BF16), o(*x.shape), o(1, dn), o(*win.shape), o(sz.taps, cn), o(1, cn), o(1, kn), o(*gout.shape),
                   o(1, sz.heads), o(1, sz.heads), o(1, sz.heads)],
        scratch_shapes=[same(hs), same(gs), same(x), same(go), same(raz), same(rax), same(gtl), same(gout), same(win),
                        same(x), same(gs), pltpu.VMEM(win.shape, F32), pltpu.SemaphoreType.DMA((13,))],
        compiler_params=pltpu.CompilerParams(vmem_limit_bytes=67043328),
        name="finish",
    )(hs, gs, x, go, raz, rax, gtl, gout, gsm, win, norm, par)


def sizes(mesh, hidden, lengths, in_proj, conv_weight, gate_gain, decay_log):
    sz = Sizes()
    sz.f, sz.p = mesh.shape["fsdp"], mesh.shape["dp"]
    sz.n = sz.f * sz.p
    sz.rows, sz.d = hidden.shape
    sz.seqs = lengths.shape[1]
    sz.conv, sz.taps = conv_weight.shape[0] * sz.n, conv_weight.shape[1]
    sz.di = gate_gain.shape[0] * sz.n
    sz.state = (sz.conv - sz.di) // 2
    sz.heads = decay_log.shape[0]
    sz.hd = sz.di // sz.heads
    sz.fi = math.gcd(sz.f, sz.di // (2 * LANES))
    sz.t = 2 * sz.fi
    sz.z = sz.p // 2
    sz.g = sz.f // sz.fi * sz.z
    sz.aligned = sz.f == sz.fi
    sz.cs, sz.nh = sz.di // sz.t, sz.heads // sz.t
    sz.tail = in_proj.shape[1] - 2 * sz.di
    sz.tl = -(-sz.tail // LANES) * LANES
    sz.parts, sz.rparts = 2, 2
    sz.part_rows = sz.rows // sz.parts
    small_layout(sz)
    return sz


def local(mesh, hidden_in, lengths, norm_gain, in_proj, conv_weight, conv_bias, gate_gain, out_proj, decay_log, step_bias, skip_gain, grad_out):
    sz = sizes(mesh, hidden_in, lengths, in_proj, conv_weight, gate_gain, decay_log)
    di = sz.di
    dn, cn, kn = norm_gain.shape[0], conv_bias.shape[0], gate_gain.shape[0]

    tail = jnp.pad(in_proj[:, 2 * di :], ((0, 0), (0, sz.tl - sz.tail)))
    row = lambda a: a.reshape(1, -1)
    turned, go_all, px, pt, pz, y, gm, wx, wz, wt, wo, q, par, head, tile = run_front(
        sz, hidden_in, grad_out, in_proj, tail, out_proj, row(norm_gain), conv_weight.T, row(conv_bias), row(gate_gain), lengths,
        row(decay_log), row(step_bias), row(skip_gain))
    hs, gs, raz, rax, gtl, gout, gsm = run_back(sz, turned, go_all, px, pt, pz, y, gm, wx, wz, wt, wo, q, par, head, tile)
    hidden, gin, gnorm, gw, gcw, gcb, ggate, gwo, gdecay, gbias, gskip = run_finish(
        sz, hs, gs, hidden_in, grad_out, raz, rax, gtl, gout, gsm, in_proj, row(norm_gain), par, kn, cn)
    flat = lambda a: a.reshape(-1)
    return hidden, gin, flat(gnorm), gw, gcw.T, flat(gcb), flat(ggate), gwo, flat(gdecay), flat(gbias), flat(gskip)


def solution(mesh):
    both = ("fsdp", "dp")
    wide, flat, free = P(both, None), P(both), P()
    in_specs = (wide, wide, flat, wide, wide, flat, flat, wide, free, free, free, wide)
    out_specs = (wide, wide, flat, wide, wide, flat, flat, wide, free, free, free)
    return jax.shard_map(functools.partial(local, mesh), mesh=mesh, in_specs=in_specs, out_specs=out_specs, check_vma=False)
```

```python
import functools
import math

import jax
import jax.numpy as jnp
from jax import lax
from jax.experimental import pallas as pl
from jax.experimental.pallas import tpu as pltpu
from jax.sharding import PartitionSpec as P

EPS = 1e-05
F32 = jnp.float32
BF16 = jnp.bfloat16
EXACT = lax.Precision.HIGHEST
LANES = 128
LOG2E = math.log2(math.e)


def nn(a, b):
    return lax.dot_general(a, b, (((1,), (0,)), ((), ())), preferred_element_type=F32)


def nt(a, b):
    return lax.dot_general(a, b, (((1,), (1,)), ((), ())), preferred_element_type=F32)


def tn(a, b):
    return lax.dot_general(a, b, (((0,), (0,)), ((), ())), preferred_element_type=F32)


def iota(shape, dim):
    return lax.broadcasted_iota(jnp.int32, shape, dim)


def conv_tile(u, weights, bias, keeps, taps):
    pre = bias + u * weights[taps - 1 : taps, :]
    for off in range(1, taps):
        pre = pre + pltpu.roll(u, off, 0) * keeps[off - 1] * weights[taps - 1 - off : taps - off, :]
    return pre


def softplus(v):
    return jnp.maximum(v, 0.0) + jnp.log1p(jnp.exp(-jnp.abs(v)))


def split(a):
    hi = a.astype(BF16)
    return hi, (a - hi.astype(F32)).astype(BF16)


def three(product, a, b):
    ah, al = split(a)
    bh, bl = split(b)
    return product(ah, bh) + (product(ah, bl) + product(al, bh))


def running(mask, a):
    hi, mid = split(a)
    rest = a - hi.astype(F32) - mid.astype(F32)
    ones = jnp.where(mask, 1.0, 0.0).astype(BF16)
    return nn(ones, hi) + (nn(ones, mid) + nn(ones, rest.astype(BF16)))


class Sizes:
    pass


def up8(count):
    return -(-count // 8) * 8


def small_layout(sz):
    tiles = sz.cs // LANES
    sz.at_bc = 0
    sz.common = 2 * sz.state // LANES * 8
    sz.at_conv = sz.common
    sz.at_gate = sz.at_conv + tiles * 8
    sz.at_head = sz.at_gate + up8(tiles)
    sz.small_rows = sz.at_head + up8(3 + tiles)


def device_of(sz, g, t):
    return (lax.div(g, sz.z) * sz.fi + lax.div(t, 2), lax.rem(g, sz.z) * 2 + lax.rem(t, 2))


def index_of(sz, g, t):
    f, p = device_of(sz, g, t)
    return f * sz.p + p


class Place:
    def __init__(self, sz):
        f, p = lax.axis_index("fsdp"), lax.axis_index("dp")
        fi, z = lax.rem(f, sz.fi), lax.div(p, 2)
        self.c = lax.rem(p, 2)
        self.g = lax.div(f, sz.fi) * sz.z + z
        self.t = fi * 2 + self.c
        self.i = f * sz.p + p
        u, v = lax.rem(fi, 2), lax.div(fi, 2)
        across, along = v * 2 + 1 - u, (1 - v) * 2 + u
        self.fi = fi
        self.fa = across * (1 - self.c) + along * self.c
        self.fb = along * (1 - self.c) + across * self.c
        self.fd = sz.fi - 1 - fi
        self.other = 1 - self.c


def remote(sz, src, dst, send, recv, g, t):
    return pltpu.make_async_remote_copy(
        src_ref=src, dst_ref=dst, send_sem=send, recv_sem=recv, device_id=device_of(sz, g, t), device_id_type=pl.DeviceIdType.MESH
    )


def landed(ref, sem):
    pltpu.make_async_copy(ref, ref, sem).wait()


def greet_all(sz, me):
    barrier = pltpu.get_barrier_semaphore()

    @pl.loop(1, sz.n)
    def _(step):
        there = lax.rem(me.i + step, sz.n)
        pl.semaphore_signal(barrier, inc=1, device_id=(lax.div(there, sz.p), lax.rem(there, sz.p)), device_id_type=pl.DeviceIdType.MESH)

    pl.semaphore_wait(barrier, sz.n - 1)


def greet_near(sz, me):
    barrier = pltpu.get_barrier_semaphore()
    near = [(me.g, lax.rem(me.t + step, sz.t)) for step in range(1, sz.t)] + [(lax.rem(me.g + step, sz.g), me.t) for step in range(1, sz.g)]
    for g, t in near:
        pl.semaphore_signal(barrier, inc=1, device_id=device_of(sz, g, t), device_id_type=pl.DeviceIdType.MESH)
    pl.semaphore_wait(barrier, len(near))


class PlaneGather:
    def __init__(self, sz, me, parts, own, views, gauge, bulk, send, recv):
        self.sz, self.me, self.parts, self.own, self.views, self.gauge, self.bulk, self.send, self.recv = sz, me, parts, own, views, gauge, bulk, send, recv
        self.a, self.b, self.d = me.fa * 2 + me.c, me.fb * 2 + me.c, me.fd * 2 + me.c
        self.pair = me.fi * 2 + me.other

    def push(self, kind, part):
        slot = (self.me.t, self.me.t, self.me.t, self.a, self.a, self.b, self.d)[kind]
        target = (self.a, self.b, self.pair, self.b, self.pair, self.pair, self.pair)[kind]
        views = self.views(slot, part)
        for src, dst in zip(self.own(part) if kind < 3 else views, views):
            remote(self.sz, src, dst, self.send.at[0], self.recv.at[slot, part], self.me.g, target).start()

    def arrived(self, slot, part):
        landed(self.gauge, self.recv.at[slot, part])

    def start(self, part):
        for kind in range(3):
            self.push(kind, part)

    def relay(self, part):
        self.arrived(self.a, part)
        self.push(3, part)
        self.push(4, part)
        self.arrived(self.b, part)
        self.push(5, part)

    def relay_far(self, part):
        self.arrived(self.d, part)
        self.push(6, part)

    def sent(self):
        landed(self.bulk, self.send.at[0])


def t_differs(sz, me, k):
    return me.t * sz.g + k != me.i


def select_rows(sz, packed, channel, per):
    n = packed.shape[0]
    wide = channel.shape[1]
    owner = jnp.floor((channel + 0.5) * (1.0 / per))
    place = channel - owner * per
    pick = (iota((LANES, wide), 0).astype(F32) == place).astype(BF16)
    spread = nn(packed.reshape(n * 8, LANES).astype(BF16), pick).reshape(n, 8, wide)
    over = lambda v, by: jnp.floor((v + 0.5) * (1.0 / by))
    spot = iota((n, 8, LANES), 0).astype(F32)
    rank = over(spot, sz.g)
    plane = spot - sz.g * rank
    fi, fo = over(rank, 2), over(plane, sz.z)
    device = ((fo * sz.fi + fi) * sz.z + plane - sz.z * fo) * 2 + rank - 2 * fi
    total = jnp.zeros((8, wide), F32)
    parts = []
    for at in range(0, wide, LANES):
        hit = device == owner[None, :, at : at + LANES]
        parts.append(jnp.sum(jnp.where(hit, spread[:, :, at : at + LANES], 0.0), axis=0))
    return jnp.concatenate(parts, axis=1)


def lanes_of(wide):
    return iota((1, wide), 1).astype(F32)


def slot_of(me, k):
    flip = lambda bit, other: bit + other - 2 * bit * other
    v, u, c = lax.div(me.t, 4), lax.rem(lax.div(me.t, 2), 2), me.c
    kv, ku, kc = lax.div(k, 4), lax.rem(lax.div(k, 2), 2), lax.rem(k, 2)
    return (flip(v, kv) * 2 + flip(u, ku)) * 2 + flip(c, kc)


def ends_of(row, count):
    ends, total = [], jnp.zeros((1, 1), F32)
    for slot in range(count):
        total = total + row[:, slot : slot + 1]
        ends.append(total)
    return ends


def segments(pos, ends):
    total = jnp.zeros(pos.shape, F32)
    for end in ends:
        total = total + (pos >= end).astype(F32)
    return total


def masks(rows, ends, taps):
    pos = iota((rows, LANES), 0).astype(F32)
    seg = segments(pos, ends)
    keeps = []
    for off in range(1, taps):
        same = (segments(pos - off, ends) == seg) & (pos >= off)
        keeps.append(same.astype(F32))
    valid = (seg < len(ends)).astype(F32)
    seg_row = segments(lanes_of(rows), ends)
    same = jnp.concatenate([(seg == seg_row[:, at : at + LANES]) for at in range(0, rows, LANES)], axis=1)
    return keeps, valid, same


def triangle(rows):
    return iota((rows, rows), 0) >= iota((rows, rows), 1)


def front_kernel(sz, x, go, win, tail, wout, norm, cw, cb, gate, lens, decay, bias, skip,
                 NT, GO, PX, PT, PZ, Y, GM, WX, WZ, WT, WO, Q, PAR, HEAD, TILE,
                 xv, nv, gov, px, pt, pz, yv, gmv, wxv, wzv, wtv, wov, pack, smv, par, head, qv, qr, tilev, flip,
                 xsend, xrecv, gsend, grecv, wsend, wrecv, axsend, axrecv, azsend, azrecv, zxsend, zxrecv, zzsend, zzrecv,
                 tsend, trecv, osend, orecv, ssend, srecv, qsend, qrecv, lsem, esem, wsem):
    me = Place(sz)
    cs, rows, G, T, st, taps = sz.cs, sz.rows, sz.g, sz.t, sz.state, sz.taps
    tiles = cs // LANES
    pack[...] = jnp.zeros(pack.shape, F32)
    dn, cn, kn = norm.shape[1], cb.shape[1], gate.shape[1]
    pack[0:taps, 0:cn] = cw[...].astype(F32)
    pack[taps : taps + 1, 0:cn] = cb[...].astype(F32)
    pack[taps + 1 : taps + 2, 0:kn] = gate[...].astype(F32)
    pack[taps + 2 : taps + 3, 0:dn] = norm[...].astype(F32)
    pack[taps + 3 : taps + 4, 0 : sz.seqs] = lens[...].astype(F32)
    (greet_near if sz.aligned else greet_all)(sz, me)

    tile_of = lambda g, t: smv.at[t * G + g]

    def pack_line(step):
        return remote(sz, pack, tile_of(me.g, me.t), ssend.at[0], srecv.at[0], lax.rem(me.g + step, G), me.t)

    def pack_plane(step):
        mine = smv.at[pl.ds(me.t * G, G)]
        return remote(sz, mine, mine, ssend.at[1], srecv.at[1], me.g, lax.rem(me.t + step, T))

    def columns(half, t):
        return win.at[:, pl.ds(pl.multiple_of(half * sz.di + t * cs, LANES), cs)]

    def exchange(half, step):
        there = lax.rem(me.t + step, T)
        wv, send, recv = ((wzv, azsend, azrecv), (wxv, axsend, axrecv))[half]
        return remote(sz, columns(half, there), wv.at[me.i], send.at[0], recv.at[0], me.g, there)

    def tail_copy(step):
        there = lax.rem(me.g + step, G)
        return remote(sz, tail, wtv.at[me.i], tsend.at[0], trecv.at[0], there, me.t)

    for step in range(1, G):
        tail_copy(step).start()
        pack_line(step).start()
    for step in range(1, T):
        exchange(1, step).start()

    part = lambda ref, k: ref.at[pl.ds(k * sz.part_rows, sz.part_rows)]
    gx = PlaneGather(sz, me, sz.parts, lambda k: [part(x, k)], lambda s, k: [part(xv.at[s], k)], part(xv.at[0], 0), xv.at[pl.ds(0, T - 1)], xsend, xrecv)
    gg = PlaneGather(sz, me, sz.parts, lambda k: [part(go, k)], lambda s, k: [part(gov.at[s], k)], part(gov.at[0], 0), gov.at[pl.ds(0, T - 1)], gsend, grecv)
    tails_of = lambda s, k: [wtv.at[index_of(sz, jnp.int32(g), s)] for g in range(G)]
    gt = PlaneGather(sz, me, 1, lambda k: tails_of(me.t, k), tails_of, wtv.at[pl.ds(0, G)], wtv.at[pl.ds(0, (T - 1) * G)], wsend, wrecv)

    gx.start(0)
    owner_t, piece = lax.div(me.i, G), lax.rem(me.i, G)

    def out_copy(g):
        return remote(sz, wout, wov.at[piece], osend.at[2, g], orecv.at[piece], g, owner_t)

    def out_targets():
        planes = (me.g,) if sz.aligned else tuple(range(G))
        for g in planes:
            elsewhere = (owner_t != me.t) | (me.g != g)
            yield elsewhere, (lambda g=g: out_copy(jnp.int32(0) + g))

    def out_line(step, half, up):
        plane = me.g - step if up else me.g + step
        first = 2 * plane - me.c * sz.z
        have = (plane >= 0 if up else plane < G) & (first >= 0) & (first < G)
        more = (me.g < G - 1) if up else (me.g > 0)
        k = jnp.clip(first, 0, G - 2) + half
        nxt = jnp.clip(me.g + 1 if up else me.g - 1, 0, G - 1)
        copy = lambda: remote(sz, wov.at[k], wov.at[k], osend.at[int(up), k], orecv.at[k], nxt, me.t)
        return have, more, k, copy

    def out_advance(step):
        for half in range(2):
            if step == 0:
                have, _, k, _ = out_line(0, half, True)

                @pl.when(have & t_differs(sz, me, k))
                def _(k=k):
                    landed(wov.at[k], orecv.at[k])
            for up in (True, False):
                have, more, k, copy = out_line(step, half, up)
                if step > 0:
                    @pl.when(have)
                    def _(k=k):
                        landed(wov.at[k], orecv.at[k])
                if step < G - 1:
                    @pl.when(have & more)
                    def _(copy=copy):
                        copy().start()

    def out_steps(*steps):
        if sz.aligned:
            for step in steps:
                out_advance(step)

    for elsewhere, copy in out_targets():
        @pl.when(elsewhere)
        def _(copy=copy):
            copy().start()

    ins = [
        pltpu.make_async_copy(columns(1, me.t), wxv.at[me.i], lsem.at[0]),
        pltpu.make_async_copy(columns(0, me.t), wzv.at[me.i], lsem.at[1]),
        pltpu.make_async_copy(tail, wtv.at[me.i], lsem.at[2]),
        pltpu.make_async_copy(pack, tile_of(me.g, me.t), lsem.at[3]),
        pltpu.make_async_copy(x, xv.at[me.t], lsem.at[4]),
        pltpu.make_async_copy(go, gov.at[me.t], lsem.at[5]),
    ]
    for copy in ins:
        copy.start()
    for copy in ins:
        copy.wait()

    @pl.when(owner_t == me.t)
    def _():
        copy = pltpu.make_async_copy(wout, wov.at[piece], lsem.at[6])
        copy.start()
        copy.wait()

    head[...] = jnp.zeros(head.shape, F32)
    head[0:1, 0 : sz.heads] = bias[...]
    head[1:2, 0 : sz.heads] = decay[...]
    head[2:3, 0 : sz.heads] = skip[...]
    lead = lax.rem(LANES - sz.nh * me.t, LANES)
    head[...] = pltpu.roll(head[...], lead, 1)

    landed(smv.at[pl.ds(0, G - 1)], srecv.at[0])
    landed(wtv.at[pl.ds(0, G - 1)], trecv.at[0])
    for step in range(1, T):
        pack_plane(step).start()
    gt.start(0)
    for step in range(1, T):
        exchange(0, step).start()

    def arrive(half):
        wv, _, recv = ((wzv, azsend, azrecv), (wxv, axsend, axrecv))[half]
        landed(wv.at[pl.ds(0, T - 1)], recv.at[0])

    def line(half, step, up):
        wv, send, recv = ((wzv, zzsend, zzrecv), (wxv, zxsend, zxrecv))[half]
        plane = me.g - step if up else me.g + step
        have = (plane >= 0) if up else (plane < G)
        more = (me.g < G - 1) if up else (me.g > 0)
        plane = jnp.clip(plane, 0, G - 1)
        nxt = jnp.clip(me.g + 1 if up else me.g - 1, 0, G - 1)

        def push():
            for fi in range(sz.fi):
                block = wv.at[pl.ds(index_of(sz, plane, jnp.int32(2 * fi)), 2)]
                remote(sz, block, block, send.at[int(up), plane], recv.at[plane], nxt, me.t).start()

        return have, more, plane, push, wv.at[pl.ds(0, T)], send, recv

    def advance(half, step):
        for up in (True, False):
            have, more, plane, push, gauge, _, recv = line(half, step, up)
            if step > 0:
                @pl.when(have)
                def _(gauge=gauge, recv=recv, plane=plane):
                    landed(gauge, recv.at[plane])
            if step < G - 1:
                pl.when(have & more)(push)

    arrive(1)
    advance(1, 0)
    advance(1, 1)
    landed(smv.at[pl.ds(0, (T - 1) * G)], srecv.at[1])
    packed = smv[...]
    ch = lanes_of(cs + 2 * st)
    start_ch = (me.t * cs).astype(F32)
    ch = jnp.where(ch < cs, ch + start_ch, ch + (sz.di - cs))
    par[:, 0 : cs + 2 * st] = select_rows(sz, packed, ch, cn)
    picked = select_rows(sz, packed, lanes_of(cs) + start_ch, kn)
    par[taps + 1 : taps + 2, 0:cs] = picked[taps + 1 : taps + 2]
    gains = select_rows(sz, packed, lanes_of(sz.d), dn)
    par[taps + 2 : taps + 3, 0 : sz.d] = gains[taps + 2 : taps + 3]

    def normalize(k):
        slot = slot_of(me, k)
        xb = xv[slot].astype(F32)
        mean = jnp.mean(xb * xb, axis=1, keepdims=True)
        nrm = (xb * lax.rsqrt(mean + EPS) * par[taps + 2 : taps + 3, 0 : sz.d]).astype(BF16)
        nv[slot] = nrm
        flip[...] = nrm.T
        turn = pltpu.make_async_copy(flip, NT.at[:, pl.ds(pl.multiple_of(slot * rows, LANES), rows)], esem.at[0])
        turn.start()
        turn.wait()

    def wait_pair(gather, k):
        slot = slot_of(me, k)
        for p in range(sz.parts):
            gather.arrived(slot, p)

    gt.relay(0)
    for p in range(1, sz.parts):
        gx.start(p)
    normalize(jnp.int32(0))
    wait_pair(gx, jnp.int32(1))
    normalize(jnp.int32(1))
    gx.relay(0)
    for step in range(2, G - 1):
        advance(1, step)
    arrive(0)
    advance(0, 0)
    gt.relay_far(0)
    advance(1, G - 1)
    for fi in (me.fi, me.fa, me.fb, me.fd):
        gt.arrived(fi * 2 + me.other, 0)

    low = iota((rows, LANES), 1) < sz.hd
    tri = triangle(rows)
    half_rows = rows // 2

    def scan(k):
        slot = slot_of(me, k)

        @pl.when((k > 2) & (lax.rem(k, 2) == 1))
        def _():
            wait_pair(gx, k)

        @pl.when(k > 1)
        def _():
            normalize(k)

        keeps, _, same = masks(rows, ends_of(smv[slot * G + me.g, taps + 3 : taps + 4, :], sz.seqs), taps)
        nrm = nv[slot]
        pxv = nn(nrm, wxv[...].reshape(sz.d, cs))
        ptl = nn(nrm, wtv[...].reshape(sz.d, sz.tl))
        px[slot] = pxv
        pltpu.make_async_copy(px.at[slot], PX.at[slot], esem.at[1]).start()

        def act(u, at):
            return jax.nn.silu(conv_tile(u, par[0:taps, at : at + LANES], par[taps : taps + 1, at : at + LANES], keeps, taps))

        bm = act(ptl[:, 0:st], cs)
        cm = act(ptl[:, st : 2 * st], cs + st)
        raw = pltpu.roll(ptl[:, 2 * st : 2 * st + LANES], lead, 1) + head[0:1, :]
        dt = softplus(raw)
        rate = -jnp.exp(head[1:2, :])
        log_decay = running(tri, dt * rate) * LOG2E
        pt[slot, :, 0 : 2 * st] = ptl[:, 0 : 2 * st]
        for a, kept in enumerate((raw, dt, log_decay)):
            pt[slot, :, 2 * st + a * LANES : 2 * st + (a + 1) * LANES] = kept
        pltpu.make_async_copy(pt.at[slot], PT.at[slot], esem.at[2]).start()
        log_t = log_decay.T
        drop = jnp.where(same & tri, 0.0, -jnp.inf)
        inner = three(nt, cm, bm)
        for j in range(tiles):
            at = j * LANES
            xa = act(pxv[:, at : at + LANES], at)
            dt2 = jnp.where(low, dt[:, 2 * j : 2 * j + 1], dt[:, 2 * j + 1 : 2 * j + 2])
            xd = xa * dt2
            tops, bottoms = [], []
            for e in range(2):
                h = 2 * j + e
                mine = low if e == 0 else jnp.logical_not(low)
                xm = jnp.where(mine, xd, 0.0).astype(BF16)
                for r, wide, into in ((slice(0, half_rows), half_rows, tops), (slice(half_rows, rows), rows, bottoms)):
                    spread = log_decay[r, h : h + 1] - log_t[h : h + 1, 0:wide]
                    f = (jnp.exp2(spread + drop[r, 0:wide]) * inner[r, 0:wide]).astype(BF16)
                    into.append(nn(f, xm[0:wide]))
            y = jnp.concatenate([tops[0] + tops[1], bottoms[0] + bottoms[1]], axis=0)
            skip2 = jnp.where(low[0:1], head[2:3, 2 * j : 2 * j + 1], head[2:3, 2 * j + 1 : 2 * j + 2])
            yv[slot, :, at : at + LANES] = y + xa * skip2
        pltpu.make_async_copy(yv.at[slot], Y.at[slot], esem.at[3]).start()

    def between(k, *steps):
        @pl.when(k)
        def _():
            for step in steps:
                step()

    whole = [(wxv, WX), (wtv, WT), (par, PAR), (head, HEAD), (wzv, WZ), (wov, WO), (tilev, TILE)]

    def save(*picked):
        for k in picked:
            pltpu.make_async_copy(*whole[k], wsem.at[k]).start()

    save(0, 1, 2, 3)

    @pl.loop(0, T)
    def _(k):
        between(k == 2, lambda: advance(0, 1), lambda: out_steps(0), lambda: [gx.relay(p) for p in range(1, sz.parts)],
                lambda: [gg.start(p) for p in range(sz.parts)])
        between(k == 3, lambda: gx.relay_far(0))
        between(k == 4, lambda: [advance(0, step) for step in range(2, G - 1)])
        between(k == 6, lambda: [gx.relay_far(p) for p in range(1, sz.parts)], lambda: out_steps(1))
        between(k == 7, lambda: [gg.relay(p) for p in range(sz.parts)])
        scan(k)

    advance(0, G - 1)
    out_steps(*range(2, G - 1))
    save(4)

    @pl.loop(0, T)
    def _(k):
        slot = slot_of(me, k)
        pz[slot] = nn(nv[slot], wzv[...].reshape(sz.d, cs))
        pltpu.make_async_copy(pz.at[slot], PZ.at[slot], esem.at[4]).start()

    out_steps(G - 1)
    if not sz.aligned:
        for k in range(G):
            @pl.when(t_differs(sz, me, k))
            def _(k=k):
                landed(wov.at[k], orecv.at[k])

    save(5)

    @pl.loop(0, T)
    def _(k):
        slot = slot_of(me, k)

        between(k == 6, lambda: [gg.relay_far(p) for p in range(sz.parts)])
        between(lax.rem(k, 2) == 1, lambda: wait_pair(gg, k))
        pos = iota((rows, LANES), 0).astype(F32)
        seg = segments(pos, ends_of(smv[slot * G + me.g, taps + 3 : taps + 4, :], sz.seqs))
        valid = (seg < sz.seqs).astype(F32)
        tilev[slot] = smv[slot * G + me.g]
        zt = pz[slot]
        gm = nt(gov[slot], wov[...].reshape(cs, sz.d))
        gmv[slot] = gm
        pltpu.make_async_copy(gmv.at[slot], GM.at[slot], esem.at[5]).start()
        pltpu.make_async_copy(gov.at[slot], GO.at[slot], esem.at[6]).start()
        q1 = jnp.zeros((rows, LANES), F32)
        q2 = jnp.zeros((rows, LANES), F32)
        for j in range(tiles):
            tile = slice(j * LANES, (j + 1) * LANES)
            gated = yv[slot, :, tile] * (zt[:, tile] * jax.nn.sigmoid(zt[:, tile]))
            q1 = q1 + gated * gated
            q2 = q2 + gated * gm[:, tile] * par[taps + 1 : taps + 2, tile]
        q2 = q2 * valid
        lane = iota((rows, LANES), 1)
        stats = jnp.where(lane == 0, jnp.sum(q1, axis=1, keepdims=True), jnp.sum(q2, axis=1, keepdims=True)).T
        qv[pl.ds(slot, 1), :] = stats[0:1, :]
        qv[pl.ds(T + slot, 1), :] = stats[1:2, :]

    save(6)

    def q_copy(step):
        return remote(sz, qv, qr.at[me.t], qsend.at[0], qrecv.at[0], me.g, lax.rem(me.t + step, T))

    for step in range(1, T):
        q_copy(step).start()

    landed(qr.at[pl.ds(0, T - 1)], qrecv.at[0])
    total = qv[...]
    for step in range(1, T):
        total = total + qr[lax.rem(me.t + step, T)]
    Q[...] = total

    landed(qr.at[pl.ds(0, T - 1)], qsend.at[0])
    landed(wxv.at[pl.ds(0, T - 1)], axsend.at[0])
    landed(wzv.at[pl.ds(0, T - 1)], azsend.at[0])
    landed(wtv.at[pl.ds(0, G - 1)], tsend.at[0])
    landed(smv.at[pl.ds(0, G - 1)], ssend.at[0])
    landed(smv.at[pl.ds(0, (T - 1) * G)], ssend.at[1])
    for gather in (gx, gg, gt):
        gather.sent()
    for elsewhere, copy in out_targets():
        @pl.when(elsewhere)
        def _(copy=copy):
            copy().wait_send()
    if sz.aligned:
        for step in range(G - 1):
            for half in range(2):
                for up in (True, False):
                    have, more, _, copy = out_line(step, half, up)

                    @pl.when(have & more)
                    def _(copy=copy):
                        copy().wait_send()
    for half in range(2):
        for step in range(G - 1):
            for up in (True, False):
                have, more, plane, _, gauge, send, _ = line(half, step, up)

                @pl.when(have & more)
                def _(gauge=gauge, send=send, plane=plane, up=up):
                    landed(gauge, send.at[int(up), plane])
    for k, (src, dst) in enumerate(whole):
        pltpu.make_async_copy(src, dst, wsem.at[k]).wait()
    for a, (src, dst) in enumerate([(px, PX), (pt, PT), (yv, Y), (pz, PZ), (gmv, GM), (gov, GO)]):
        pltpu.make_async_copy(src, dst, esem.at[a + 1]).wait()


def run_front(sz, x, go, win, tail, wout, norm, cw, cb, gate, lens, decay, bias, skip):
    n, g, t, rows, d, cs, tl, parts, fi = sz.n, sz.g, sz.t, sz.rows, sz.d, sz.cs, sz.tl, sz.parts, sz.fi
    dn, on = win.shape[0], wout.shape[0]
    any_ = pl.BlockSpec(memory_space=pl.ANY)
    vmem = pl.BlockSpec(memory_space=pltpu.VMEM)
    dma = pltpu.SemaphoreType.DMA
    shapes = dict(
        nrm=((t, rows, d), BF16), nt=((d, t * rows), BF16), go=((t, rows, d), BF16), px=((t, rows, cs), F32), pt=((t, rows, 2 * sz.state + 3 * LANES), F32), pz=((t, rows, cs), F32),
        y=((t, rows, cs), F32), gm=((t, rows, cs), F32), wx=((n, dn, cs), BF16), wz=((n, dn, cs), BF16), wt=((n, dn, tl), BF16),
        wo=((g, on, d), BF16), q=((2 * t, rows), F32), par=((8, d), F32), head=((8, LANES), F32), tile=((t, 8, LANES), F32),
    )
    out = lambda *names: [jax.ShapeDtypeStruct(*shapes[name]) for name in names]
    scr = lambda *names: [pltpu.VMEM(*shapes[name]) for name in names]
    return pl.pallas_call(
        functools.partial(front_kernel, sz),
        in_specs=[any_] * 5 + [vmem] * 8,
        out_specs=[any_] * 11 + [vmem] + [any_] * 3,
        out_shape=out("nt", "go", "px", "pt", "pz", "y", "gm", "wx", "wz", "wt", "wo", "q", "par", "head", "tile"),
        scratch_shapes=scr("nrm", "nrm", "go", "px", "pt", "pz", "y", "gm", "wx", "wz", "wt", "wo")
        + [pltpu.VMEM((8, LANES), F32), pltpu.VMEM((n, 8, LANES), F32)]
        + scr("par", "head", "q")
        + [pltpu.VMEM((t, 2 * t, rows), F32), pltpu.VMEM((t, 8, LANES), F32), pltpu.VMEM((d, rows), BF16)]
        + [dma((1,)), dma((t, parts)), dma((1,)), dma((t, parts)), dma((1,)), dma((t, 1)), dma((1,)), dma((1,)), dma((1,)), dma((1,)),
           dma((2, g)), dma((g,)), dma((2, g)), dma((g,)), dma((1,)), dma((1,)), dma((3, g)), dma((g,)), dma((2,)), dma((2,)),
           dma((1,)), dma((1,)), dma((7,)), dma((7,)), dma((7,))],
        compiler_params=pltpu.CompilerParams(collective_id=0, has_side_effects=True, vmem_limit_bytes=67043328),
        name="front",
    )(x, go, win, tail, wout, norm, cw, cb, gate, lens, decay, bias, skip)


class LineReduce:
    def __init__(self, sz, me, own, recv, send_sem, recv_sem):
        self.sz, self.me, self.own, self.recv, self.send_sem, self.recv_sem = sz, me, own, recv, send_sem, recv_sem

    def piece(self, p):
        return self.own.at[pl.ds(p * self.sz.t, self.sz.t)]

    def leg(self, step, up):
        g, last = self.me.g, self.sz.g - 1
        late = step - g if up else step - (last - g)
        p = last - late if up else late
        moves = (late >= 0) & ((p > g) if up else (p < g))
        p = jnp.clip(p, 0, last)
        inner = (g > 0) if up else (g < last)
        nxt = jnp.clip(g + 1 if up else g - 1, 0, last)
        there = p if up else jnp.where(p == nxt, last + 1, p)
        copy = lambda: remote(self.sz, self.piece(p), self.recv.at[there], self.send_sem.at[p], self.recv_sem.at[there], nxt, self.me.t)
        return p, moves, inner, copy

    def step(self, step):
        for up in (True, False):
            p, moves, inner, copy = self.leg(step, up)

            @pl.when(moves & inner)
            def _(p=p):
                landed(self.recv.at[p], self.recv_sem.at[p])
                piece = self.piece(p)
                piece[...] = (piece[...].astype(F32) + self.recv[p].astype(F32)).astype(BF16)

            @pl.when(moves)
            def _(copy=copy):
                copy().start()

    def total(self, acc):
        g = self.me.g
        acc[...] = self.piece(g)[...].astype(F32)
        for k, there in ((g, g > 0), (self.sz.g, g < self.sz.g - 1)):
            @pl.when(there)
            def _(k=k):
                landed(self.recv.at[k], self.recv_sem.at[k])
                acc[...] += self.recv[k].astype(F32)

    def sent(self):
        for step in range(self.sz.g - 1):
            for up in (True, False):
                _, moves, _, copy = self.leg(step, up)

                @pl.when(moves)
                def _(copy=copy):
                    copy().wait_send()


class PlaneReduce:
    def __init__(self, sz, me, stage, r0, s, r1, r2, out, sems):
        self.sz, self.me, self.stage, self.r0, self.s, self.r1, self.r2, self.out = sz, me, stage, r0, s, r1, r2, out
        self.send0, self.recv0, self.send1, self.recv1, self.send2, self.recv2 = sems

    def chip(self, w):
        m = self.me
        return jnp.where(w == 0, m.fa, jnp.where(w == 1, m.fd, jnp.where(w == 2, m.fb, m.fi)))

    def slot(self, k):
        w = lax.rem(k, 4)
        core = jnp.where(k < 4, self.me.other, self.me.c)
        return self.chip(w) * 2 + core

    def put0(self, w):
        return remote(self.sz, self.stage.at[w], self.r0.at[w], self.send0.at[w], self.recv0.at[w], self.me.g, self.me.fi * 2 + self.me.other)

    def put1(self, w):
        return remote(self.sz, self.s.at[w], self.r1.at[w], self.send1.at[w], self.recv1.at[w], self.me.g, self.me.fa * 2 + self.me.c)

    def put2(self):
        return remote(self.sz, self.s.at[2], self.r2, self.send2.at[0], self.recv2.at[0], self.me.g, self.me.fb * 2 + self.me.c)

    def block(self, k, value):
        w = lax.rem(k, 4)

        @pl.when(k < 4)
        def _():
            self.stage[w] = value.astype(BF16)
            self.put0(w).start()

        @pl.when(k >= 4)
        def _():
            there = jnp.where(w == 0, 2, jnp.where(w == 2, 0, w))
            landed(self.r0.at[there], self.recv0.at[there])
            total = value + self.r0[there].astype(F32)

            @pl.when(w < 3)
            def _():
                self.s[w] = total.astype(BF16)

            @pl.when(w < 2)
            def _():
                self.put1(w).start()

            @pl.when(w == 3)
            def _():
                self.out(total, False)

    def middle(self):
        landed(self.r1.at[1], self.recv1.at[1])
        self.s[2] = (self.s[2].astype(F32) + self.r1[1].astype(F32)).astype(BF16)
        self.put2().start()

    def finish(self):
        landed(self.r1.at[0], self.recv1.at[0])
        landed(self.r2, self.recv2.at[0])
        self.out(self.r1[0].astype(F32) + self.r2[...].astype(F32), True)

    def sent0(self):
        for w in range(4):
            self.put0(w).wait_send()

    def sent1(self):
        for w in range(2):
            self.put1(w).wait_send()

    def sent2(self):
        self.put2().wait_send()


def back_kernel(sz, NT, GO, PX, PT, PZ, Y, GM, WX, WZ, WT, WO, q_ref, par, head, tile_ref,
                HS, GS, RAZ, RAX, GTL, GOUT, GSM,
                nt_, gov, ra, rx, rt_, wall, wo, dp, dyv, r0h, r1h, r2h, r0g, r1g, r2g, gs,
                dwz, dwx, dwo, rzz, rzx, acc, szz, raz, rax, ro, gout, rtp, rtt, st, rtz, gtl, small, rs1, s1, rs2, gsm,
                lsem, asem, bsem, h0s, h0r, h1s, h1r, h2s, h2r, g0s, g0r, g1s, g1r, g2s, g2r, zzs, zzr, zxs, zxr, os_, or_, as_, ar_, ts, tr, us, ur, ss, sr, wsem):
    me = Place(sz)
    rows, cs, st_dim, taps, T, G, d = sz.rows, sz.cs, sz.state, sz.taps, sz.t, sz.g, sz.d
    tiles = cs // LANES
    half = rows // 2
    barrier = pltpu.get_barrier_semaphore()

    @pl.loop(1, sz.n)
    def _(step):
        there = lax.rem(me.i + step, sz.n)
        pl.semaphore_signal(barrier, inc=1, device_id=(lax.div(there, sz.p), lax.rem(there, sz.p)), device_id_type=pl.DeviceIdType.MESH)

    stage, sums = gov.at[pl.ds(0, 4)], gov.at[pl.ds(4, 3)]
    pieces = d // cs

    class Folded:
        def at(self, c):
            return ra.at[c // (pieces // 2), pl.ds(c % (pieces // 2) * rows, rows)]

        def put(self, value, more):
            for c in range(pieces):
                part = value[:, c * cs : (c + 1) * cs]
                self.at(c)[...] = self.at(c)[...] + part if more else part

    hid = PlaneReduce(sz, me, stage, r0h, sums, r1h, r2h, Folded().put, (h0s, h0r, h1s, h1r, h2s, h2r))
    def put_gs(value, more):
        gs[...] = gs[...] + value if more else value

    gn = PlaneReduce(sz, me, stage, r0g, sums, r1g, r2g, put_gs, (g0s, g0r, g1s, g1r, g2s, g2r))

    def fetch_a(k):
        slot, par_ = hid.slot(k), lax.rem(k, 2)
        return [pltpu.make_async_copy(src.at[slot], ra.at[par_, pl.ds(a * rows, rows)], asem.at[par_]) for a, src in enumerate((PZ, Y, GM))]

    def fetch_b(k):
        slot, par_ = gn.slot(k), lax.rem(k, 2)
        return [pltpu.make_async_copy(PX.at[slot], rx.at[par_], bsem.at[0, par_]), pltpu.make_async_copy(PT.at[slot], rt_.at[par_], bsem.at[1, par_])]

    for k in range(2):
        for copy in fetch_a(jnp.int32(k)):
            copy.start()
    loads = [pltpu.make_async_copy(src, dst, lsem.at[k]) for k, (src, dst) in enumerate((
        (NT, nt_), (WO, wo), (GO, gov), (WX, wall.at[:, :, pl.ds(cs, cs)]), (WZ, wall.at[:, :, pl.ds(0, cs)]), (WT, wall.at[:, :, pl.ds(2 * cs, sz.tl)])))]
    for copy in fetch_b(jnp.int32(0)):
        copy.start()
    small[...] = jnp.zeros(small.shape, F32)

    def colsum(v):
        return jnp.sum(v, axis=0, keepdims=True)

    def silu_pair(v):
        s = jax.nn.sigmoid(v)
        return v * s, s * (1.0 + v * (1.0 - s))

    def between(k, *steps):
        @pl.when(k)
        def _():
            for step in steps:
                step()

    @pl.loop(0, T)
    def _(k):
        slot, par_ = hid.slot(k), lax.rem(k, 2)

        @pl.when(k == T // 2)
        def _():
            loads[0].start()

        landed(ra.at[par_, pl.ds(0, 3 * rows)], asem.at[par_])
        pos = iota((rows, LANES), 0).astype(F32)
        valid = (segments(pos, ends_of(tile_ref[slot, taps + 3 : taps + 4, :], sz.seqs)) < sz.seqs).astype(F32)
        q1 = jnp.broadcast_to(q_ref[pl.ds(slot, 1), :], (LANES, rows)).T
        q2 = jnp.broadcast_to(q_ref[pl.ds(T + slot, 1), :], (LANES, rows)).T
        scale = lax.rsqrt(q1 / sz.di + EPS)
        pull = scale * scale * scale * q2 / sz.di
        for j in range(tiles):
            at = j * LANES
            tile = slice(at, at + LANES)
            zt, y, gm = (ra[par_, a * rows : (a + 1) * rows, tile] for a in range(3))
            gm = gm * valid
            gate = par[taps + 1 : taps + 2, tile]
            up, slope = silu_pair(zt)
            gated = y * up
            unit = gated * scale
            dp[slot, :, cs + at : cs + at + LANES] = (unit * gate * valid).astype(BF16)
            small[sz.at_gate + j : sz.at_gate + j + 1, :] += colsum(gm * unit)
            dgated = scale * gm * gate - gated * pull
            dp[slot, :, tile] = (dgated * y * slope).astype(BF16)
            dyv[slot, :, tile] = dgated * up

        @pl.when(k + 2 < T)
        def _():
            for copy in fetch_a(k + 2):
                copy.start()

    for copy in loads[1:3]:
        copy.start()

    def weight_grad(first, wide, into, place):
        dn = sz.d // sz.n
        for at in range(0, sz.n, sz.n // 4):
            span = sz.n // 4 * dn
            got = nn(nt_[at * dn : at * dn + span, :], dp[:, :, first : first + wide].reshape(T * rows, wide))
            for i in range(at, at + sz.n // 4):
                f, p = i // sz.p, i % sz.p
                fo, fi, z, c = f // sz.fi, f % sz.fi, p // 2, p % 2
                into[place(fo * sz.z + z, fi * 2 + c), :, 0:wide] = got[(i - at) * dn : (i - at + 1) * dn].astype(BF16)

    line_z = LineReduce(sz, me, dwz.at[:, :, pl.ds(0, cs)], rzz, zzs, zzr)
    line_x = LineReduce(sz, me, dwx, rzx, zxs, zxr)
    loads[0].wait()
    by_plane, by_rank = lambda g, t: g * T + t, lambda g, t: t * G + g
    weight_grad(0, cs, dwz, by_plane)
    for copy in loads[3:]:
        copy.start()
    pl.semaphore_wait(barrier, sz.n - 1)
    line_z.step(0)
    loads[1].wait()

    loads[2].wait()

    def o_copy(k):
        owner = me.t * G + k
        return pltpu.make_async_remote_copy(src_ref=dwo.at[k], dst_ref=ro.at[me.g], send_sem=os_.at[k], recv_sem=or_.at[me.g],
                                            device_id=(lax.div(owner, sz.p), lax.rem(owner, sz.p)), device_id_type=pl.DeviceIdType.MESH)

    for at in range(0, d, d // 3):
        got = tn(dp[:, :, cs : 2 * cs].reshape(T * rows, cs), gov[:, :, at : at + d // 3].reshape(T * rows, d // 3))
        for k in range(G):
            dwo[k, :, at : at + d // 3] = got[k * (cs // G) : (k + 1) * (cs // G)].astype(BF16)
    def out_sends():
        for k in range(G):
            @pl.when(t_differs(sz, me, k))
            def _(k=k):
                o_copy(k).start()

    @pl.loop(0, T)
    def _(k):
        hid.block(k, nn(dp[hid.slot(k), :, cs : 2 * cs], wo[...].reshape(cs, d)))

    for copy in loads[3:]:
        copy.wait()

    low = iota((rows, LANES), 1) < sz.hd
    lane = iota((rows, LANES), 1)
    lead = lax.rem(LANES - sz.nh * me.t, LANES)
    quads = ((slice(0, half), slice(0, rows)), (slice(half, rows), slice(half, rows)))

    def scan_back(k):
        slot, par_ = gn.slot(k), lax.rem(k, 2)

        @pl.when(k + 1 < T)
        def _():
            for copy in fetch_b(k + 1):
                copy.start()

        landed(rx.at[par_], bsem.at[0, par_])
        landed(rt_.at[par_], bsem.at[1, par_])
        keeps, _, same = masks(rows, ends_of(tile_ref[slot, taps + 3 : taps + 4, :], sz.seqs), taps)

        def conv_pre(u, at):
            return conv_tile(u, par[0:taps, at : at + LANES], par[taps : taps + 1, at : at + LANES], keeps, taps)

        def conv_back(u, dact, dsilu, at):
            dpre = dact * dsilu
            tile = at // LANES
            row = sz.at_conv + tile * 8 if tile < tiles else sz.at_bc + (tile - tiles) * 8
            back = dpre * par[taps - 1 : taps, at : at + LANES]
            small[row + taps - 1 : row + taps, :] += colsum(dpre * u)
            small[row + taps : row + taps + 1, :] += colsum(dpre)
            for off in range(1, taps):
                kept = dpre * keeps[off - 1]
                tap = taps - 1 - off
                small[row + tap : row + tap + 1, :] += colsum(kept * pltpu.roll(u, off, 0))
                back = back + pltpu.roll(kept, rows - off, 0) * par[tap : tap + 1, at : at + LANES]
            return back

        ub, uc = rt_[par_, :, 0:st_dim], rt_[par_, :, st_dim : 2 * st_dim]
        bm, bslope = silu_pair(conv_pre(ub, cs))
        cm, cslope = silu_pair(conv_pre(uc, cs + st_dim))
        raw, dt, log_decay = (rt_[par_, :, 2 * st_dim + a * LANES : 2 * st_dim + (a + 1) * LANES] for a in range(3))
        rate = -jnp.exp(head[1:2, :])
        log_t = log_decay.T
        upper = iota((rows, rows), 1) >= iota((rows, rows), 0)
        drop = jnp.where(same & upper, 0.0, -jnp.inf)
        inner_t = three(nt, bm, cm)
        dcb = [jnp.zeros((half, rows), F32), jnp.zeros((half, half), F32)]
        ddt = jnp.zeros((rows, LANES), F32)
        cols = jnp.zeros((rows, LANES), F32)
        rowsums = jnp.zeros((up8(sz.nh), rows), F32)
        lane_row = iota((up8(sz.nh), rows), 0)
        for j in range(tiles):
            at = j * LANES
            tile = slice(at, at + LANES)
            dy = dyv[slot, :, tile]
            ux = rx[par_, :, tile]
            xa, xslope = silu_pair(conv_pre(ux, at))
            small[sz.at_head + 3 + j : sz.at_head + 4 + j, :] += colsum(dy * xa)
            dt2 = jnp.where(low, dt[:, 2 * j : 2 * j + 1], dt[:, 2 * j + 1 : 2 * j + 2])
            xd = xa * dt2
            dyh, dyl = split(dy)
            xh, xl = split(xd)
            left = jnp.concatenate([xh, xl, xh], axis=1)
            none = jnp.zeros((), BF16)
            tops = []
            for e in range(2):
                h = 2 * j + e
                mine = low if e == 0 else jnp.logical_not(low)
                dym, dyr = jnp.where(mine, dyh, none), jnp.where(mine, dyl, none)
                right = jnp.concatenate([dym, dym, dyr], axis=1)
                parts, psums, tsum = [], [], []
                for quad, (r, c) in enumerate(quads):
                    decay = jnp.exp2(log_t[h : h + 1, c] - log_decay[r, h : h + 1] + drop[r, c])
                    df = nt(left[r], right[c]) * decay
                    dcb[quad] = dcb[quad] + df
                    p = df * inner_t[r, c]
                    psums.append(jnp.sum(p, axis=1, keepdims=True))
                    tsum.append(colsum(p))
                    parts.append(nn((decay * inner_t[r, c]).astype(BF16), dym[c]))
                cols = jnp.where(lane == h, jnp.concatenate(psums, axis=0), cols)
                tsum = tsum[0] + jnp.concatenate([jnp.zeros((1, half), F32), tsum[1]], axis=1)
                rowsums = jnp.where(lane_row == h, tsum, rowsums)
                tops.append(jnp.concatenate(parts, axis=0))
            dxd = tops[0] + tops[1]
            both = dxd * xa
            ddt = jnp.where(lane == 2 * j, jnp.sum(jnp.where(low, both, 0.0), axis=1, keepdims=True), ddt)
            ddt = jnp.where(lane == 2 * j + 1, jnp.sum(jnp.where(low, 0.0, both), axis=1, keepdims=True), ddt)
            skip2 = jnp.where(low[0:1], head[2:3, 2 * j : 2 * j + 1], head[2:3, 2 * j + 1 : 2 * j + 2])
            dp[slot, :, cs + at : cs + at + LANES] = conv_back(ux, dxd * dt2 + dy * skip2, xslope, at).astype(BF16)

        rowsums = jnp.concatenate([rowsums, jnp.zeros((LANES - up8(sz.nh), rows), F32)], axis=0)
        ga = running(upper, rowsums.T - cols)
        ddt = ddt + ga * rate
        small[sz.at_head : sz.at_head + 1, :] += rate * colsum(ga * dt)
        draw = jnp.where(lane < sz.nh, ddt * jax.nn.sigmoid(raw), 0.0)
        small[sz.at_head + 1 : sz.at_head + 2, :] += colsum(draw)
        dp[slot, :, 2 * cs + 2 * st_dim : 2 * cs + 2 * st_dim + LANES] = pltpu.roll(draw, sz.nh * me.t, 1).astype(BF16)
        top, bottom = dcb[0].astype(BF16), dcb[1].astype(BF16)
        bb, cb = bm.astype(BF16), cm.astype(BF16)
        db = jnp.concatenate([nn(top, cb), nn(bottom, cb[half:])], axis=0)
        dc = tn(top, bb[:half]) + jnp.concatenate([jnp.zeros((half, st_dim), F32), tn(bottom, bb[half:])], axis=0)
        dp[slot, :, 2 * cs : 2 * cs + st_dim] = conv_back(ub, db, bslope, cs).astype(BF16)
        dp[slot, :, 2 * cs + st_dim : 2 * cs + 2 * st_dim] = conv_back(uc, dc, cslope, cs + st_dim).astype(BF16)
        between(k == 0, hid.sent0)
        between(k == 4, hid.sent1)
        between(k == 6, hid.sent2)
        gn.block(k, nt(dp[slot], wall[...].reshape(d, 2 * cs + sz.tl)))

    @pl.loop(0, T)
    def _(k):
        between(k == 0, lambda: line_z.step(1))
        between(k == 2, lambda: [line_z.step(step) for step in range(2, G - 1)], out_sends)
        between(k == 4, hid.middle)
        between(k == 7, hid.finish)
        scan_back(k)

    weight_grad(cs, cs, dwx, by_plane)
    line_x.step(0)
    line_z.total(acc)
    szz[...] = acc[...].astype(BF16)

    def hand(sums, into, k):
        for step in range(1, T):
            there = lax.rem(me.t + step, T)
            remote(sz, sums.at[there], into.at[me.t], as_.at[k], ar_.at[k], me.g, there).start()
        into[me.t] = sums[me.t]

    hand(szz, raz, 0)
    line_z.sent()
    gn.middle()
    weight_grad(2 * cs, sz.tl, dwz, by_rank)

    tails = lambda t: dwz.at[pl.ds(t * G, G), :, pl.ds(0, sz.tl)]
    for fi in range(sz.fi):
        remote(sz, tails(2 * fi + me.other), rtp.at[fi], ts.at[0], tr.at[0], me.g, me.fi * 2 + me.other).start()
    line_x.step(1)

    for j in range(tiles):
        spot = iota((LANES, LANES), 1) == 2 * j + (iota((LANES, LANES), 0) >= sz.hd).astype(jnp.int32)
        part = jnp.dot(small[sz.at_head + 3 + j : sz.at_head + 4 + j, :], spot.astype(F32), precision=EXACT, preferred_element_type=F32)
        small[sz.at_head + 2 : sz.at_head + 3, :] += part
    s_line = lambda step: remote(sz, small, rs1.at[me.g], ss.at[0], sr.at[0], lax.rem(me.g + step, G), me.t)
    for step in range(1, G):
        s_line(step).start()

    saves = [pltpu.make_async_copy(Folded().at(c), HS.at[:, pl.ds(c * cs, cs)], wsem.at[7 + c]) for c in range(pieces)]
    for copy in saves:
        copy.start()
    landed(rtp, tr.at[0])
    for fi in (me.fa, me.fb, me.fd, me.fi):
        mine = tails(2 * fi + me.c)
        mine[...] = (mine[...].astype(F32) + rtp[fi].astype(F32)).astype(BF16)
    for fi in (me.fd, me.fa, me.fb):
        remote(sz, tails(2 * fi + me.c), rtt.at[me.fi], ts.at[1], tr.at[1], me.g, 2 * fi + me.c).start()

    mine = lax.div(me.i, G) == me.t

    @pl.when(mine)
    def _():
        gout[...] = dwo[lax.rem(me.i, G)].astype(F32)

    @pl.when(jnp.logical_not(mine))
    def _():
        gout[...] = jnp.zeros(gout.shape, F32)

    for g in range(G):
        @pl.when(jnp.logical_not(mine & (me.g == g)))
        def _(g=g):
            landed(ro.at[g], or_.at[g])
            gout[...] += ro[g].astype(F32)

    saves.append(pltpu.make_async_copy(gout, GOUT, wsem.at[1]))
    saves[-1].start()
    landed(rs1.at[pl.ds(0, G - 1)], sr.at[0])
    total = small[...]
    for step in range(1, G):
        total = total + rs1[lax.rem(me.g + step, G)]
    s1[...] = total
    rs2[me.t] = total
    s_plane = lambda step: remote(sz, s1, rs2.at[me.t], ss.at[1], sr.at[1], me.g, lax.rem(me.t + step, T))
    for step in range(1, T):
        s_plane(step).start()

    for step in range(2, G - 1):
        line_x.step(step)
    gn.finish()
    saves.append(pltpu.make_async_copy(gs, GS, wsem.at[2]))
    saves[-1].start()
    landed(rs2.at[pl.ds(0, T - 1)], sr.at[1])
    total = rs2[0, 0 : sz.common]
    for t in range(1, T):
        total = total + rs2[t, 0 : sz.common]
    gsm[0 : sz.common] = total
    width = sz.small_rows - sz.common
    for t in range(T):
        gsm[sz.common + t * width : sz.common + (t + 1) * width] = rs2[t, sz.common :]
    saves.append(pltpu.make_async_copy(gsm, GSM, wsem.at[3]))
    saves[-1].start()

    line_x.total(acc)
    landed(raz.at[pl.ds(0, T - 1)], as_.at[0])
    szz[...] = acc[...].astype(BF16)
    hand(szz, rax, 1)
    landed(rtt.at[pl.ds(0, sz.fi - 1)], tr.at[1])
    st[...] = (tails(me.t)[...].astype(F32) + rtt[me.fa].astype(F32) + rtt[me.fb].astype(F32) + rtt[me.fd].astype(F32)).astype(BF16)
    t_line = lambda step: remote(sz, st.at[lax.rem(me.g + step, G)], rtz.at[me.g], us.at[0], ur.at[0], lax.rem(me.g + step, G), me.t)
    for step in range(1, G):
        t_line(step).start()
    landed(raz.at[pl.ds(0, T - 1)], ar_.at[0])
    saves.append(pltpu.make_async_copy(raz, RAZ, wsem.at[4]))
    saves[-1].start()
    landed(rtz.at[pl.ds(0, G - 1)], ur.at[0])
    total = st[me.g].astype(F32)
    for step in range(1, G):
        total = total + rtz[lax.rem(me.g + step, G)].astype(F32)
    gtl[...] = total
    saves.append(pltpu.make_async_copy(gtl, GTL, wsem.at[5]))
    saves[-1].start()
    landed(rax.at[pl.ds(0, T - 1)], ar_.at[1])
    saves.append(pltpu.make_async_copy(rax, RAX, wsem.at[6]))
    saves[-1].start()

    gn.sent0()
    gn.sent1()
    gn.sent2()
    line_x.sent()
    for k in range(G):
        @pl.when(t_differs(sz, me, k))
        def _(k=k):
            o_copy(k).wait_send()
    landed(raz.at[pl.ds(0, T - 1)], as_.at[1])
    landed(rtp, ts.at[0])
    landed(rtt.at[pl.ds(0, sz.fi - 1)], ts.at[1])
    landed(rtz.at[pl.ds(0, G - 1)], us.at[0])
    landed(rs1.at[pl.ds(0, G - 1)], ss.at[0])
    landed(rs2.at[pl.ds(0, T - 1)], ss.at[1])
    for copy in saves:
        copy.wait()


def run_back(sz, nt, go, px, pt, pz, y, gm, wx, wz, wt, wo, q, par, head, tile):
    n, g, t, rows, d, cs, tl = sz.n, sz.g, sz.t, sz.rows, sz.d, sz.cs, sz.tl
    dn, on = d // n, sz.di // n
    any_ = pl.BlockSpec(memory_space=pl.ANY)
    vmem = pl.BlockSpec(memory_space=pltpu.VMEM)
    dma = pltpu.SemaphoreType.DMA
    b = lambda *s: pltpu.VMEM(s, BF16)
    f = lambda *s: pltpu.VMEM(s, F32)
    sr = sz.small_rows
    total_rows = sz.common + t * (sr - sz.common)
    plane = lambda: [dma((4,)), dma((4,)), dma((2,)), dma((2,)), dma((1,)), dma((1,))]
    return pl.pallas_call(
        functools.partial(back_kernel, sz),
        in_specs=[any_] * 11 + [vmem] * 4,
        out_specs=[any_] * 7,
        out_shape=[
            jax.ShapeDtypeStruct((rows, d), F32),
            jax.ShapeDtypeStruct((rows, d), F32),
            jax.ShapeDtypeStruct((t, dn, cs), BF16),
            jax.ShapeDtypeStruct((t, dn, cs), BF16),
            jax.ShapeDtypeStruct((dn, tl), F32),
            jax.ShapeDtypeStruct((on, d), F32),
            jax.ShapeDtypeStruct((total_rows, LANES), F32),
        ],
        scratch_shapes=[
            b(d, t * rows), b(t, rows, d), f(2, max(3 * rows, -(-d // (2 * cs)) * rows), cs), f(2, rows, cs), f(2, rows, pt.shape[2]), b(n, dn, 2 * cs + tl), b(g, on, d),
            b(t, rows, 2 * cs + tl), f(t, rows, cs),
            b(4, rows, d), b(2, rows, d), b(rows, d), b(4, rows, d), b(2, rows, d), b(rows, d), f(rows, d),
            b(n, dn, max(cs, tl)), b(n, dn, cs), b(g, on, d), b(g + 1, t, dn, cs), b(g + 1, t, dn, cs), f(t, dn, cs),
            b(t, dn, cs), b(t, dn, cs), b(t, dn, cs), b(g, on, d), f(on, d), b(sz.fi, g, dn, tl), b(sz.fi, g, dn, tl), b(g, dn, tl), b(g, dn, tl), f(dn, tl),
            f(sr, LANES), f(g, sr, LANES), f(sr, LANES), f(t, sr, LANES), f(total_rows, LANES),
            dma((6,)), dma((2,)), dma((2, 2)), *plane(), *plane(), dma((g,)), dma((g + 1,)), dma((g,)), dma((g + 1,)), dma((g,)), dma((g,)),
            dma((2,)), dma((2,)), dma((2,)), dma((2,)), dma((1,)), dma((1,)), dma((2,)), dma((2,)), dma((7 + d // cs,)),
        ],
        compiler_params=pltpu.CompilerParams(collective_id=1, has_side_effects=True, vmem_limit_bytes=67043328),
        name="back",
    )(nt, go, px, pt, pz, y, gm, wx, wz, wt, wo, q, par, head, tile)


def finish_kernel(sz, HS, GS, X, GO, RAZ, RAX, GTL, GOUT, gsm, WIN, norm, par, HID, GIN, gnorm, GW, gcw, gcb, ggate, GWO, gdecay, gbias, gskip,
                  hs, gs, x, go, raz, rax, gtl, gout, win, hidden, gin, gw, sem):
    me = Place(sz)
    cs, T, taps = sz.cs, sz.t, sz.taps
    tiles = cs // LANES
    width = sz.small_rows - sz.common
    loads = [pltpu.make_async_copy(src, dst, sem.at[k]) for k, (src, dst) in enumerate(
        ((X, x), (HS, hs), (GS, gs), (GO, go), (GOUT, gout), (WIN, win), (RAZ, raz), (RAX, rax), (GTL, gtl)))]
    for copy in loads:
        copy.start()
    saves = [pltpu.make_async_copy(src, dst, sem.at[9 + k]) for k, (src, dst) in enumerate(((hidden, HID), (gin, GIN), (gout, GWO), (gw, GW)))]
    loads[0].wait()
    loads[1].wait()
    xb = x[...].astype(F32)
    hidden[...] = (xb + hs[...]).astype(BF16)
    saves[0].start()
    loads[2].wait()
    loads[3].wait()
    scale = lax.rsqrt(jnp.mean(xb * xb, axis=1, keepdims=True) + EPS)
    dxhat = gs[...] * par[taps + 2 : taps + 3, 0 : sz.d]
    inner = jnp.mean(dxhat * xb, axis=1, keepdims=True)
    gin[...] = go[...].astype(F32) + scale * (dxhat - xb * (scale * scale * inner))
    saves[1].start()
    loads[4].wait()
    saves[2].start()
    for copy in loads[5:]:
        copy.wait()
    dot = jnp.zeros((gw.shape[0], LANES), F32)
    for side, ref in ((0, raz), (1, rax)):
        for t in range(T):
            at = side * sz.di + t * cs
            piece = ref[t].astype(F32)
            gw[:, at : at + cs] = piece
            both = piece * win[:, at : at + cs].astype(F32)
            for j in range(tiles):
                dot = dot + both[:, j * LANES : (j + 1) * LANES]
    at = 2 * sz.di
    gw[:, at:] = gtl[:, 0 : sz.tail]
    saves[3].start()
    last = jnp.sum(gtl[:, 0 : sz.tail] * win[:, at:].astype(F32), axis=1, keepdims=True)
    dot = jnp.sum(dot, axis=1, keepdims=True) + last
    gnorm[...] = jnp.broadcast_to(dot, (dot.shape[0], LANES)).T[0:1, :] / norm[...].astype(F32)

    def window(row_of, rows, per):
        first = lax.div(me.i * per, LANES)
        off = lax.rem(me.i * per, LANES)
        wide = jnp.concatenate([gsm[pl.ds(row_of(first), rows), :], gsm[pl.ds(row_of(first + 1), rows), :]], axis=1)
        return pltpu.roll(wide, lax.rem(2 * LANES - off, 2 * LANES), 1)

    def conv_row(q):
        q = jnp.clip(q, 0, T * tiles + 2 * sz.state // LANES - 1)
        inside = sz.common + lax.div(q, tiles) * width + 8 * lax.rem(q, tiles)
        return pl.multiple_of(jnp.where(q < T * tiles, inside, sz.at_bc + 8 * (q - T * tiles)), 8)

    def gate_row(q):
        q = jnp.clip(q, 0, T * tiles - 1)
        return sz.common + lax.div(q, tiles) * width + sz.at_gate - sz.common + lax.rem(q, tiles)

    conv = window(conv_row, 8, gcb.shape[1])
    gcw[...] = conv[0:taps, 0 : gcw.shape[1]]
    gcb[...] = conv[taps : taps + 1, 0 : gcb.shape[1]]

    def spread(q):
        return jnp.broadcast_to(gsm[pl.ds(gate_row(q), 1), :], (8, LANES))

    first, off = lax.div(me.i * ggate.shape[1], LANES), lax.rem(me.i * ggate.shape[1], LANES)
    wide = jnp.concatenate([spread(first), spread(first + 1)], axis=1)
    ggate[...] = pltpu.roll(wide, lax.rem(2 * LANES - off, 2 * LANES), 1)[0:1, 0 : ggate.shape[1]]
    for t in range(T):
        row = sz.common + t * width + sz.at_head - sz.common
        for k, ref in enumerate((gdecay, gbias, gskip)):
            ref[:, t * sz.nh : (t + 1) * sz.nh] = gsm[row + k : row + k + 1, 0 : sz.nh]
    for copy in saves:
        copy.wait()


def run_finish(sz, hs, gs, x, go, raz, rax, gtl, gout, gsm, win, norm, par, kn, cn):
    vmem, any_ = pl.BlockSpec(memory_space=pltpu.VMEM), pl.BlockSpec(memory_space=pltpu.HBM)
    o = lambda *s: jax.ShapeDtypeStruct(s, F32)
    dn = win.shape[0]
    same = lambda a: pltpu.VMEM(a.shape, a.dtype)
    return pl.pallas_call(
        functools.partial(finish_kernel, sz),
        in_specs=[any_] * 8 + [vmem, any_, vmem, vmem],
        out_specs=[any_, any_, vmem, any_, vmem, vmem, vmem, any_, vmem, vmem, vmem],
        out_shape=[jax.ShapeDtypeStruct(x.shape, BF16), o(*x.shape), o(1, dn), o(*win.shape), o(sz.taps, cn), o(1, cn), o(1, kn), o(*gout.shape),
                   o(1, sz.heads), o(1, sz.heads), o(1, sz.heads)],
        scratch_shapes=[same(hs), same(gs), same(x), same(go), same(raz), same(rax), same(gtl), same(gout), same(win),
                        same(x), same(gs), pltpu.VMEM(win.shape, F32), pltpu.SemaphoreType.DMA((13,))],
        compiler_params=pltpu.CompilerParams(vmem_limit_bytes=67043328),
        name="finish",
    )(hs, gs, x, go, raz, rax, gtl, gout, gsm, win, norm, par)


def sizes(mesh, hidden, lengths, in_proj, conv_weight, gate_gain, decay_log):
    sz = Sizes()
    sz.f, sz.p = mesh.shape["fsdp"], mesh.shape["dp"]
    sz.n = sz.f * sz.p
    sz.rows, sz.d = hidden.shape
    sz.seqs = lengths.shape[1]
    sz.conv, sz.taps = conv_weight.shape[0] * sz.n, conv_weight.shape[1]
    sz.di = gate_gain.shape[0] * sz.n
    sz.state = (sz.conv - sz.di) // 2
    sz.heads = decay_log.shape[0]
    sz.hd = sz.di // sz.heads
    sz.fi = math.gcd(sz.f, sz.di // (2 * LANES))
    sz.t = 2 * sz.fi
    sz.z = sz.p // 2
    sz.g = sz.f // sz.fi * sz.z
    sz.aligned = sz.f == sz.fi
    sz.cs, sz.nh = sz.di // sz.t, sz.heads // sz.t
    sz.tail = in_proj.shape[1] - 2 * sz.di
    sz.tl = -(-sz.tail // LANES) * LANES
    sz.parts, sz.rparts = 2, 2
    sz.part_rows = sz.rows // sz.parts
    small_layout(sz)
    return sz


def local(mesh, hidden_in, lengths, norm_gain, in_proj, conv_weight, conv_bias, gate_gain, out_proj, decay_log, step_bias, skip_gain, grad_out):
    sz = sizes(mesh, hidden_in, lengths, in_proj, conv_weight, gate_gain, decay_log)
    di = sz.di
    dn, cn, kn = norm_gain.shape[0], conv_bias.shape[0], gate_gain.shape[0]

    tail = jnp.pad(in_proj[:, 2 * di :], ((0, 0), (0, sz.tl - sz.tail)))
    row = lambda a: a.reshape(1, -1)
    turned, go_all, px, pt, pz, y, gm, wx, wz, wt, wo, q, par, head, tile = run_front(
        sz, hidden_in, grad_out, in_proj, tail, out_proj, row(norm_gain), conv_weight.T, row(conv_bias), row(gate_gain), lengths,
        row(decay_log), row(step_bias), row(skip_gain))
    hs, gs, raz, rax, gtl, gout, gsm = run_back(sz, turned, go_all, px, pt, pz, y, gm, wx, wz, wt, wo, q, par, head, tile)
    hidden, gin, gnorm, gw, gcw, gcb, ggate, gwo, gdecay, gbias, gskip = run_finish(
        sz, hs, gs, hidden_in, grad_out, raz, rax, gtl, gout, gsm, in_proj, row(norm_gain), par, kn, cn)
    flat = lambda a: a.reshape(-1)
    return hidden, gin, flat(gnorm), gw, gcw.T, flat(gcb), flat(ggate), gwo, flat(gdecay), flat(gbias), flat(gskip)


def solution(mesh):
    both = ("fsdp", "dp")
    wide, flat, free = P(both, None), P(both), P()
    in_specs = (wide, wide, flat, wide, wide, flat, flat, wide, free, free, free, wide)
    out_specs = (wide, wide, flat, wide, wide, flat, flat, wide, free, free, free)
    return jax.shard_map(functools.partial(local, mesh), mesh=mesh, in_specs=in_specs, out_specs=out_specs, check_vma=False)
```

```python
import functools
import math

import jax
import jax.numpy as jnp
from jax import lax
from jax.experimental import pallas as pl
from jax.experimental.pallas import tpu as pltpu
from jax.sharding import PartitionSpec as P

EPS = 1e-05
F32 = jnp.float32
BF16 = jnp.bfloat16
EXACT = lax.Precision.HIGHEST
LANES = 128
LOG2E = math.log2(math.e)


def nn(a, b):
    return lax.dot_general(a, b, (((1,), (0,)), ((), ())), preferred_element_type=F32)


def nt(a, b):
    return lax.dot_general(a, b, (((1,), (1,)), ((), ())), preferred_element_type=F32)


def tn(a, b):
    return lax.dot_general(a, b, (((0,), (0,)), ((), ())), preferred_element_type=F32)


def iota(shape, dim):
    return lax.broadcasted_iota(jnp.int32, shape, dim)


def conv_tile(u, weights, bias, keeps, taps):
    pre = bias + u * weights[taps - 1 : taps, :]
    for off in range(1, taps):
        pre = pre + pltpu.roll(u, off, 0) * keeps[off - 1] * weights[taps - 1 - off : taps - off, :]
    return pre


def softplus(v):
    return jnp.maximum(v, 0.0) + jnp.log1p(jnp.exp(-jnp.abs(v)))


def split(a):
    hi = a.astype(BF16)
    return hi, (a - hi.astype(F32)).astype(BF16)


def three(product, a, b):
    ah, al = split(a)
    bh, bl = split(b)
    return product(ah, bh) + (product(ah, bl) + product(al, bh))


def running(mask, a):
    hi, mid = split(a)
    rest = a - hi.astype(F32) - mid.astype(F32)
    ones = jnp.where(mask, 1.0, 0.0).astype(BF16)
    return nn(ones, hi) + (nn(ones, mid) + nn(ones, rest.astype(BF16)))


class Sizes:
    pass


def up8(count):
    return -(-count // 8) * 8


def small_layout(sz):
    tiles = sz.cs // LANES
    sz.at_bc = 0
    sz.common = 2 * sz.state // LANES * 8
    sz.at_conv = sz.common
    sz.at_gate = sz.at_conv + tiles * 8
    sz.at_head = sz.at_gate + up8(tiles)
    sz.small_rows = sz.at_head + up8(3 + tiles)


def device_of(sz, g, t):
    return (lax.div(g, sz.z) * sz.fi + lax.div(t, 2), lax.rem(g, sz.z) * 2 + lax.rem(t, 2))


def index_of(sz, g, t):
    f, p = device_of(sz, g, t)
    return f * sz.p + p


class Place:
    def __init__(self, sz):
        f, p = lax.axis_index("fsdp"), lax.axis_index("dp")
        fi, z = lax.rem(f, sz.fi), lax.div(p, 2)
        self.c = lax.rem(p, 2)
        self.g = lax.div(f, sz.fi) * sz.z + z
        self.t = fi * 2 + self.c
        self.i = f * sz.p + p
        u, v = lax.rem(fi, 2), lax.div(fi, 2)
        across, along = v * 2 + 1 - u, (1 - v) * 2 + u
        self.fi = fi
        self.fa = across * (1 - self.c) + along * self.c
        self.fb = along * (1 - self.c) + across * self.c
        self.fd = sz.fi - 1 - fi
        self.other = 1 - self.c


def remote(sz, src, dst, send, recv, g, t):
    return pltpu.make_async_remote_copy(
        src_ref=src, dst_ref=dst, send_sem=send, recv_sem=recv, device_id=device_of(sz, g, t), device_id_type=pl.DeviceIdType.MESH
    )


def landed(ref, sem):
    pltpu.make_async_copy(ref, ref, sem).wait()


def greet_all(sz, me):
    barrier = pltpu.get_barrier_semaphore()

    @pl.loop(1, sz.n)
    def _(step):
        there = lax.rem(me.i + step, sz.n)
        pl.semaphore_signal(barrier, inc=1, device_id=(lax.div(there, sz.p), lax.rem(there, sz.p)), device_id_type=pl.DeviceIdType.MESH)

    pl.semaphore_wait(barrier, sz.n - 1)


def greet_near(sz, me):
    barrier = pltpu.get_barrier_semaphore()
    near = [(me.g, lax.rem(me.t + step, sz.t)) for step in range(1, sz.t)] + [(lax.rem(me.g + step, sz.g), me.t) for step in range(1, sz.g)]
    for g, t in near:
        pl.semaphore_signal(barrier, inc=1, device_id=device_of(sz, g, t), device_id_type=pl.DeviceIdType.MESH)
    pl.semaphore_wait(barrier, len(near))


class PlaneGather:
    def __init__(self, sz, me, parts, own, views, gauge, bulk, send, recv):
        self.sz, self.me, self.parts, self.own, self.views, self.gauge, self.bulk, self.send, self.recv = sz, me, parts, own, views, gauge, bulk, send, recv
        self.a, self.b, self.d = me.fa * 2 + me.c, me.fb * 2 + me.c, me.fd * 2 + me.c
        self.pair = me.fi * 2 + me.other

    def push(self, kind, part):
        slot = (self.me.t, self.me.t, self.me.t, self.a, self.a, self.b, self.d)[kind]
        target = (self.a, self.b, self.pair, self.b, self.pair, self.pair, self.pair)[kind]
        views = self.views(slot, part)
        for src, dst in zip(self.own(part) if kind < 3 else views, views):
            remote(self.sz, src, dst, self.send.at[0], self.recv.at[slot, part], self.me.g, target).start()

    def arrived(self, slot, part):
        landed(self.gauge, self.recv.at[slot, part])

    def start(self, part):
        for kind in range(3):
            self.push(kind, part)

    def relay(self, part):
        self.arrived(self.a, part)
        self.push(3, part)
        self.push(4, part)
        self.arrived(self.b, part)
        self.push(5, part)

    def relay_far(self, part):
        self.arrived(self.d, part)
        self.push(6, part)

    def sent(self):
        landed(self.bulk, self.send.at[0])


def t_differs(sz, me, k):
    return me.t * sz.g + k != me.i


def select_rows(sz, packed, channel, per):
    n = packed.shape[0]
    wide = channel.shape[1]
    owner = jnp.floor((channel + 0.5) * (1.0 / per))
    place = channel - owner * per
    pick = (iota((LANES, wide), 0).astype(F32) == place).astype(BF16)
    spread = nn(packed.reshape(n * 8, LANES).astype(BF16), pick).reshape(n, 8, wide)
    over = lambda v, by: jnp.floor((v + 0.5) * (1.0 / by))
    spot = iota((n, 8, LANES), 0).astype(F32)
    rank = over(spot, sz.g)
    plane = spot - sz.g * rank
    fi, fo = over(rank, 2), over(plane, sz.z)
    device = ((fo * sz.fi + fi) * sz.z + plane - sz.z * fo) * 2 + rank - 2 * fi
    total = jnp.zeros((8, wide), F32)
    parts = []
    for at in range(0, wide, LANES):
        hit = device == owner[None, :, at : at + LANES]
        parts.append(jnp.sum(jnp.where(hit, spread[:, :, at : at + LANES], 0.0), axis=0))
    return jnp.concatenate(parts, axis=1)


def lanes_of(wide):
    return iota((1, wide), 1).astype(F32)


def slot_of(me, k):
    flip = lambda bit, other: bit + other - 2 * bit * other
    v, u, c = lax.div(me.t, 4), lax.rem(lax.div(me.t, 2), 2), me.c
    kv, ku, kc = lax.div(k, 4), lax.rem(lax.div(k, 2), 2), lax.rem(k, 2)
    return (flip(v, kv) * 2 + flip(u, ku)) * 2 + flip(c, kc)


def ends_of(row, count):
    ends, total = [], jnp.zeros((1, 1), F32)
    for slot in range(count):
        total = total + row[:, slot : slot + 1]
        ends.append(total)
    return ends


def segments(pos, ends):
    total = jnp.zeros(pos.shape, F32)
    for end in ends:
        total = total + (pos >= end).astype(F32)
    return total


def masks(rows, ends, taps):
    pos = iota((rows, LANES), 0).astype(F32)
    seg = segments(pos, ends)
    keeps = []
    for off in range(1, taps):
        same = (segments(pos - off, ends) == seg) & (pos >= off)
        keeps.append(same.astype(F32))
    valid = (seg < len(ends)).astype(F32)
    seg_row = segments(lanes_of(rows), ends)
    same = jnp.concatenate([(seg == seg_row[:, at : at + LANES]) for at in range(0, rows, LANES)], axis=1)
    return keeps, valid, same


def triangle(rows):
    return iota((rows, rows), 0) >= iota((rows, rows), 1)


def front_kernel(sz, x, go, win, tail, wout, norm, cw, cb, gate, lens, decay, bias, skip,
                 NT, GO, PX, PT, PZ, Y, GM, WX, WZ, WT, WO, Q, PAR, HEAD, TILE,
                 xv, nv, gov, px, pt, pz, yv, gmv, wxv, wzv, wtv, wov, pack, smv, par, head, qv, qr, tilev, flip,
                 xsend, xrecv, gsend, grecv, wsend, wrecv, axsend, axrecv, azsend, azrecv, zxsend, zxrecv, zzsend, zzrecv,
                 tsend, trecv, osend, orecv, ssend, srecv, qsend, qrecv, lsem, esem, wsem, fsem):
    me = Place(sz)
    cs, rows, G, T, st, taps = sz.cs, sz.rows, sz.g, sz.t, sz.state, sz.taps
    tiles = cs // LANES
    pack[...] = jnp.zeros(pack.shape, F32)
    dn, cn, kn = norm.shape[1], cb.shape[1], gate.shape[1]
    pack[0:taps, 0:cn] = cw[...].astype(F32)
    pack[taps : taps + 1, 0:cn] = cb[...].astype(F32)
    pack[taps + 1 : taps + 2, 0:kn] = gate[...].astype(F32)
    pack[taps + 2 : taps + 3, 0:dn] = norm[...].astype(F32)
    pack[taps + 3 : taps + 4, 0 : sz.seqs] = lens[...].astype(F32)
    (greet_near if sz.aligned else greet_all)(sz, me)

    tile_of = lambda g, t: smv.at[t * G + g]

    def pack_line(step):
        return remote(sz, pack, tile_of(me.g, me.t), ssend.at[0], srecv.at[0], lax.rem(me.g + step, G), me.t)

    def pack_plane(step):
        mine = smv.at[pl.ds(me.t * G, G)]
        return remote(sz, mine, mine, ssend.at[1], srecv.at[1], me.g, lax.rem(me.t + step, T))

    def columns(half, t):
        return win.at[:, pl.ds(pl.multiple_of(half * sz.di + t * cs, LANES), cs)]

    def exchange(half, step):
        there = lax.rem(me.t + step, T)
        wv, send, recv = ((wzv, azsend, azrecv), (wxv, axsend, axrecv))[half]
        return remote(sz, columns(half, there), wv.at[me.i], send.at[0], recv.at[0], me.g, there)

    def tail_copy(step):
        there = lax.rem(me.g + step, G)
        return remote(sz, tail, wtv.at[me.i], tsend.at[0], trecv.at[0], there, me.t)

    for step in range(1, G):
        tail_copy(step).start()
        pack_line(step).start()
    for step in range(1, T):
        exchange(1, step).start()

    part = lambda ref, k: ref.at[pl.ds(k * sz.part_rows, sz.part_rows)]
    gx = PlaneGather(sz, me, sz.parts, lambda k: [part(x, k)], lambda s, k: [part(xv.at[s], k)], part(xv.at[0], 0), xv.at[pl.ds(0, T - 1)], xsend, xrecv)
    gg = PlaneGather(sz, me, sz.parts, lambda k: [part(go, k)], lambda s, k: [part(gov.at[s], k)], part(gov.at[0], 0), gov.at[pl.ds(0, T - 1)], gsend, grecv)
    tails_of = lambda s, k: [wtv.at[index_of(sz, jnp.int32(g), s)] for g in range(G)]
    gt = PlaneGather(sz, me, 1, lambda k: tails_of(me.t, k), tails_of, wtv.at[pl.ds(0, G)], wtv.at[pl.ds(0, (T - 1) * G)], wsend, wrecv)

    gx.start(0)
    owner_t, piece = lax.div(me.i, G), lax.rem(me.i, G)

    def out_copy(g):
        return remote(sz, wout, wov.at[piece], osend.at[2, g], orecv.at[piece], g, owner_t)

    def out_targets():
        planes = (me.g,) if sz.aligned else tuple(range(G))
        for g in planes:
            elsewhere = (owner_t != me.t) | (me.g != g)
            yield elsewhere, (lambda g=g: out_copy(jnp.int32(0) + g))

    def out_line(step, half, up):
        plane = me.g - step if up else me.g + step
        first = 2 * plane - me.c * sz.z
        have = (plane >= 0 if up else plane < G) & (first >= 0) & (first < G)
        more = (me.g < G - 1) if up else (me.g > 0)
        k = jnp.clip(first, 0, G - 2) + half
        nxt = jnp.clip(me.g + 1 if up else me.g - 1, 0, G - 1)
        copy = lambda: remote(sz, wov.at[k], wov.at[k], osend.at[int(up), k], orecv.at[k], nxt, me.t)
        return have, more, k, copy

    def out_advance(step):
        for half in range(2):
            if step == 0:
                have, _, k, _ = out_line(0, half, True)

                @pl.when(have & t_differs(sz, me, k))
                def _(k=k):
                    landed(wov.at[k], orecv.at[k])
            for up in (True, False):
                have, more, k, copy = out_line(step, half, up)
                if step > 0:
                    @pl.when(have)
                    def _(k=k):
                        landed(wov.at[k], orecv.at[k])
                if step < G - 1:
                    @pl.when(have & more)
                    def _(copy=copy):
                        copy().start()

    def out_steps(*steps):
        if sz.aligned:
            for step in steps:
                out_advance(step)

    for elsewhere, copy in out_targets():
        @pl.when(elsewhere)
        def _(copy=copy):
            copy().start()

    ins = [
        pltpu.make_async_copy(columns(1, me.t), wxv.at[me.i], lsem.at[0]),
        pltpu.make_async_copy(columns(0, me.t), wzv.at[me.i], lsem.at[1]),
        pltpu.make_async_copy(tail, wtv.at[me.i], lsem.at[2]),
        pltpu.make_async_copy(pack, tile_of(me.g, me.t), lsem.at[3]),
        pltpu.make_async_copy(x, xv.at[me.t], lsem.at[4]),
        pltpu.make_async_copy(go, gov.at[me.t], lsem.at[5]),
    ]
    for copy in ins:
        copy.start()
    for copy in ins:
        copy.wait()

    @pl.when(owner_t == me.t)
    def _():
        copy = pltpu.make_async_copy(wout, wov.at[piece], lsem.at[6])
        copy.start()
        copy.wait()

    head[...] = jnp.zeros(head.shape, F32)
    head[0:1, 0 : sz.heads] = bias[...]
    head[1:2, 0 : sz.heads] = decay[...]
    head[2:3, 0 : sz.heads] = skip[...]
    lead = lax.rem(LANES - sz.nh * me.t, LANES)
    head[...] = pltpu.roll(head[...], lead, 1)

    landed(smv.at[pl.ds(0, G - 1)], srecv.at[0])
    landed(wtv.at[pl.ds(0, G - 1)], trecv.at[0])
    for step in range(1, T):
        pack_plane(step).start()
    gt.start(0)
    for step in range(1, T):
        exchange(0, step).start()
    for p in range(1, sz.parts):
        gx.start(p)

    def arrive(half):
        wv, _, recv = ((wzv, azsend, azrecv), (wxv, axsend, axrecv))[half]
        landed(wv.at[pl.ds(0, T - 1)], recv.at[0])

    def line(half, step, up):
        wv, send, recv = ((wzv, zzsend, zzrecv), (wxv, zxsend, zxrecv))[half]
        plane = me.g - step if up else me.g + step
        have = (plane >= 0) if up else (plane < G)
        more = (me.g < G - 1) if up else (me.g > 0)
        plane = jnp.clip(plane, 0, G - 1)
        nxt = jnp.clip(me.g + 1 if up else me.g - 1, 0, G - 1)

        def push(part):
            for fi in range(part * sz.fi // 2, (part + 1) * sz.fi // 2):
                block = wv.at[pl.ds(index_of(sz, plane, jnp.int32(2 * fi)), 2)]
                remote(sz, block, block, send.at[int(up), plane], recv.at[part, plane], nxt, me.t).start()

        return have, more, plane, push, wv.at[pl.ds(0, T)], send, recv

    def advance(half, step):
        for part in range(2):
            for up in (True, False):
                have, more, plane, push, _, _, recv = line(half, step, up)
                if step > 0:
                    @pl.when(have)
                    def _(recv=recv, plane=plane, part=part):
                        landed(wxv.at[pl.ds(0, T // 2)], recv.at[part, plane])
                if step < G - 1:
                    @pl.when(have & more)
                    def _(push=push, part=part):
                        push(part)

    arrive(1)
    advance(1, 0)
    advance(1, 1)
    landed(smv.at[pl.ds(0, (T - 1) * G)], srecv.at[1])
    packed = smv[...]
    ch = lanes_of(cs + 2 * st)
    start_ch = (me.t * cs).astype(F32)
    ch = jnp.where(ch < cs, ch + start_ch, ch + (sz.di - cs))
    par[:, 0 : cs + 2 * st] = select_rows(sz, packed, ch, cn)
    picked = select_rows(sz, packed, lanes_of(cs) + start_ch, kn)
    par[taps + 1 : taps + 2, 0:cs] = picked[taps + 1 : taps + 2]
    gains = select_rows(sz, packed, lanes_of(sz.d), dn)
    par[taps + 2 : taps + 3, 0 : sz.d] = gains[taps + 2 : taps + 3]

    def normalize(k):
        slot = slot_of(me, k)
        xb = xv[slot].astype(F32)
        mean = jnp.mean(xb * xb, axis=1, keepdims=True)
        nrm = (xb * lax.rsqrt(mean + EPS) * par[taps + 2 : taps + 3, 0 : sz.d]).astype(BF16)
        nv[slot] = nrm
        half = lax.rem(k, 2)

        @pl.when(k > 1)
        def _():
            landed(flip.at[half], fsem.at[half])

        flip[half] = nrm.T
        pltpu.make_async_copy(flip.at[half], NT.at[:, pl.ds(pl.multiple_of(slot * rows, LANES), rows)], fsem.at[half]).start()

    def wait_pair(gather, k):
        slot = slot_of(me, k)
        for p in range(sz.parts):
            gather.arrived(slot, p)

    gt.relay(0)
    normalize(jnp.int32(0))
    wait_pair(gx, jnp.int32(1))
    normalize(jnp.int32(1))
    gx.relay(0)
    for step in range(2, G - 1):
        advance(1, step)
    arrive(0)
    advance(0, 0)
    advance(1, G - 1)
    for p in range(1, sz.parts):
        gx.relay(p)
    for p in range(sz.parts):
        gg.start(p)
    gt.relay_far(0)
    advance(0, 1)
    out_steps(0)
    for fi in (me.fi, me.fa, me.fb, me.fd):
        gt.arrived(fi * 2 + me.other, 0)

    low = iota((rows, LANES), 1) < sz.hd
    tri = triangle(rows)
    half_rows = rows // 2

    def scan(k):
        slot = slot_of(me, k)

        @pl.when((k > 2) & (lax.rem(k, 2) == 1))
        def _():
            wait_pair(gx, k)

        @pl.when(k > 1)
        def _():
            normalize(k)

        keeps, _, same = masks(rows, ends_of(smv[slot * G + me.g, taps + 3 : taps + 4, :], sz.seqs), taps)
        nrm = nv[slot]
        pxv = nn(nrm, wxv[...].reshape(sz.d, cs))
        ptl = nn(nrm, wtv[...].reshape(sz.d, sz.tl))
        px[slot] = pxv
        pltpu.make_async_copy(px.at[slot], PX.at[slot], esem.at[1]).start()

        def act(u, at):
            return jax.nn.silu(conv_tile(u, par[0:taps, at : at + LANES], par[taps : taps + 1, at : at + LANES], keeps, taps))

        bm = act(ptl[:, 0:st], cs)
        cm = act(ptl[:, st : 2 * st], cs + st)
        raw = pltpu.roll(ptl[:, 2 * st : 2 * st + LANES], lead, 1) + head[0:1, :]
        dt = softplus(raw)
        rate = -jnp.exp(head[1:2, :])
        log_decay = running(tri, dt * rate) * LOG2E
        pt[slot, :, 0 : 2 * st] = ptl[:, 0 : 2 * st]
        for a, kept in enumerate((raw, dt, log_decay)):
            pt[slot, :, 2 * st + a * LANES : 2 * st + (a + 1) * LANES] = kept
        pltpu.make_async_copy(pt.at[slot], PT.at[slot], esem.at[2]).start()
        log_t = log_decay.T
        drop = jnp.where(same & tri, 0.0, -jnp.inf)
        inner = three(nt, cm, bm)
        for j in range(tiles):
            at = j * LANES
            xa = act(pxv[:, at : at + LANES], at)
            dt2 = jnp.where(low, dt[:, 2 * j : 2 * j + 1], dt[:, 2 * j + 1 : 2 * j + 2])
            xd = xa * dt2
            tops, bottoms = [], []
            for e in range(2):
                h = 2 * j + e
                mine = low if e == 0 else jnp.logical_not(low)
                xm = jnp.where(mine, xd, 0.0).astype(BF16)
                for r, wide, into in ((slice(0, half_rows), half_rows, tops), (slice(half_rows, rows), rows, bottoms)):
                    spread = log_decay[r, h : h + 1] - log_t[h : h + 1, 0:wide]
                    f = (jnp.exp2(spread + drop[r, 0:wide]) * inner[r, 0:wide]).astype(BF16)
                    into.append(nn(f, xm[0:wide]))
            y = jnp.concatenate([tops[0] + tops[1], bottoms[0] + bottoms[1]], axis=0)
            skip2 = jnp.where(low[0:1], head[2:3, 2 * j : 2 * j + 1], head[2:3, 2 * j + 1 : 2 * j + 2])
            yv[slot, :, at : at + LANES] = y + xa * skip2
        pltpu.make_async_copy(yv.at[slot], Y.at[slot], esem.at[3]).start()

    def between(k, *steps):
        @pl.when(k)
        def _():
            for step in steps:
                step()

    whole = [(wxv, WX), (wtv, WT), (par, PAR), (head, HEAD), (wzv, WZ), (wov, WO), (tilev, TILE)]

    def save(*picked):
        for k in picked:
            pltpu.make_async_copy(*whole[k], wsem.at[k]).start()

    save(0, 1, 2, 3)

    @pl.loop(0, T)
    def _(k):
        between(k == 3, lambda: gx.relay_far(0))
        between(k == 4, lambda: [advance(0, step) for step in range(2, G - 1)])
        between(k == 5, lambda: [gx.relay_far(p) for p in range(1, sz.parts)])
        between(k == 6, lambda: out_steps(1))
        between(k == 7, lambda: advance(0, G - 1))
        scan(k)

    for p in range(sz.parts):
        gg.relay(p)
    out_steps(*range(2, G - 1))
    save(4)

    @pl.loop(0, T)
    def _(k):
        slot = slot_of(me, k)
        pz[slot] = nn(nv[slot], wzv[...].reshape(sz.d, cs))
        pltpu.make_async_copy(pz.at[slot], PZ.at[slot], esem.at[4]).start()

    out_steps(G - 1)
    if not sz.aligned:
        for k in range(G):
            @pl.when(t_differs(sz, me, k))
            def _(k=k):
                landed(wov.at[k], orecv.at[k])

    save(5)

    @pl.loop(0, T)
    def _(k):
        slot = slot_of(me, k)

        between(k == 6, lambda: [gg.relay_far(p) for p in range(sz.parts)])
        between(lax.rem(k, 2) == 1, lambda: wait_pair(gg, k))
        pos = iota((rows, LANES), 0).astype(F32)
        seg = segments(pos, ends_of(smv[slot * G + me.g, taps + 3 : taps + 4, :], sz.seqs))
        valid = (seg < sz.seqs).astype(F32)
        tilev[slot] = smv[slot * G + me.g]
        zt = pz[slot]
        gm = nt(gov[slot], wov[...].reshape(cs, sz.d))
        gmv[slot] = gm
        pltpu.make_async_copy(gmv.at[slot], GM.at[slot], esem.at[5]).start()
        pltpu.make_async_copy(gov.at[slot], GO.at[slot], esem.at[6]).start()
        q1 = jnp.zeros((rows, LANES), F32)
        q2 = jnp.zeros((rows, LANES), F32)
        for j in range(tiles):
            tile = slice(j * LANES, (j + 1) * LANES)
            gated = yv[slot, :, tile] * (zt[:, tile] * jax.nn.sigmoid(zt[:, tile]))
            q1 = q1 + gated * gated
            q2 = q2 + gated * gm[:, tile] * par[taps + 1 : taps + 2, tile]
        q2 = q2 * valid
        lane = iota((rows, LANES), 1)
        stats = jnp.where(lane == 0, jnp.sum(q1, axis=1, keepdims=True), jnp.sum(q2, axis=1, keepdims=True)).T
        qv[pl.ds(slot, 1), :] = stats[0:1, :]
        qv[pl.ds(T + slot, 1), :] = stats[1:2, :]

    save(6)

    def q_copy(step):
        return remote(sz, qv, qr.at[me.t], qsend.at[0], qrecv.at[0], me.g, lax.rem(me.t + step, T))

    for step in range(1, T):
        q_copy(step).start()

    landed(qr.at[pl.ds(0, T - 1)], qrecv.at[0])
    total = qv[...]
    for step in range(1, T):
        total = total + qr[lax.rem(me.t + step, T)]
    Q[...] = total

    landed(qr.at[pl.ds(0, T - 1)], qsend.at[0])
    landed(wxv.at[pl.ds(0, T - 1)], axsend.at[0])
    landed(wzv.at[pl.ds(0, T - 1)], azsend.at[0])
    landed(wtv.at[pl.ds(0, G - 1)], tsend.at[0])
    landed(smv.at[pl.ds(0, G - 1)], ssend.at[0])
    landed(smv.at[pl.ds(0, (T - 1) * G)], ssend.at[1])
    for gather in (gx, gg, gt):
        gather.sent()
    for elsewhere, copy in out_targets():
        @pl.when(elsewhere)
        def _(copy=copy):
            copy().wait_send()
    if sz.aligned:
        for step in range(G - 1):
            for half in range(2):
                for up in (True, False):
                    have, more, _, copy = out_line(step, half, up)

                    @pl.when(have & more)
                    def _(copy=copy):
                        copy().wait_send()
    for half in range(2):
        for step in range(G - 1):
            for up in (True, False):
                have, more, plane, _, gauge, send, _ = line(half, step, up)

                @pl.when(have & more)
                def _(gauge=gauge, send=send, plane=plane, up=up):
                    landed(gauge, send.at[int(up), plane])
    for k, (src, dst) in enumerate(whole):
        pltpu.make_async_copy(src, dst, wsem.at[k]).wait()
    for half in range(2):
        landed(flip.at[half], fsem.at[half])
    for a, (src, dst) in enumerate([(px, PX), (pt, PT), (yv, Y), (pz, PZ), (gmv, GM), (gov, GO)]):
        pltpu.make_async_copy(src, dst, esem.at[a + 1]).wait()


def run_front(sz, x, go, win, tail, wout, norm, cw, cb, gate, lens, decay, bias, skip):
    n, g, t, rows, d, cs, tl, parts, fi = sz.n, sz.g, sz.t, sz.rows, sz.d, sz.cs, sz.tl, sz.parts, sz.fi
    dn, on = win.shape[0], wout.shape[0]
    any_ = pl.BlockSpec(memory_space=pl.ANY)
    vmem = pl.BlockSpec(memory_space=pltpu.VMEM)
    dma = pltpu.SemaphoreType.DMA
    shapes = dict(
        nrm=((t, rows, d), BF16), nt=((d, t * rows), BF16), go=((t, rows, d), BF16), px=((t, rows, cs), F32), pt=((t, rows, 2 * sz.state + 3 * LANES), F32), pz=((t, rows, cs), F32),
        y=((t, rows, cs), F32), gm=((t, rows, cs), F32), wx=((n, dn, cs), BF16), wz=((n, dn, cs), BF16), wt=((n, dn, tl), BF16),
        wo=((g, on, d), BF16), q=((2 * t, rows), F32), par=((8, d), F32), head=((8, LANES), F32), tile=((t, 8, LANES), F32),
    )
    out = lambda *names: [jax.ShapeDtypeStruct(*shapes[name]) for name in names]
    scr = lambda *names: [pltpu.VMEM(*shapes[name]) for name in names]
    return pl.pallas_call(
        functools.partial(front_kernel, sz),
        in_specs=[any_] * 5 + [vmem] * 8,
        out_specs=[any_] * 11 + [vmem] + [any_] * 3,
        out_shape=out("nt", "go", "px", "pt", "pz", "y", "gm", "wx", "wz", "wt", "wo", "q", "par", "head", "tile"),
        scratch_shapes=scr("nrm", "nrm", "go", "px", "pt", "pz", "y", "gm", "wx", "wz", "wt", "wo")
        + [pltpu.VMEM((8, LANES), F32), pltpu.VMEM((n, 8, LANES), F32)]
        + scr("par", "head", "q")
        + [pltpu.VMEM((t, 2 * t, rows), F32), pltpu.VMEM((t, 8, LANES), F32), pltpu.VMEM((2, d, rows), BF16)]
        + [dma((1,)), dma((t, parts)), dma((1,)), dma((t, parts)), dma((1,)), dma((t, 1)), dma((1,)), dma((1,)), dma((1,)), dma((1,)),
           dma((2, g)), dma((2, g)), dma((2, g)), dma((2, g)), dma((1,)), dma((1,)), dma((3, g)), dma((g,)), dma((2,)), dma((2,)),
           dma((1,)), dma((1,)), dma((7,)), dma((7,)), dma((7,)), dma((2,))],
        compiler_params=pltpu.CompilerParams(collective_id=0, has_side_effects=True, vmem_limit_bytes=67043328),
        name="front",
    )(x, go, win, tail, wout, norm, cw, cb, gate, lens, decay, bias, skip)


class LineReduce:
    def __init__(self, sz, me, own, recv, send_sem, recv_sem):
        self.sz, self.me, self.own, self.recv, self.send_sem, self.recv_sem = sz, me, own, recv, send_sem, recv_sem

    def piece(self, p, part=None):
        t = self.sz.t
        return self.own.at[pl.ds(p * t, t)] if part is None else self.own.at[pl.ds(p * t + part * (t // 2), t // 2)]

    def got(self, p, part):
        return self.recv.at[p, pl.ds(part * (self.sz.t // 2), self.sz.t // 2)]

    def leg(self, step, up):
        g, last = self.me.g, self.sz.g - 1
        late = step - g if up else step - (last - g)
        p = last - late if up else late
        moves = (late >= 0) & ((p > g) if up else (p < g))
        p = jnp.clip(p, 0, last)
        inner = (g > 0) if up else (g < last)
        nxt = jnp.clip(g + 1 if up else g - 1, 0, last)
        there = p if up else jnp.where(p == nxt, last + 1, p)
        copy = lambda part: remote(self.sz, self.piece(p, part), self.got(there, part), self.send_sem.at[p], self.recv_sem.at[part, there], nxt, self.me.t)
        return p, moves, inner, copy

    def step(self, step):
        for part in range(2):
            for up in (True, False):
                p, moves, inner, copy = self.leg(step, up)

                @pl.when(moves & inner)
                def _(p=p, part=part):
                    landed(self.got(p, part), self.recv_sem.at[part, p])
                    piece = self.piece(p, part)
                    piece[...] = (piece[...].astype(F32) + self.got(p, part)[...].astype(F32)).astype(BF16)

                @pl.when(moves)
                def _(copy=copy, part=part):
                    copy(part).start()

    def total(self, acc):
        g = self.me.g
        acc[...] = self.piece(g)[...].astype(F32)
        for k, there in ((g, g > 0), (self.sz.g, g < self.sz.g - 1)):
            @pl.when(there)
            def _(k=k):
                for part in range(2):
                    landed(self.got(k, part), self.recv_sem.at[part, k])
                acc[...] += self.recv[k].astype(F32)

    def sent(self):
        for step in range(self.sz.g - 1):
            for up in (True, False):
                p, moves, _, _ = self.leg(step, up)

                @pl.when(moves)
                def _(p=p):
                    landed(self.piece(p), self.send_sem.at[p])


class PlaneReduce:
    def __init__(self, sz, me, stage, r0, s, r1, r2, out, sems):
        self.sz, self.me, self.stage, self.r0, self.s, self.r1, self.r2, self.out = sz, me, stage, r0, s, r1, r2, out
        self.send0, self.recv0, self.send1, self.recv1, self.send2, self.recv2 = sems

    def chip(self, w):
        m = self.me
        return jnp.where(w == 0, m.fa, jnp.where(w == 1, m.fd, jnp.where(w == 2, m.fb, m.fi)))

    def slot(self, k):
        w = lax.rem(k, 4)
        core = jnp.where(k < 4, self.me.other, self.me.c)
        return self.chip(w) * 2 + core

    def put0(self, w):
        return remote(self.sz, self.stage.at[w], self.r0.at[w], self.send0.at[w], self.recv0.at[w], self.me.g, self.me.fi * 2 + self.me.other)

    def put1(self, w):
        return remote(self.sz, self.s.at[w], self.r1.at[w], self.send1.at[w], self.recv1.at[w], self.me.g, self.me.fa * 2 + self.me.c)

    def put2(self):
        return remote(self.sz, self.s.at[2], self.r2, self.send2.at[0], self.recv2.at[0], self.me.g, self.me.fb * 2 + self.me.c)

    def block(self, k, value):
        w = lax.rem(k, 4)

        @pl.when(k < 4)
        def _():
            self.stage[w] = value.astype(BF16)
            self.put0(w).start()

        @pl.when(k >= 4)
        def _():
            there = jnp.where(w == 0, 2, jnp.where(w == 2, 0, w))
            landed(self.r0.at[there], self.recv0.at[there])
            total = value + self.r0[there].astype(F32)

            @pl.when(w < 3)
            def _():
                self.s[w] = total.astype(BF16)

            @pl.when(w < 2)
            def _():
                self.put1(w).start()

            @pl.when(w == 3)
            def _():
                self.out(total, False)

    def middle(self):
        landed(self.r1.at[1], self.recv1.at[1])
        self.s[2] = (self.s[2].astype(F32) + self.r1[1].astype(F32)).astype(BF16)
        self.put2().start()

    def finish(self):
        landed(self.r1.at[0], self.recv1.at[0])
        landed(self.r2, self.recv2.at[0])
        self.out(self.r1[0].astype(F32) + self.r2[...].astype(F32), True)

    def sent0(self):
        for w in range(4):
            self.put0(w).wait_send()

    def sent1(self):
        for w in range(2):
            self.put1(w).wait_send()

    def sent2(self):
        self.put2().wait_send()


def back_kernel(sz, NT, GO, PX, PT, PZ, Y, GM, WX, WZ, WT, WO, q_ref, par, head, tile_ref,
                HS, GS, RAZ, RAX, GTL, GOUT, GSM,
                nt_, gov, ra, rx, rt_, wall, wo, dp, dyv, r0h, r1h, r2h, r0g, r1g, r2g, gs,
                dwz, dwx, dwo, rzz, rzx, acc, szz, raz, rax, ro, gout, rtp, rtt, st, rtz, gtl, small, rs1, s1, rs2, gsm,
                lsem, asem, gsem, bsem, h0s, h0r, h1s, h1r, h2s, h2r, g0s, g0r, g1s, g1r, g2s, g2r, zzs, zzr, zxs, zxr, os_, or_, as_, ar_, ts, tr, us, ur, ss, sr, wsem):
    me = Place(sz)
    rows, cs, st_dim, taps, T, G, d = sz.rows, sz.cs, sz.state, sz.taps, sz.t, sz.g, sz.d
    tiles = cs // LANES
    half = rows // 2
    barrier = pltpu.get_barrier_semaphore()

    @pl.loop(1, sz.n)
    def _(step):
        there = lax.rem(me.i + step, sz.n)
        pl.semaphore_signal(barrier, inc=1, device_id=(lax.div(there, sz.p), lax.rem(there, sz.p)), device_id_type=pl.DeviceIdType.MESH)

    stage, sums = gov.at[pl.ds(0, 4)], gov.at[pl.ds(4, 3)]
    pieces = d // cs

    class Folded:
        def at(self, c):
            return ra.at[c // 2, pl.ds(c % 2 * rows, rows)]

        def put(self, value, more):
            for c in range(pieces):
                part = value[:, c * cs : (c + 1) * cs]
                self.at(c)[...] = self.at(c)[...] + part if more else part

    hid = PlaneReduce(sz, me, stage, r0h, sums, r1h, r2h, Folded().put, (h0s, h0r, h1s, h1r, h2s, h2r))
    def put_gs(value, more):
        gs[...] = gs[...] + value if more else value

    gn = PlaneReduce(sz, me, stage, r0g, sums, r1g, r2g, put_gs, (g0s, g0r, g1s, g1r, g2s, g2r))

    def fetch_a(k):
        slot, turn = hid.slot(k), lax.rem(k, 3)
        ring = [pltpu.make_async_copy(src.at[slot], ra.at[turn, pl.ds(a * rows, rows)], asem.at[turn]) for a, src in enumerate((PZ, Y))]
        return ring + [pltpu.make_async_copy(GM.at[slot], dyv.at[slot], gsem.at[slot])]

    def fetch_b(k):
        slot, par_ = gn.slot(k), lax.rem(k, 2)
        return [pltpu.make_async_copy(PX.at[slot], rx.at[par_], bsem.at[0, par_]), pltpu.make_async_copy(PT.at[slot], rt_.at[par_], bsem.at[1, par_])]

    for k in range(3):
        for copy in fetch_a(jnp.int32(k)):
            copy.start()
    loads = [pltpu.make_async_copy(src, dst, lsem.at[k]) for k, (src, dst) in enumerate((
        (NT, nt_), (WO, wo), (GO, gov), (WX, wall.at[:, :, pl.ds(cs, cs)]), (WZ, wall.at[:, :, pl.ds(0, cs)]), (WT, wall.at[:, :, pl.ds(2 * cs, sz.tl)])))]
    for copy in fetch_b(jnp.int32(0)):
        copy.start()
    small[...] = jnp.zeros(small.shape, F32)

    def colsum(v):
        return jnp.sum(v, axis=0, keepdims=True)

    def silu_pair(v):
        s = jax.nn.sigmoid(v)
        return v * s, s * (1.0 + v * (1.0 - s))

    def between(k, *steps):
        @pl.when(k)
        def _():
            for step in steps:
                step()

    @pl.loop(0, T)
    def _(k):
        slot, turn = hid.slot(k), lax.rem(k, 3)

        @pl.when(k == T // 2)
        def _():
            loads[0].start()

        landed(ra.at[turn], asem.at[turn])
        landed(dyv.at[slot], gsem.at[slot])
        pos = iota((rows, LANES), 0).astype(F32)
        valid = (segments(pos, ends_of(tile_ref[slot, taps + 3 : taps + 4, :], sz.seqs)) < sz.seqs).astype(F32)
        q1 = jnp.broadcast_to(q_ref[pl.ds(slot, 1), :], (LANES, rows)).T
        q2 = jnp.broadcast_to(q_ref[pl.ds(T + slot, 1), :], (LANES, rows)).T
        scale = lax.rsqrt(q1 / sz.di + EPS)
        pull = scale * scale * scale * q2 / sz.di
        for j in range(tiles):
            at = j * LANES
            tile = slice(at, at + LANES)
            zt, y = (ra[turn, a * rows : (a + 1) * rows, tile] for a in range(2))
            gm = dyv[slot, :, tile] * valid
            gate = par[taps + 1 : taps + 2, tile]
            up, slope = silu_pair(zt)
            gated = y * up
            unit = gated * scale
            dp[slot, :, cs + at : cs + at + LANES] = (unit * gate * valid).astype(BF16)
            small[sz.at_gate + j : sz.at_gate + j + 1, :] += colsum(gm * unit)
            dgated = scale * gm * gate - gated * pull
            dp[slot, :, tile] = (dgated * y * slope).astype(BF16)
            dyv[slot, :, tile] = dgated * up

        @pl.when(k + 3 < T)
        def _():
            for copy in fetch_a(k + 3):
                copy.start()

    for copy in loads[1:3]:
        copy.start()

    def weight_grad(first, wide, into, place):
        dn = sz.d // sz.n
        for at in range(0, sz.n, sz.n // 4):
            span = sz.n // 4 * dn
            got = nn(nt_[at * dn : at * dn + span, :], dp[:, :, first : first + wide].reshape(T * rows, wide))
            for i in range(at, at + sz.n // 4):
                f, p = i // sz.p, i % sz.p
                fo, fi, z, c = f // sz.fi, f % sz.fi, p // 2, p % 2
                into[place(fo * sz.z + z, fi * 2 + c), :, 0:wide] = got[(i - at) * dn : (i - at + 1) * dn].astype(BF16)

    line_z = LineReduce(sz, me, dwz.at[:, :, pl.ds(0, cs)], rzz, zzs, zzr)
    line_x = LineReduce(sz, me, dwx, rzx, zxs, zxr)
    loads[0].wait()
    by_plane, by_rank = lambda g, t: g * T + t, lambda g, t: t * G + g
    weight_grad(0, cs, dwz, by_plane)
    for copy in loads[3:]:
        copy.start()
    pl.semaphore_wait(barrier, sz.n - 1)
    line_z.step(0)
    loads[1].wait()

    loads[2].wait()

    def o_copy(k):
        owner = me.t * G + k
        return pltpu.make_async_remote_copy(src_ref=dwo.at[k], dst_ref=ro.at[me.g], send_sem=os_.at[k], recv_sem=or_.at[me.g],
                                            device_id=(lax.div(owner, sz.p), lax.rem(owner, sz.p)), device_id_type=pl.DeviceIdType.MESH)

    for at in range(0, d, d // 3):
        got = tn(dp[:, :, cs : 2 * cs].reshape(T * rows, cs), gov[:, :, at : at + d // 3].reshape(T * rows, d // 3))
        for k in range(G):
            dwo[k, :, at : at + d // 3] = got[k * (cs // G) : (k + 1) * (cs // G)].astype(BF16)
    def out_sends():
        for k in range(G):
            @pl.when(t_differs(sz, me, k))
            def _(k=k):
                o_copy(k).start()

    @pl.loop(0, T)
    def _(k):
        hid.block(k, nn(dp[hid.slot(k), :, cs : 2 * cs], wo[...].reshape(cs, d)))

    for copy in loads[3:]:
        copy.wait()

    low = iota((rows, LANES), 1) < sz.hd
    lane = iota((rows, LANES), 1)
    lead = lax.rem(LANES - sz.nh * me.t, LANES)
    quads = ((slice(0, half), slice(0, rows)), (slice(half, rows), slice(half, rows)))

    def scan_back(k):
        slot, par_ = gn.slot(k), lax.rem(k, 2)

        @pl.when(k + 1 < T)
        def _():
            for copy in fetch_b(k + 1):
                copy.start()

        landed(rx.at[par_], bsem.at[0, par_])
        landed(rt_.at[par_], bsem.at[1, par_])
        keeps, _, same = masks(rows, ends_of(tile_ref[slot, taps + 3 : taps + 4, :], sz.seqs), taps)

        def conv_pre(u, at):
            return conv_tile(u, par[0:taps, at : at + LANES], par[taps : taps + 1, at : at + LANES], keeps, taps)

        def conv_back(u, dact, dsilu, at):
            dpre = dact * dsilu
            tile = at // LANES
            row = sz.at_conv + tile * 8 if tile < tiles else sz.at_bc + (tile - tiles) * 8
            back = dpre * par[taps - 1 : taps, at : at + LANES]
            small[row + taps - 1 : row + taps, :] += colsum(dpre * u)
            small[row + taps : row + taps + 1, :] += colsum(dpre)
            for off in range(1, taps):
                kept = dpre * keeps[off - 1]
                tap = taps - 1 - off
                small[row + tap : row + tap + 1, :] += colsum(kept * pltpu.roll(u, off, 0))
                back = back + pltpu.roll(kept, rows - off, 0) * par[tap : tap + 1, at : at + LANES]
            return back

        ub, uc = rt_[par_, :, 0:st_dim], rt_[par_, :, st_dim : 2 * st_dim]
        bm, bslope = silu_pair(conv_pre(ub, cs))
        cm, cslope = silu_pair(conv_pre(uc, cs + st_dim))
        raw, dt, log_decay = (rt_[par_, :, 2 * st_dim + a * LANES : 2 * st_dim + (a + 1) * LANES] for a in range(3))
        rate = -jnp.exp(head[1:2, :])
        log_t = log_decay.T
        upper = iota((rows, rows), 1) >= iota((rows, rows), 0)
        drop = jnp.where(same & upper, 0.0, -jnp.inf)
        inner_t = three(nt, bm, cm)
        dcb = [jnp.zeros((half, rows), F32), jnp.zeros((half, half), F32)]
        ddt = jnp.zeros((rows, LANES), F32)
        cols = jnp.zeros((rows, LANES), F32)
        rowsums = jnp.zeros((up8(sz.nh), rows), F32)
        lane_row = iota((up8(sz.nh), rows), 0)
        for j in range(tiles):
            at = j * LANES
            tile = slice(at, at + LANES)
            dy = dyv[slot, :, tile]
            ux = rx[par_, :, tile]
            xa, xslope = silu_pair(conv_pre(ux, at))
            small[sz.at_head + 3 + j : sz.at_head + 4 + j, :] += colsum(dy * xa)
            dt2 = jnp.where(low, dt[:, 2 * j : 2 * j + 1], dt[:, 2 * j + 1 : 2 * j + 2])
            xd = xa * dt2
            dyh, dyl = split(dy)
            xh, xl = split(xd)
            left = jnp.concatenate([xh, xl, xh], axis=1)
            none = jnp.zeros((), BF16)
            tops = []
            for e in range(2):
                h = 2 * j + e
                mine = low if e == 0 else jnp.logical_not(low)
                dym, dyr = jnp.where(mine, dyh, none), jnp.where(mine, dyl, none)
                right = jnp.concatenate([dym, dym, dyr], axis=1)
                parts, psums, tsum = [], [], []
                for quad, (r, c) in enumerate(quads):
                    decay = jnp.exp2(log_t[h : h + 1, c] - log_decay[r, h : h + 1] + drop[r, c])
                    df = nt(left[r], right[c]) * decay
                    dcb[quad] = dcb[quad] + df
                    p = df * inner_t[r, c]
                    psums.append(jnp.sum(p, axis=1, keepdims=True))
                    tsum.append(colsum(p))
                    parts.append(nn((decay * inner_t[r, c]).astype(BF16), dym[c]))
                cols = jnp.where(lane == h, jnp.concatenate(psums, axis=0), cols)
                tsum = tsum[0] + jnp.concatenate([jnp.zeros((1, half), F32), tsum[1]], axis=1)
                rowsums = jnp.where(lane_row == h, tsum, rowsums)
                tops.append(jnp.concatenate(parts, axis=0))
            dxd = tops[0] + tops[1]
            both = dxd * xa
            ddt = jnp.where(lane == 2 * j, jnp.sum(jnp.where(low, both, 0.0), axis=1, keepdims=True), ddt)
            ddt = jnp.where(lane == 2 * j + 1, jnp.sum(jnp.where(low, 0.0, both), axis=1, keepdims=True), ddt)
            skip2 = jnp.where(low[0:1], head[2:3, 2 * j : 2 * j + 1], head[2:3, 2 * j + 1 : 2 * j + 2])
            dp[slot, :, cs + at : cs + at + LANES] = conv_back(ux, dxd * dt2 + dy * skip2, xslope, at).astype(BF16)

        rowsums = jnp.concatenate([rowsums, jnp.zeros((LANES - up8(sz.nh), rows), F32)], axis=0)
        ga = running(upper, rowsums.T - cols)
        ddt = ddt + ga * rate
        small[sz.at_head : sz.at_head + 1, :] += rate * colsum(ga * dt)
        draw = jnp.where(lane < sz.nh, ddt * jax.nn.sigmoid(raw), 0.0)
        small[sz.at_head + 1 : sz.at_head + 2, :] += colsum(draw)
        dp[slot, :, 2 * cs + 2 * st_dim : 2 * cs + 2 * st_dim + LANES] = pltpu.roll(draw, sz.nh * me.t, 1).astype(BF16)
        top, bottom = dcb[0].astype(BF16), dcb[1].astype(BF16)
        bb, cb = bm.astype(BF16), cm.astype(BF16)
        db = jnp.concatenate([nn(top, cb), nn(bottom, cb[half:])], axis=0)
        dc = tn(top, bb[:half]) + jnp.concatenate([jnp.zeros((half, st_dim), F32), tn(bottom, bb[half:])], axis=0)
        dp[slot, :, 2 * cs : 2 * cs + st_dim] = conv_back(ub, db, bslope, cs).astype(BF16)
        dp[slot, :, 2 * cs + st_dim : 2 * cs + 2 * st_dim] = conv_back(uc, dc, cslope, cs + st_dim).astype(BF16)
        between(k == 0, hid.sent0)
        between(k == 4, hid.sent1)
        between(k == 6, hid.sent2)
        gn.block(k, nt(dp[slot], wall[...].reshape(d, 2 * cs + sz.tl)))

    @pl.loop(0, T)
    def _(k):
        between(k == 0, lambda: line_z.step(1))
        between(k == 2, lambda: [line_z.step(step) for step in range(2, G - 1)], out_sends)
        between(k == 4, hid.middle)
        between(k == 7, hid.finish)
        scan_back(k)

    for j in range(tiles):
        spot = iota((LANES, LANES), 1) == 2 * j + (iota((LANES, LANES), 0) >= sz.hd).astype(jnp.int32)
        part = jnp.dot(small[sz.at_head + 3 + j : sz.at_head + 4 + j, :], spot.astype(F32), precision=EXACT, preferred_element_type=F32)
        small[sz.at_head + 2 : sz.at_head + 3, :] += part
    s_line = lambda step: remote(sz, small, rs1.at[me.g], ss.at[0], sr.at[0], lax.rem(me.g + step, G), me.t)
    for step in range(1, G):
        s_line(step).start()

    weight_grad(cs, cs, dwx, by_plane)
    line_x.step(0)
    line_z.total(acc)
    szz[...] = acc[...].astype(BF16)

    def hand(sums, into, k):
        for step in range(1, T):
            there = lax.rem(me.t + step, T)
            remote(sz, sums.at[there], into.at[me.t], as_.at[k], ar_.at[k], me.g, there).start()
        into[me.t] = sums[me.t]

    hand(szz, raz, 0)
    line_z.sent()
    weight_grad(2 * cs, sz.tl, dwz, by_rank)

    tails = lambda t: dwz.at[pl.ds(t * G, G), :, pl.ds(0, sz.tl)]
    for fi in range(sz.fi):
        remote(sz, tails(2 * fi + me.other), rtp.at[fi], ts.at[0], tr.at[0], me.g, me.fi * 2 + me.other).start()
    landed(rs1.at[pl.ds(0, G - 1)], sr.at[0])
    total = small[...]
    for step in range(1, G):
        total = total + rs1[lax.rem(me.g + step, G)]
    s1[...] = total
    rs2[me.t] = total
    s_plane = lambda step: remote(sz, s1, rs2.at[me.t], ss.at[1], sr.at[1], me.g, lax.rem(me.t + step, T))
    for step in range(1, T):
        s_plane(step).start()
    gn.middle()
    line_x.step(1)

    saves = [pltpu.make_async_copy(Folded().at(c), HS.at[:, pl.ds(c * cs, cs)], wsem.at[7 + c]) for c in range(pieces)]
    for copy in saves:
        copy.start()
    landed(rtp, tr.at[0])
    for fi in (me.fa, me.fb, me.fd, me.fi):
        mine = tails(2 * fi + me.c)
        mine[...] = (mine[...].astype(F32) + rtp[fi].astype(F32)).astype(BF16)
    for fi in (me.fd, me.fa, me.fb):
        remote(sz, tails(2 * fi + me.c), rtt.at[me.fi], ts.at[1], tr.at[1], me.g, 2 * fi + me.c).start()

    mine = lax.div(me.i, G) == me.t

    @pl.when(mine)
    def _():
        gout[...] = dwo[lax.rem(me.i, G)].astype(F32)

    @pl.when(jnp.logical_not(mine))
    def _():
        gout[...] = jnp.zeros(gout.shape, F32)

    for g in range(G):
        @pl.when(jnp.logical_not(mine & (me.g == g)))
        def _(g=g):
            landed(ro.at[g], or_.at[g])
            gout[...] += ro[g].astype(F32)

    saves.append(pltpu.make_async_copy(gout, GOUT, wsem.at[1]))
    saves[-1].start()
    for step in range(2, G - 1):
        line_x.step(step)
    gn.finish()
    saves.append(pltpu.make_async_copy(gs, GS, wsem.at[2]))
    saves[-1].start()
    landed(rtt.at[pl.ds(0, sz.fi - 1)], tr.at[1])
    st[...] = (tails(me.t)[...].astype(F32) + rtt[me.fa].astype(F32) + rtt[me.fb].astype(F32) + rtt[me.fd].astype(F32)).astype(BF16)
    t_line = lambda step: remote(sz, st.at[lax.rem(me.g + step, G)], rtz.at[me.g], us.at[0], ur.at[0], lax.rem(me.g + step, G), me.t)
    for step in range(1, G):
        t_line(step).start()
    landed(rs2.at[pl.ds(0, T - 1)], sr.at[1])
    total = rs2[0, 0 : sz.common]
    for t in range(1, T):
        total = total + rs2[t, 0 : sz.common]
    gsm[0 : sz.common] = total
    width = sz.small_rows - sz.common
    for t in range(T):
        gsm[sz.common + t * width : sz.common + (t + 1) * width] = rs2[t, sz.common :]
    saves.append(pltpu.make_async_copy(gsm, GSM, wsem.at[3]))
    saves[-1].start()

    line_x.total(acc)
    landed(raz.at[pl.ds(0, T - 1)], as_.at[0])
    szz[...] = acc[...].astype(BF16)
    hand(szz, rax, 1)
    landed(raz.at[pl.ds(0, T - 1)], ar_.at[0])
    saves.append(pltpu.make_async_copy(raz, RAZ, wsem.at[4]))
    saves[-1].start()
    landed(rtz.at[pl.ds(0, G - 1)], ur.at[0])
    total = st[me.g].astype(F32)
    for step in range(1, G):
        total = total + rtz[lax.rem(me.g + step, G)].astype(F32)
    gtl[...] = total
    saves.append(pltpu.make_async_copy(gtl, GTL, wsem.at[5]))
    saves[-1].start()
    landed(rax.at[pl.ds(0, T - 1)], ar_.at[1])
    saves.append(pltpu.make_async_copy(rax, RAX, wsem.at[6]))
    saves[-1].start()

    gn.sent0()
    gn.sent1()
    gn.sent2()
    line_x.sent()
    for k in range(G):
        @pl.when(t_differs(sz, me, k))
        def _(k=k):
            o_copy(k).wait_send()
    landed(raz.at[pl.ds(0, T - 1)], as_.at[1])
    landed(rtp, ts.at[0])
    landed(rtt.at[pl.ds(0, sz.fi - 1)], ts.at[1])
    landed(rtz.at[pl.ds(0, G - 1)], us.at[0])
    landed(rs1.at[pl.ds(0, G - 1)], ss.at[0])
    landed(rs2.at[pl.ds(0, T - 1)], ss.at[1])
    for copy in saves:
        copy.wait()


def run_back(sz, nt, go, px, pt, pz, y, gm, wx, wz, wt, wo, q, par, head, tile):
    n, g, t, rows, d, cs, tl = sz.n, sz.g, sz.t, sz.rows, sz.d, sz.cs, sz.tl
    dn, on = d // n, sz.di // n
    any_ = pl.BlockSpec(memory_space=pl.ANY)
    vmem = pl.BlockSpec(memory_space=pltpu.VMEM)
    dma = pltpu.SemaphoreType.DMA
    b = lambda *s: pltpu.VMEM(s, BF16)
    f = lambda *s: pltpu.VMEM(s, F32)
    sr = sz.small_rows
    total_rows = sz.common + t * (sr - sz.common)
    plane = lambda: [dma((4,)), dma((4,)), dma((2,)), dma((2,)), dma((1,)), dma((1,))]
    return pl.pallas_call(
        functools.partial(back_kernel, sz),
        in_specs=[any_] * 11 + [vmem] * 4,
        out_specs=[any_] * 7,
        out_shape=[
            jax.ShapeDtypeStruct((rows, d), F32),
            jax.ShapeDtypeStruct((rows, d), F32),
            jax.ShapeDtypeStruct((t, dn, cs), BF16),
            jax.ShapeDtypeStruct((t, dn, cs), BF16),
            jax.ShapeDtypeStruct((dn, tl), F32),
            jax.ShapeDtypeStruct((on, d), F32),
            jax.ShapeDtypeStruct((total_rows, LANES), F32),
        ],
        scratch_shapes=[
            b(d, t * rows), b(t, rows, d), f(3, 2 * rows, cs), f(2, rows, cs), f(2, rows, pt.shape[2]), b(n, dn, 2 * cs + tl), b(g, on, d),
            b(t, rows, 2 * cs + tl), f(t, rows, cs),
            b(4, rows, d), b(2, rows, d), b(rows, d), b(4, rows, d), b(2, rows, d), b(rows, d), f(rows, d),
            b(n, dn, max(cs, tl)), b(n, dn, cs), b(g, on, d), b(g + 1, t, dn, cs), b(g + 1, t, dn, cs), f(t, dn, cs),
            b(t, dn, cs), b(t, dn, cs), b(t, dn, cs), b(g, on, d), f(on, d), b(sz.fi, g, dn, tl), b(sz.fi, g, dn, tl), b(g, dn, tl), b(g, dn, tl), f(dn, tl),
            f(sr, LANES), f(g, sr, LANES), f(sr, LANES), f(t, sr, LANES), f(total_rows, LANES),
            dma((6,)), dma((3,)), dma((t,)), dma((2, 2)), *plane(), *plane(), dma((g,)), dma((2, g + 1)), dma((g,)), dma((2, g + 1)), dma((g,)), dma((g,)),
            dma((2,)), dma((2,)), dma((2,)), dma((2,)), dma((1,)), dma((1,)), dma((2,)), dma((2,)), dma((7 + d // cs,)),
        ],
        compiler_params=pltpu.CompilerParams(collective_id=1, has_side_effects=True, vmem_limit_bytes=67043328),
        name="back",
    )(nt, go, px, pt, pz, y, gm, wx, wz, wt, wo, q, par, head, tile)


def finish_kernel(sz, HS, GS, X, GO, RAZ, RAX, GTL, GOUT, gsm, WIN, norm, par, HID, GIN, gnorm, GW, gcw, gcb, ggate, GWO, gdecay, gbias, gskip,
                  hs, gs, x, go, raz, rax, gtl, gout, win, hidden, gin, gw, sem):
    me = Place(sz)
    cs, T, taps = sz.cs, sz.t, sz.taps
    tiles = cs // LANES
    width = sz.small_rows - sz.common
    loads = [pltpu.make_async_copy(src, dst, sem.at[k]) for k, (src, dst) in enumerate(
        ((X, x), (HS, hs), (GS, gs), (GO, go), (GOUT, gout), (WIN, win), (RAZ, raz), (RAX, rax), (GTL, gtl)))]
    for copy in loads:
        copy.start()
    saves = [pltpu.make_async_copy(src, dst, sem.at[9 + k]) for k, (src, dst) in enumerate(((hidden, HID), (gin, GIN), (gout, GWO), (gw, GW)))]
    loads[0].wait()
    loads[1].wait()
    xb = x[...].astype(F32)
    hidden[...] = (xb + hs[...]).astype(BF16)
    saves[0].start()
    loads[2].wait()
    loads[3].wait()
    scale = lax.rsqrt(jnp.mean(xb * xb, axis=1, keepdims=True) + EPS)
    dxhat = gs[...] * par[taps + 2 : taps + 3, 0 : sz.d]
    inner = jnp.mean(dxhat * xb, axis=1, keepdims=True)
    gin[...] = go[...].astype(F32) + scale * (dxhat - xb * (scale * scale * inner))
    saves[1].start()
    loads[4].wait()
    saves[2].start()
    for copy in loads[5:]:
        copy.wait()
    dot = jnp.zeros((gw.shape[0], LANES), F32)
    for side, ref in ((0, raz), (1, rax)):
        for t in range(T):
            at = side * sz.di + t * cs
            piece = ref[t].astype(F32)
            gw[:, at : at + cs] = piece
            both = piece * win[:, at : at + cs].astype(F32)
            for j in range(tiles):
                dot = dot + both[:, j * LANES : (j + 1) * LANES]
    at = 2 * sz.di
    gw[:, at:] = gtl[:, 0 : sz.tail]
    saves[3].start()
    last = jnp.sum(gtl[:, 0 : sz.tail] * win[:, at:].astype(F32), axis=1, keepdims=True)
    dot = jnp.sum(dot, axis=1, keepdims=True) + last
    gnorm[...] = jnp.broadcast_to(dot, (dot.shape[0], LANES)).T[0:1, :] / norm[...].astype(F32)

    def window(row_of, rows, per):
        first = lax.div(me.i * per, LANES)
        off = lax.rem(me.i * per, LANES)
        wide = jnp.concatenate([gsm[pl.ds(row_of(first), rows), :], gsm[pl.ds(row_of(first + 1), rows), :]], axis=1)
        return pltpu.roll(wide, lax.rem(2 * LANES - off, 2 * LANES), 1)

    def conv_row(q):
        q = jnp.clip(q, 0, T * tiles + 2 * sz.state // LANES - 1)
        inside = sz.common + lax.div(q, tiles) * width + 8 * lax.rem(q, tiles)
        return pl.multiple_of(jnp.where(q < T * tiles, inside, sz.at_bc + 8 * (q - T * tiles)), 8)

    def gate_row(q):
        q = jnp.clip(q, 0, T * tiles - 1)
        return sz.common + lax.div(q, tiles) * width + sz.at_gate - sz.common + lax.rem(q, tiles)

    conv = window(conv_row, 8, gcb.shape[1])
    gcw[...] = conv[0:taps, 0 : gcw.shape[1]]
    gcb[...] = conv[taps : taps + 1, 0 : gcb.shape[1]]

    def spread(q):
        return jnp.broadcast_to(gsm[pl.ds(gate_row(q), 1), :], (8, LANES))

    first, off = lax.div(me.i * ggate.shape[1], LANES), lax.rem(me.i * ggate.shape[1], LANES)
    wide = jnp.concatenate([spread(first), spread(first + 1)], axis=1)
    ggate[...] = pltpu.roll(wide, lax.rem(2 * LANES - off, 2 * LANES), 1)[0:1, 0 : ggate.shape[1]]
    for t in range(T):
        row = sz.common + t * width + sz.at_head - sz.common
        for k, ref in enumerate((gdecay, gbias, gskip)):
            ref[:, t * sz.nh : (t + 1) * sz.nh] = gsm[row + k : row + k + 1, 0 : sz.nh]
    for copy in saves:
        copy.wait()


def run_finish(sz, hs, gs, x, go, raz, rax, gtl, gout, gsm, win, norm, par, kn, cn):
    vmem, any_ = pl.BlockSpec(memory_space=pltpu.VMEM), pl.BlockSpec(memory_space=pltpu.HBM)
    o = lambda *s: jax.ShapeDtypeStruct(s, F32)
    dn = win.shape[0]
    same = lambda a: pltpu.VMEM(a.shape, a.dtype)
    return pl.pallas_call(
        functools.partial(finish_kernel, sz),
        in_specs=[any_] * 8 + [vmem, any_, vmem, vmem],
        out_specs=[any_, any_, vmem, any_, vmem, vmem, vmem, any_, vmem, vmem, vmem],
        out_shape=[jax.ShapeDtypeStruct(x.shape, BF16), o(*x.shape), o(1, dn), o(*win.shape), o(sz.taps, cn), o(1, cn), o(1, kn), o(*gout.shape),
                   o(1, sz.heads), o(1, sz.heads), o(1, sz.heads)],
        scratch_shapes=[same(hs), same(gs), same(x), same(go), same(raz), same(rax), same(gtl), same(gout), same(win),
                        same(x), same(gs), pltpu.VMEM(win.shape, F32), pltpu.SemaphoreType.DMA((13,))],
        compiler_params=pltpu.CompilerParams(vmem_limit_bytes=67043328),
        name="finish",
    )(hs, gs, x, go, raz, rax, gtl, gout, gsm, win, norm, par)


def sizes(mesh, hidden, lengths, in_proj, conv_weight, gate_gain, decay_log):
    sz = Sizes()
    sz.f, sz.p = mesh.shape["fsdp"], mesh.shape["dp"]
    sz.n = sz.f * sz.p
    sz.rows, sz.d = hidden.shape
    sz.seqs = lengths.shape[1]
    sz.conv, sz.taps = conv_weight.shape[0] * sz.n, conv_weight.shape[1]
    sz.di = gate_gain.shape[0] * sz.n
    sz.state = (sz.conv - sz.di) // 2
    sz.heads = decay_log.shape[0]
    sz.hd = sz.di // sz.heads
    sz.fi = math.gcd(sz.f, sz.di // (2 * LANES))
    sz.t = 2 * sz.fi
    sz.z = sz.p // 2
    sz.g = sz.f // sz.fi * sz.z
    sz.aligned = sz.f == sz.fi
    sz.cs, sz.nh = sz.di // sz.t, sz.heads // sz.t
    sz.tail = in_proj.shape[1] - 2 * sz.di
    sz.tl = -(-sz.tail // LANES) * LANES
    sz.parts, sz.rparts = 2, 2
    sz.part_rows = sz.rows // sz.parts
    small_layout(sz)
    return sz


def local(mesh, hidden_in, lengths, norm_gain, in_proj, conv_weight, conv_bias, gate_gain, out_proj, decay_log, step_bias, skip_gain, grad_out):
    sz = sizes(mesh, hidden_in, lengths, in_proj, conv_weight, gate_gain, decay_log)
    di = sz.di
    dn, cn, kn = norm_gain.shape[0], conv_bias.shape[0], gate_gain.shape[0]

    tail = jnp.pad(in_proj[:, 2 * di :], ((0, 0), (0, sz.tl - sz.tail)))
    row = lambda a: a.reshape(1, -1)
    turned, go_all, px, pt, pz, y, gm, wx, wz, wt, wo, q, par, head, tile = run_front(
        sz, hidden_in, grad_out, in_proj, tail, out_proj, row(norm_gain), conv_weight.T, row(conv_bias), row(gate_gain), lengths,
        row(decay_log), row(step_bias), row(skip_gain))
    hs, gs, raz, rax, gtl, gout, gsm = run_back(sz, turned, go_all, px, pt, pz, y, gm, wx, wz, wt, wo, q, par, head, tile)
    hidden, gin, gnorm, gw, gcw, gcb, ggate, gwo, gdecay, gbias, gskip = run_finish(
        sz, hs, gs, hidden_in, grad_out, raz, rax, gtl, gout, gsm, in_proj, row(norm_gain), par, kn, cn)
    flat = lambda a: a.reshape(-1)
    return hidden, gin, flat(gnorm), gw, gcw.T, flat(gcb), flat(ggate), gwo, flat(gdecay), flat(gbias), flat(gskip)


def solution(mesh):
    both = ("fsdp", "dp")
    wide, flat, free = P(both, None), P(both), P()
    in_specs = (wide, wide, flat, wide, wide, flat, flat, wide, free, free, free, wide)
    out_specs = (wide, wide, flat, wide, wide, flat, flat, wide, free, free, free)
    return jax.shard_map(functools.partial(local, mesh), mesh=mesh, in_specs=in_specs, out_specs=out_specs, check_vma=False)
```
